8 devices in a mesh: dp: 1 (over z), col: 2 (over y), row: 4 (over x, core).
Axes of the slice: x: 2, y: 2, z: 1, core: 2. Of those that a mesh axis runs over, the one named last changes fastest.
Arguments:
- x_in: bfloat16 [2048, 2048], P(('dp', 'row'), 'col')
- w_qkv: bfloat16 [2048, 6144], P('row', 'col')
- w_out: bfloat16 [2048, 2048], P('row', 'col')
- doc_ids: int32 [2048], P(('dp', 'row'))
- grad_y: bfloat16 [2048, 2048], P(('dp', 'row'), 'col')
Outputs:
- output 1: bfloat16 [2048, 2048], P(('dp', 'row'), 'col')
- output 2: bfloat16 [2048, 6144], P(('dp', 'row'), 'col')
- output 3: bfloat16 [2048, 2048], P(('dp', 'row'), 'col')
All inputs are finite; a program needn't handle non-finite values.
Results may differ from the reference program's by a relative error of at most 0.00385.
Values are sent between devices in bfloat16 or wider.
A program may use at most 1 GiB of HBM per device.

```python
import jax
import jax.numpy as jnp
from jax import lax

TOKENS = 2048
HIDDEN = 2048
HEADS = 16
HEAD_DIM = 128
QUERY_BLOCK = 256
DOCS = 3


def setup_inputs(seed: int = 0, part: int = 0) -> dict:
    part_key = jax.random.fold_in(jax.random.key(seed), part)
    key_x, key_doc, key_dy = jax.random.split(part_key, 3)
    key_wq, key_wo = jax.random.split(jax.random.key(seed + 1), 2)
    x_in = jax.random.normal(key_x, (TOKENS, HIDDEN), jnp.float32).astype(jnp.bfloat16)
    w_qkv = (jax.random.normal(key_wq, (HIDDEN, 3 * HIDDEN), jnp.float32) * HIDDEN ** -0.5).astype(jnp.bfloat16)
    w_out = (jax.random.normal(key_wo, (HIDDEN, HIDDEN), jnp.float32) * HIDDEN ** -0.5).astype(jnp.bfloat16)
    doc_cuts = jax.random.randint(key_doc, (DOCS - 1,), 1, TOKENS)
    doc_ids = jnp.sum(jnp.arange(TOKENS)[:, None] >= doc_cuts[None, :], axis=1).astype(jnp.int32)
    grad_y = jax.random.normal(key_dy, (TOKENS, HIDDEN), jnp.float32).astype(jnp.bfloat16)
    return {'x_in': x_in, 'w_qkv': w_qkv, 'w_out': w_out, 'doc_ids': doc_ids, 'grad_y': grad_y}


def reference(x_in, w_qkv, w_out, doc_ids, grad_y):
    sm_scale = HEAD_DIM ** -0.5
    n_blocks = TOKENS // QUERY_BLOCK
    qkv_all = jnp.dot(x_in, w_qkv, preferred_element_type=jnp.float32).astype(jnp.bfloat16)
    qkv_heads = jnp.transpose(qkv_all.reshape(TOKENS, HEADS, 3, HEAD_DIM), (1, 2, 0, 3))
    d_attn = jnp.dot(grad_y, w_out.T, preferred_element_type=jnp.float32).astype(jnp.bfloat16)
    dattn_heads = jnp.transpose(d_attn.reshape(TOKENS, HEADS, HEAD_DIM), (1, 0, 2))
    seg_blocks = doc_ids.reshape(n_blocks, QUERY_BLOCK)

    def one_head(head_args):
        qkv_head, do_head = head_args
        q_head = qkv_head[0]
        k_head = qkv_head[1]
        v_head = qkv_head[2]

        def one_block(acc_pair, blk_args):
            dk_acc, dv_acc = acc_pair
            q_blk, do_blk, seg_blk = blk_args
            scores = jnp.dot(q_blk, k_head.T, preferred_element_type=jnp.float32) * sm_scale
            scores = jnp.where(seg_blk[:, None] == doc_ids[None, :], scores, -jnp.inf)
            p_attn = jax.nn.softmax(scores, axis=-1)
            p_bf = p_attn.astype(jnp.bfloat16)
            o_blk = jnp.dot(p_bf, v_head, preferred_element_type=jnp.float32).astype(jnp.bfloat16)
            d_probs = jnp.dot(do_blk, v_head.T, preferred_element_type=jnp.float32)
            row_dot = jnp.sum(p_attn * d_probs, axis=-1, keepdims=True)
            d_scores = (p_attn * (d_probs - row_dot) * sm_scale).astype(jnp.bfloat16)
            dq_blk = jnp.dot(d_scores, k_head, preferred_element_type=jnp.float32)
            dk_acc = dk_acc + jnp.dot(d_scores.T, q_blk, preferred_element_type=jnp.float32)
            dv_acc = dv_acc + jnp.dot(p_bf.T, do_blk, preferred_element_type=jnp.float32)
            return (dk_acc, dv_acc), (o_blk, dq_blk)

        zero_acc = jnp.zeros((TOKENS, HEAD_DIM), jnp.float32)
        blk_inputs = (q_head.reshape(n_blocks, QUERY_BLOCK, HEAD_DIM), do_head.reshape(n_blocks, QUERY_BLOCK, HEAD_DIM), seg_blocks)
        (dk_head, dv_head), (o_head, dq_head) = lax.scan(one_block, (zero_acc, zero_acc), blk_inputs)
        dqkv_head = jnp.stack([dq_head.reshape(TOKENS, HEAD_DIM), dk_head, dv_head])
        return o_head.reshape(TOKENS, HEAD_DIM), dqkv_head

    attn_heads, dqkv_heads = lax.map(one_head, (qkv_heads, dattn_heads))
    attn_out = jnp.transpose(attn_heads, (1, 0, 2)).reshape(TOKENS, HIDDEN)
    d_qkv = jnp.transpose(dqkv_heads, (2, 0, 1, 3)).reshape(TOKENS, 3 * HIDDEN).astype(jnp.bfloat16)
    grad_x = jnp.dot(d_qkv, w_qkv.T, preferred_element_type=jnp.float32).astype(jnp.bfloat16)
    grad_wqkv = jnp.dot(x_in.T, d_qkv, preferred_element_type=jnp.float32).astype(jnp.bfloat16)
    grad_wout = jnp.dot(attn_out.T, grad_y, preferred_element_type=jnp.float32).astype(jnp.bfloat16)
    return (grad_x, grad_wqkv, grad_wout)
```

```python
import jax
import jax.numpy as jnp
from jax import lax
from jax.experimental import pallas as pl
from jax.experimental.pallas import tpu as pltpu
from jax.sharding import PartitionSpec as P

NT = (((1,), (1,)), ((), ()))
TN = (((0,), (0,)), ((), ()))
BQ = 256
BK = 512
D = 128

def attn_kernel(seg_ref, qkv_ref, do_ref, dqkv_ref, o_ref, cut, s_scr, dp_scr, dk_acc, dv_acc):
    qb = pl.program_id(0)
    n_q = pl.num_programs(0)
    seq = qkv_ref.shape[0]
    heads = qkv_ref.shape[1] // (3 * D)
    scale = D ** -0.5

    @pl.when(qb == 0)
    def _():
        seg = seg_ref[...]
        cut[0] = jnp.sum((seg < 1).astype(jnp.int32))
        cut[1] = jnp.sum((seg < 2).astype(jnp.int32))
        dk_acc[...] = jnp.zeros_like(dk_acc)
        dv_acc[...] = jnp.zeros_like(dv_acc)

    c1 = cut[0]
    c2 = cut[1]
    q0 = qb * BQ
    q1 = q0 + BQ - 1
    lo = jnp.where(q0 >= c2, c2, jnp.where(q0 >= c1, c1, 0))
    hi = jnp.where(q1 < c1, c1, jnp.where(q1 < c2, c2, seq))
    b_lo = lo // BK
    b_hi = (hi + BK - 1) // BK
    rows = pl.ds(pl.multiple_of(q0, BQ), BQ)
    iq = q0 + lax.broadcasted_iota(jnp.int32, (BQ, 1), 0)
    dq_doc = (iq >= c1).astype(jnp.int32) + (iq >= c2).astype(jnp.int32)
    q = [qkv_ref[rows, 3 * D * h:3 * D * h + D] for h in range(heads)]
    do = [do_ref[rows, D * h:D * h + D] for h in range(heads)]

    def first(kb, m):
        k0 = pl.multiple_of(kb * BK, BK)
        keys = pl.ds(k0, BK)
        ik = k0 + lax.broadcasted_iota(jnp.int32, (1, BK), 1)
        k_doc = (ik >= c1).astype(jnp.int32) + (ik >= c2).astype(jnp.int32)
        same = dq_doc == k_doc
        out = []
        for h in range(heads):
            k = qkv_ref[keys, 3 * D * h + D:3 * D * h + 2 * D]
            v = qkv_ref[keys, 3 * D * h + 2 * D:3 * D * h + 3 * D]
            s = lax.dot_general(q[h], k, NT, preferred_element_type=jnp.float32) * scale
            s = jnp.where(same, s, -jnp.inf)
            s_scr[h, :, keys] = s
            dp_scr[h, :, keys] = lax.dot_general(do[h], v, NT, preferred_element_type=jnp.float32)
            out.append(jnp.maximum(m[h], jnp.max(s, axis=1, keepdims=True)))
        return tuple(out)

    m = lax.fori_loop(b_lo, b_hi, first, tuple(jnp.full((BQ, 1), -jnp.inf, jnp.float32) for _ in range(heads)))

    def second(kb, ld):
        keys = pl.ds(pl.multiple_of(kb * BK, BK), BK)
        out = []
        for h in range(heads):
            p = jnp.exp(s_scr[h, :, keys] - m[h])
            s_scr[h, :, keys] = p
            l, dd = ld[h]
            out.append((l + jnp.sum(p, axis=1, keepdims=True), dd + jnp.sum(p * dp_scr[h, :, keys], axis=1, keepdims=True)))
        return tuple(out)

    zero = jnp.zeros((BQ, 1), jnp.float32)
    ld = lax.fori_loop(b_lo, b_hi, second, tuple((zero, zero) for _ in range(heads)))
    inv = [1.0 / ld[h][0] for h in range(heads)]
    row_dot = [ld[h][1] * inv[h] for h in range(heads)]
    inv_sc = [inv[h] * scale for h in range(heads)]

    def third(kb, acc):
        keys = pl.ds(pl.multiple_of(kb * BK, BK), BK)
        out = []
        for h in range(heads):
            k = qkv_ref[keys, 3 * D * h + D:3 * D * h + 2 * D]
            v = qkv_ref[keys, 3 * D * h + 2 * D:3 * D * h + 3 * D]
            p = s_scr[h, :, keys]
            p_bf = (p * inv[h]).astype(jnp.bfloat16)
            ds = ((p * inv_sc[h]) * (dp_scr[h, :, keys] - row_dot[h])).astype(jnp.bfloat16)
            o, dq = acc[h]
            o = o + jnp.dot(p_bf, v, preferred_element_type=jnp.float32)
            dq = dq + jnp.dot(ds, k, preferred_element_type=jnp.float32)
            dk_acc[h, keys, :] += lax.dot_general(ds, q[h], TN, preferred_element_type=jnp.float32)
            dv_acc[h, keys, :] += lax.dot_general(p_bf, do[h], TN, preferred_element_type=jnp.float32)
            out.append((o, dq))
        return tuple(out)

    zacc = jnp.zeros((BQ, D), jnp.float32)
    acc = lax.fori_loop(b_lo, b_hi, third, tuple((zacc, zacc) for _ in range(heads)))
    for h in range(heads):
        o_ref[rows, D * h:D * h + D] = acc[h][0].astype(jnp.bfloat16)
        dqkv_ref[rows, 3 * D * h:3 * D * h + D] = acc[h][1].astype(jnp.bfloat16)

    @pl.when(qb == n_q - 1)
    def _():
        for h in range(heads):
            dqkv_ref[:, 3 * D * h + D:3 * D * h + 2 * D] = dk_acc[h].astype(jnp.bfloat16)
            dqkv_ref[:, 3 * D * h + 2 * D:3 * D * h + 3 * D] = dv_acc[h].astype(jnp.bfloat16)

def attention(seg_row, qkv, d_attn):
    seq, width = qkv.shape
    heads = width // (3 * D)
    full = lambda shape: pl.BlockSpec(shape, lambda i: tuple(0 for _ in shape))
    return pl.pallas_call(
        attn_kernel,
        grid=(seq // BQ,),
        in_specs=[full(seg_row.shape), full(qkv.shape), full(d_attn.shape)],
        out_specs=[full(qkv.shape), full(d_attn.shape)],
        out_shape=[jax.ShapeDtypeStruct(qkv.shape, jnp.bfloat16), jax.ShapeDtypeStruct(d_attn.shape, jnp.bfloat16)],
        scratch_shapes=[
            pltpu.SMEM((2,), jnp.int32),
            pltpu.VMEM((heads, BQ, seq), jnp.float32),
            pltpu.VMEM((heads, BQ, seq), jnp.float32),
            pltpu.VMEM((heads, seq, D), jnp.float32),
            pltpu.VMEM((heads, seq, D), jnp.float32),
        ],
        compiler_params=pltpu.CompilerParams(dimension_semantics=("arbitrary",), vmem_limit_bytes=60 * 1024 * 1024),
    )(seg_row, qkv, d_attn)


def solution(mesh):
    tok_spec = P(('dp', 'row'), 'col')
    mat_spec = P('row', 'col')
    seg_spec = P(('dp', 'row'))

    def grad_step(x_blk, wqkv_blk, wout_blk, seg_blk, dy_blk):
        seq_loc, width_loc = x_blk.shape
        y = lax.axis_index('col')
        r = lax.axis_index('row')
        x_all = lax.all_gather(lax.all_gather(x_blk, 'col', axis=1, tiled=True), 'row', axis=0, tiled=True)
        dy_all = lax.all_gather(lax.all_gather(dy_blk, 'col', axis=1, tiled=True), 'row', axis=0, tiled=True)
        w_col = lax.all_gather(wqkv_blk, 'row', axis=0, tiled=True)
        wo_all = lax.all_gather(lax.all_gather(wout_blk, 'col', axis=1, tiled=True), 'row', axis=0, tiled=True)
        seg_all = lax.all_gather(seg_blk, 'row', axis=0, tiled=True)
        hw = w_col.shape[1] // 4
        ow = hw // 3
        w_h = lax.dynamic_slice_in_dim(w_col, r * hw, hw, 1)
        wo_h = lax.dynamic_slice_in_dim(wo_all, (y * 4 + r) * ow, ow, 0)
        qkv = jnp.dot(x_all, w_h, preferred_element_type=jnp.float32).astype(jnp.bfloat16)
        d_attn = lax.dot_general(dy_all, wo_h, NT, preferred_element_type=jnp.float32).astype(jnp.bfloat16)
        d_qkv, attn_out = attention(seg_all.reshape(-1, 128), qkv, d_attn)
        dw_h = lax.dot_general(x_all, d_qkv, TN, preferred_element_type=jnp.float32).astype(jnp.bfloat16)
        grad_wqkv = lax.all_to_all(dw_h, 'row', 0, 1, tiled=True)
        d_tok = lax.all_to_all(d_qkv, 'row', 0, 1, tiled=True)
        dx_part = lax.dot_general(d_tok, w_col, NT, preferred_element_type=jnp.float32)
        grad_x = lax.psum_scatter(dx_part, 'col', scatter_dimension=1, tiled=True).astype(jnp.bfloat16)
        dwo_h = lax.dot_general(attn_out, dy_all, TN, preferred_element_type=jnp.float32).astype(jnp.bfloat16)
        dwo_all = lax.all_gather(lax.all_gather(dwo_h, 'row', axis=0, tiled=True), 'col', axis=0, tiled=True)
        grad_wout = lax.dynamic_slice(dwo_all, (r * seq_loc, y * width_loc), (seq_loc, width_loc))
        return grad_x, grad_wqkv, grad_wout

    return jax.shard_map(grad_step, mesh=mesh, in_specs=(tok_spec, mat_spec, mat_spec, seg_spec, tok_spec), out_specs=(tok_spec, tok_spec, tok_spec), check_vma=False)
```

```python
import jax
import jax.numpy as jnp
from jax import lax
from jax.experimental import pallas as pl
from jax.experimental.pallas import tpu as pltpu
from jax.sharding import PartitionSpec as P

NT = (((1,), (1,)), ((), ()))
TN = (((0,), (0,)), ((), ()))
BQ = 256
BK = 512
D = 128

def attn_kernel(seg_ref, qkv_ref, do_ref, dqkv_ref, o_ref, cut, s_scr, dp_scr, dk_acc, dv_acc):
    qb = pl.program_id(0)
    n_q = pl.num_programs(0)
    seq = qkv_ref.shape[0]
    heads = qkv_ref.shape[1] // (3 * D)
    scale = D ** -0.5

    @pl.when(qb == 0)
    def _():
        seg = seg_ref[...]
        cut[0] = jnp.sum((seg < 1).astype(jnp.int32))
        cut[1] = jnp.sum((seg < 2).astype(jnp.int32))
        dk_acc[...] = jnp.zeros_like(dk_acc)
        dv_acc[...] = jnp.zeros_like(dv_acc)

    c1 = cut[0]
    c2 = cut[1]
    q0 = qb * BQ
    q1 = q0 + BQ - 1
    lo = jnp.where(q0 >= c2, c2, jnp.where(q0 >= c1, c1, 0))
    hi = jnp.where(q1 < c1, c1, jnp.where(q1 < c2, c2, seq))
    b_lo = lo // BK
    b_hi = (hi + BK - 1) // BK
    rows = pl.ds(pl.multiple_of(q0, BQ), BQ)
    iq = q0 + lax.broadcasted_iota(jnp.int32, (BQ, 1), 0)
    dq_doc = (iq >= c1).astype(jnp.int32) + (iq >= c2).astype(jnp.int32)
    q = [qkv_ref[rows, 3 * D * h:3 * D * h + D] for h in range(heads)]
    do = [do_ref[rows, D * h:D * h + D] for h in range(heads)]

    def first(kb, m):
        k0 = pl.multiple_of(kb * BK, BK)
        keys = pl.ds(k0, BK)
        ik = k0 + lax.broadcasted_iota(jnp.int32, (1, BK), 1)
        k_doc = (ik >= c1).astype(jnp.int32) + (ik >= c2).astype(jnp.int32)
        same = dq_doc == k_doc
        out = []
        for h in range(heads):
            k = qkv_ref[keys, 3 * D * h + D:3 * D * h + 2 * D]
            v = qkv_ref[keys, 3 * D * h + 2 * D:3 * D * h + 3 * D]
            s = lax.dot_general(q[h], k, NT, preferred_element_type=jnp.float32) * scale
            s = jnp.where(same, s, -jnp.inf)
            s_scr[h, :, keys] = s
            dp_scr[h, :, keys] = lax.dot_general(do[h], v, NT, preferred_element_type=jnp.float32)
            out.append(jnp.maximum(m[h], jnp.max(s, axis=1, keepdims=True)))
        return tuple(out)

    m = lax.fori_loop(b_lo, b_hi, first, tuple(jnp.full((BQ, 1), -jnp.inf, jnp.float32) for _ in range(heads)))

    def second(kb, ld):
        keys = pl.ds(pl.multiple_of(kb * BK, BK), BK)
        out = []
        for h in range(heads):
            p = jnp.exp(s_scr[h, :, keys] - m[h])
            s_scr[h, :, keys] = p
            l, dd = ld[h]
            out.append((l + jnp.sum(p, axis=1, keepdims=True), dd + jnp.sum(p * dp_scr[h, :, keys], axis=1, keepdims=True)))
        return tuple(out)

    zero = jnp.zeros((BQ, 1), jnp.float32)
    ld = lax.fori_loop(b_lo, b_hi, second, tuple((zero, zero) for _ in range(heads)))
    inv = [1.0 / ld[h][0] for h in range(heads)]
    row_dot = [ld[h][1] * inv[h] for h in range(heads)]
    inv_sc = [inv[h] * scale for h in range(heads)]

    def third(kb, acc):
        keys = pl.ds(pl.multiple_of(kb * BK, BK), BK)
        out = []
        for h in range(heads):
            k = qkv_ref[keys, 3 * D * h + D:3 * D * h + 2 * D]
            v = qkv_ref[keys, 3 * D * h + 2 * D:3 * D * h + 3 * D]
            p = s_scr[h, :, keys]
            p_bf = (p * inv[h]).astype(jnp.bfloat16)
            ds = ((p * inv_sc[h]) * (dp_scr[h, :, keys] - row_dot[h])).astype(jnp.bfloat16)
            o, dq = acc[h]
            o = o + jnp.dot(p_bf, v, preferred_element_type=jnp.float32)
            dq = dq + jnp.dot(ds, k, preferred_element_type=jnp.float32)
            dk_acc[h, keys, :] += lax.dot_general(ds, q[h], TN, preferred_element_type=jnp.float32)
            dv_acc[h, keys, :] += lax.dot_general(p_bf, do[h], TN, preferred_element_type=jnp.float32)
            out.append((o, dq))
        return tuple(out)

    zacc = jnp.zeros((BQ, D), jnp.float32)
    acc = lax.fori_loop(b_lo, b_hi, third, tuple((zacc, zacc) for _ in range(heads)))
    for h in range(heads):
        o_ref[rows, D * h:D * h + D] = acc[h][0].astype(jnp.bfloat16)
        dqkv_ref[rows, 3 * D * h:3 * D * h + D] = acc[h][1].astype(jnp.bfloat16)

    @pl.when(qb == n_q - 1)
    def _():
        for h in range(heads):
            dqkv_ref[:, 3 * D * h + D:3 * D * h + 2 * D] = dk_acc[h].astype(jnp.bfloat16)
            dqkv_ref[:, 3 * D * h + 2 * D:3 * D * h + 3 * D] = dv_acc[h].astype(jnp.bfloat16)

def attention(seg_row, qkv, d_attn):
    seq, width = qkv.shape
    heads = width // (3 * D)
    full = lambda shape: pl.BlockSpec(shape, lambda i: tuple(0 for _ in shape))
    return pl.pallas_call(
        attn_kernel,
        grid=(seq // BQ,),
        in_specs=[full(seg_row.shape), full(qkv.shape), full(d_attn.shape)],
        out_specs=[full(qkv.shape), full(d_attn.shape)],
        out_shape=[jax.ShapeDtypeStruct(qkv.shape, jnp.bfloat16), jax.ShapeDtypeStruct(d_attn.shape, jnp.bfloat16)],
        scratch_shapes=[
            pltpu.SMEM((2,), jnp.int32),
            pltpu.VMEM((heads, BQ, seq), jnp.float32),
            pltpu.VMEM((heads, BQ, seq), jnp.float32),
            pltpu.VMEM((heads, seq, D), jnp.float32),
            pltpu.VMEM((heads, seq, D), jnp.float32),
        ],
        compiler_params=pltpu.CompilerParams(dimension_semantics=("arbitrary",), vmem_limit_bytes=60 * 1024 * 1024),
    )(seg_row, qkv, d_attn)


MESH = pl.DeviceIdType.MESH
NC = 2


def place():
    y = lax.axis_index('col')
    r = lax.axis_index('row')
    c = lax.rem(r, 2)
    r_s = r + 1 - 2 * c
    return y, r, c, r_s, lax.rem(r + 2, 4), lax.rem(r_s + 2, 4)


def mult(i, n):
    return pl.multiple_of(i * n, n)


def gather_kernel(x_ref, w_ref, wo_ref, seg_ref, dy_ref, xg, dyg, wg, segg, qkv_ref, do_ref,
                  stage, wstage, wh, woh, tok, ssem, rsem, lsem):
    y, r, c, r_s, r_x, r_xs = place()
    x = r // 2
    t_loc, h_loc = x_ref.shape
    hw = wh.shape[1]
    ow = woh.shape[0]
    sib, xn, yn = {'row': r_s}, {'row': r_x}, {'col': 1 - y}
    ct = t_loc // NC
    started = []

    def send(i, src, dst, dev):
        cp = pltpu.make_async_remote_copy(src, dst, ssem.at[i], rsem.at[i], device_id=dev, device_id_type=MESH)
        cp.start()
        started.append(cp)

    def recv(i, dst):
        pltpu.make_async_remote_copy(dst, dst, ssem.at[i], rsem.at[i], device_id=sib, device_id_type=MESH).wait_recv()

    def local(i, src, dst):
        cp = pltpu.make_async_copy(src, dst, lsem.at[i])
        cp.start()
        return cp

    def slot(g, yy, rr, j):
        return g.at[pl.ds(pl.multiple_of(rr * t_loc + j * ct, ct), ct), pl.ds(mult(yy, h_loc), h_loc)]

    def own(a, j):
        return a.at[pl.ds(j * ct, ct)]

    def tid(base, kind, j):
        return base + kind * NC + j

    XB, YB = 0, 7 * NC
    WB = 14 * NC
    WOB = WB + 12
    SGB = WOB + 2

    def got_from(kind):
        return ((y, r_s), (y, r_x), (1 - y, r), (y, r_xs), (1 - y, r_x), (1 - y, r_s), (1 - y, r_xs))[kind]

    def send_own(a, g, base, kind, dev):
        for j in range(NC):
            send(tid(base, kind, j), own(a, j), slot(g, y, r, j), dev)

    def forward(g, base, kind_in, outs, j):
        yy, rr = got_from(kind_in)
        recv(tid(base, kind_in, j), slot(g, yy, rr, j))
        for kind_out, dev in outs:
            send(tid(base, kind_out, j), slot(g, yy, rr, j), slot(g, yy, rr, j), dev)

    def take(g, base, kind):
        yy, rr = got_from(kind)
        for j in range(NC):
            recv(tid(base, kind, j), slot(g, yy, rr, j))

    def wslot(rr, q):
        return wg.at[pl.ds(mult(rr, t_loc), t_loc), pl.ds(mult(q, hw), hw)]

    def wq(t, xx):
        return lax.rem(2 * xx + t, 4)

    def w_own(t, kind, xx, dev):
        q = wq(t, xx)
        send(WB + 4 * kind + t, w_ref.at[:, pl.ds(mult(q, hw), hw)], wslot(r, q), dev)

    def w_forward(t):
        q = wq(t, x)
        recv(WB + 4 + t, wslot(r_x, q))
        send(WB + 8 + t, wslot(r_x, q), wslot(r_x, q), sib)

    for i, (rr, dev) in enumerate(((r_s, sib), (r_x, xn), (r_xs, {'row': r_xs}))):
        send(SGB + i, seg_ref, segg.at[r], dev)
    send_own(x_ref, xg, XB, 1, xn)
    send_own(x_ref, xg, XB, 2, yn)
    for t in range(2):
        w_own(t, 1, 1 - x, xn)
    send_own(x_ref, xg, XB, 0, sib)
    for t in range(4):
        w_own(t, 0, x, sib)
    for k in range(2):
        row_to = 2 * c + k
        src = wo_ref.at[pl.ds(k * ow, ow)]
        dst = woh.at[:, pl.ds(mult(y, h_loc), h_loc)]
        mine = (x == y) & (row_to == r)

        @pl.when(mine)
        def _():
            pltpu.make_async_copy(src, dst, lsem.at[0]).start()

        @pl.when(jnp.logical_not(mine))
        def _():
            pltpu.make_async_remote_copy(src, dst, ssem.at[WOB + k], rsem.at[WOB + y],
                                         device_id={'col': x, 'row': row_to}, device_id_type=MESH).start()
    send_own(dy_ref, dyg, YB, 1, xn)
    send_own(dy_ref, dyg, YB, 0, sib)
    for t in range(2, 4):
        w_own(t, 1, 1 - x, xn)

    a = local(1, x_ref, stage.at[0])
    b = local(2, dy_ref, stage.at[1])
    d = local(3, w_ref, wstage)
    sg = local(4, seg_ref, segg.at[r])
    own_slot = lambda g: g.at[pl.ds(mult(r, t_loc), t_loc), pl.ds(mult(y, h_loc), h_loc)]
    a.wait()
    a = local(1, stage.at[0], own_slot(xg))
    b.wait()
    b = local(2, stage.at[1], own_slot(dyg))
    d.wait()
    d = local(3, wstage, wg.at[pl.ds(mult(r, t_loc), t_loc)])
    wh[pl.ds(mult(r, t_loc), t_loc), :] = wstage[:, pl.ds(mult(r, hw), hw)]

    for j in range(NC):
        forward(xg, XB, 1, ((4, yn), (3, sib)), j)
        forward(xg, XB, 2, ((5, sib),), j)
    send_own(dy_ref, dyg, YB, 2, yn)
    for j in range(NC):
        w_forward(j)
        forward(xg, XB, 4, ((6, sib),), j)
    a.wait()
    b.wait()
    d.wait()
    sg.wait()

    for t in range(4):
        recv(WB + t, wslot(r_s, wq(t, x)))
    for t in range(2):
        recv(WB + 8 + t, wslot(r_xs, wq(t, x)))
    loads = []
    for i, rr in enumerate((r_s, r_x, r_xs)):
        loads.append(local(5 + i, wslot(rr, r), wh.at[pl.ds(mult(rr, t_loc), t_loc)]))
    for kind in (0, 3, 5, 6):
        take(xg, XB, kind)

    def load_tok(g, rr, s):
        return local(8 + s, g.at[pl.ds(mult(rr, t_loc), t_loc)], tok.at[s])

    blocks = (r, r_s, r_x, r_xs)
    nxt = load_tok(xg, blocks[0], 0)
    for cp in loads:
        cp.wait()
    for i in range(4):
        nxt.wait()
        if i < 3:
            nxt = load_tok(xg, blocks[i + 1], (i + 1) % 2)
        rows = pl.ds(mult(blocks[i], t_loc), t_loc)
        for n in range(hw // 256):
            cols = slice(256 * n, 256 * n + 256)
            qkv_ref[rows, cols] = jnp.dot(tok[i % 2], wh[:, cols], preferred_element_type=jnp.float32).astype(jnp.bfloat16)

    for j in range(NC):
        forward(dyg, YB, 1, ((4, yn), (3, sib)), j)
        forward(dyg, YB, 2, ((5, sib),), j)
    for yy in range(2):
        piece = woh.at[:, pl.ds(yy * h_loc, h_loc)]
        mine = (y == yy) & (2 * y + x == r)

        @pl.when(mine)
        def _():
            pltpu.make_async_copy(wo_ref.at[pl.ds(0, ow)], piece, lsem.at[0]).wait()

        @pl.when(jnp.logical_not(mine))
        def _():
            recv(WOB + yy, piece)
    for kind in (0, 5):
        take(dyg, YB, kind)

    def d_out(i, s):
        rows = pl.ds(mult(blocks[i], t_loc), t_loc)
        do_ref[rows, :] = lax.dot_general(tok[s], woh[...], NT, preferred_element_type=jnp.float32).astype(jnp.bfloat16)

    one = load_tok(dyg, r, 0)
    two = load_tok(dyg, r_s, 1)
    one.wait()
    d_out(0, 0)
    two.wait()
    d_out(1, 1)
    for j in range(NC):
        forward(dyg, YB, 4, ((6, sib),), j)
    w_forward(2)
    take(dyg, YB, 3)
    one = load_tok(dyg, r_x, 0)
    take(dyg, YB, 6)
    two = load_tok(dyg, r_xs, 1)
    one.wait()
    d_out(2, 0)
    two.wait()
    d_out(3, 1)
    w_forward(3)
    for t in range(2, 4):
        recv(WB + 8 + t, wslot(r_xs, wq(t, x)))
    for i, rr in enumerate((r_s, r_x, r_xs)):
        recv(SGB + i, segg.at[rr])
    for cp in started:
        cp.wait_send()
    for k in range(2):
        mine = (x == y) & (2 * c + k == r)

        @pl.when(jnp.logical_not(mine))
        def _():
            pltpu.make_async_remote_copy(wo_ref.at[pl.ds(0, ow)], woh.at[:, pl.ds(0, h_loc)], ssem.at[WOB + k], rsem.at[WOB + k],
                                         device_id=sib, device_id_type=MESH).wait_send()


def gather_all(x_blk, w_blk, wo_blk, seg_blk, dy_blk):
    t_loc, h_loc = x_blk.shape
    w_loc = w_blk.shape[1]
    seq, hid = 4 * t_loc, 2 * h_loc
    hw, ow = w_loc // 4, w_loc // 12
    bf = jnp.bfloat16
    hbm = pl.BlockSpec(memory_space=pl.ANY)
    vmem = pl.BlockSpec(memory_space=pltpu.VMEM)
    n_sem = 14 * NC + 12 + 2 + 3
    return pl.pallas_call(
        gather_kernel,
        in_specs=[hbm] * 5,
        out_specs=[hbm] * 4 + [vmem] * 2,
        out_shape=[
            jax.ShapeDtypeStruct((seq, hid), bf), jax.ShapeDtypeStruct((seq, hid), bf),
            jax.ShapeDtypeStruct((hid, w_loc), bf), jax.ShapeDtypeStruct((4,) + seg_blk.shape, jnp.int32),
            jax.ShapeDtypeStruct((seq, hw), bf), jax.ShapeDtypeStruct((seq, ow), bf),
        ],
        scratch_shapes=[
            pltpu.VMEM((2, t_loc, h_loc), bf), pltpu.VMEM((t_loc, w_loc), bf), pltpu.VMEM((hid, hw), bf),
            pltpu.VMEM((ow, hid), bf), pltpu.VMEM((2, t_loc, hid), bf),
            pltpu.SemaphoreType.DMA((n_sem,)), pltpu.SemaphoreType.DMA((n_sem,)), pltpu.SemaphoreType.DMA((10,)),
        ],
        compiler_params=pltpu.CompilerParams(has_side_effects=True, vmem_limit_bytes=48 * 1024 * 1024),
        name='gather_project',
    )(x_blk, w_blk, wo_blk, seg_blk, dy_blk)


def solution(mesh):
    tok_spec = P(('dp', 'row'), 'col')
    mat_spec = P('row', 'col')
    seg_spec = P(('dp', 'row'))

    def grad_step(x_blk, wqkv_blk, wout_blk, seg_blk, dy_blk):
        seq_loc, width_loc = x_blk.shape
        y = lax.axis_index('col')
        r = lax.axis_index('row')
        x_all, dy_all, w_col, seg_all, qkv, d_attn = gather_all(x_blk, wqkv_blk, wout_blk, seg_blk.reshape(4, -1), dy_blk)
        d_qkv, attn_out = attention(seg_all, qkv, d_attn)
        dw_h = lax.dot_general(x_all, d_qkv, TN, preferred_element_type=jnp.float32).astype(jnp.bfloat16)
        grad_wqkv = lax.all_to_all(dw_h, 'row', 0, 1, tiled=True)
        d_tok = lax.all_to_all(d_qkv, 'row', 0, 1, tiled=True)
        dx_part = lax.dot_general(d_tok, w_col, NT, preferred_element_type=jnp.float32)
        grad_x = lax.psum_scatter(dx_part, 'col', scatter_dimension=1, tiled=True).astype(jnp.bfloat16)
        dwo_h = lax.dot_general(attn_out, dy_all, TN, preferred_element_type=jnp.float32).astype(jnp.bfloat16)
        dwo_all = lax.all_gather(lax.all_gather(dwo_h, 'row', axis=0, tiled=True), 'col', axis=0, tiled=True)
        grad_wout = lax.dynamic_slice(dwo_all, (r * seq_loc, y * width_loc), (seq_loc, width_loc))
        return grad_x, grad_wqkv, grad_wout

    return jax.shard_map(grad_step, mesh=mesh, in_specs=(tok_spec, mat_spec, mat_spec, seg_spec, tok_spec), out_specs=(tok_spec, tok_spec, tok_spec), check_vma=False)
```

```python
import jax
import jax.numpy as jnp
from jax import lax
from jax.experimental import pallas as pl
from jax.experimental.pallas import tpu as pltpu
from jax.sharding import PartitionSpec as P

NT = (((1,), (1,)), ((), ()))
TN = (((0,), (0,)), ((), ()))
BQ = 256
BK = 512
D = 128

def attn_kernel(seg_ref, qkv_ref, do_ref, dqkv_ref, o_ref, cut, s_scr, dp_scr, dk_acc, dv_acc):
    qb = pl.program_id(0)
    n_q = pl.num_programs(0)
    seq = qkv_ref.shape[0]
    heads = qkv_ref.shape[1] // (3 * D)
    scale = D ** -0.5

    @pl.when(qb == 0)
    def _():
        seg = seg_ref[...]
        cut[0] = jnp.sum((seg < 1).astype(jnp.int32))
        cut[1] = jnp.sum((seg < 2).astype(jnp.int32))
        dk_acc[...] = jnp.zeros_like(dk_acc)
        dv_acc[...] = jnp.zeros_like(dv_acc)

    c1 = cut[0]
    c2 = cut[1]
    q0 = qb * BQ
    q1 = q0 + BQ - 1
    lo = jnp.where(q0 >= c2, c2, jnp.where(q0 >= c1, c1, 0))
    hi = jnp.where(q1 < c1, c1, jnp.where(q1 < c2, c2, seq))
    b_lo = lo // BK
    b_hi = (hi + BK - 1) // BK
    rows = pl.ds(pl.multiple_of(q0, BQ), BQ)
    iq = q0 + lax.broadcasted_iota(jnp.int32, (BQ, 1), 0)
    dq_doc = (iq >= c1).astype(jnp.int32) + (iq >= c2).astype(jnp.int32)
    q = [qkv_ref[rows, 3 * D * h:3 * D * h + D] for h in range(heads)]
    do = [do_ref[rows, D * h:D * h + D] for h in range(heads)]

    def first(kb, m):
        k0 = pl.multiple_of(kb * BK, BK)
        keys = pl.ds(k0, BK)
        ik = k0 + lax.broadcasted_iota(jnp.int32, (1, BK), 1)
        k_doc = (ik >= c1).astype(jnp.int32) + (ik >= c2).astype(jnp.int32)
        same = dq_doc == k_doc
        out = []
        for h in range(heads):
            k = qkv_ref[keys, 3 * D * h + D:3 * D * h + 2 * D]
            v = qkv_ref[keys, 3 * D * h + 2 * D:3 * D * h + 3 * D]
            s = lax.dot_general(q[h], k, NT, preferred_element_type=jnp.float32) * scale
            s = jnp.where(same, s, -jnp.inf)
            s_scr[h, :, keys] = s
            dp_scr[h, :, keys] = lax.dot_general(do[h], v, NT, preferred_element_type=jnp.float32)
            out.append(jnp.maximum(m[h], jnp.max(s, axis=1, keepdims=True)))
        return tuple(out)

    m = lax.fori_loop(b_lo, b_hi, first, tuple(jnp.full((BQ, 1), -jnp.inf, jnp.float32) for _ in range(heads)))

    def second(kb, ld):
        keys = pl.ds(pl.multiple_of(kb * BK, BK), BK)
        out = []
        for h in range(heads):
            p = jnp.exp(s_scr[h, :, keys] - m[h])
            s_scr[h, :, keys] = p
            l, dd = ld[h]
            out.append((l + jnp.sum(p, axis=1, keepdims=True), dd + jnp.sum(p * dp_scr[h, :, keys], axis=1, keepdims=True)))
        return tuple(out)

    zero = jnp.zeros((BQ, 1), jnp.float32)
    ld = lax.fori_loop(b_lo, b_hi, second, tuple((zero, zero) for _ in range(heads)))
    inv = [1.0 / ld[h][0] for h in range(heads)]
    row_dot = [ld[h][1] * inv[h] for h in range(heads)]
    inv_sc = [inv[h] * scale for h in range(heads)]

    def third(kb, acc):
        keys = pl.ds(pl.multiple_of(kb * BK, BK), BK)
        out = []
        for h in range(heads):
            k = qkv_ref[keys, 3 * D * h + D:3 * D * h + 2 * D]
            v = qkv_ref[keys, 3 * D * h + 2 * D:3 * D * h + 3 * D]
            p = s_scr[h, :, keys]
            p_bf = (p * inv[h]).astype(jnp.bfloat16)
            ds = ((p * inv_sc[h]) * (dp_scr[h, :, keys] - row_dot[h])).astype(jnp.bfloat16)
            o, dq = acc[h]
            o = o + jnp.dot(p_bf, v, preferred_element_type=jnp.float32)
            dq = dq + jnp.dot(ds, k, preferred_element_type=jnp.float32)
            dk_acc[h, keys, :] += lax.dot_general(ds, q[h], TN, preferred_element_type=jnp.float32)
            dv_acc[h, keys, :] += lax.dot_general(p_bf, do[h], TN, preferred_element_type=jnp.float32)
            out.append((o, dq))
        return tuple(out)

    zacc = jnp.zeros((BQ, D), jnp.float32)
    acc = lax.fori_loop(b_lo, b_hi, third, tuple((zacc, zacc) for _ in range(heads)))
    for h in range(heads):
        o_ref[rows, D * h:D * h + D] = acc[h][0].astype(jnp.bfloat16)
        dqkv_ref[rows, 3 * D * h:3 * D * h + D] = acc[h][1].astype(jnp.bfloat16)

    @pl.when(qb == n_q - 1)
    def _():
        for h in range(heads):
            dqkv_ref[:, 3 * D * h + D:3 * D * h + 2 * D] = dk_acc[h].astype(jnp.bfloat16)
            dqkv_ref[:, 3 * D * h + 2 * D:3 * D * h + 3 * D] = dv_acc[h].astype(jnp.bfloat16)

def attention(seg_row, qkv, d_attn):
    seq, width = qkv.shape
    heads = width // (3 * D)
    full = lambda shape: pl.BlockSpec(shape, lambda i: tuple(0 for _ in shape))
    return pl.pallas_call(
        attn_kernel,
        grid=(seq // BQ,),
        in_specs=[full(seg_row.shape), full(qkv.shape), full(d_attn.shape)],
        out_specs=[full(qkv.shape), full(d_attn.shape)],
        out_shape=[jax.ShapeDtypeStruct(qkv.shape, jnp.bfloat16), jax.ShapeDtypeStruct(d_attn.shape, jnp.bfloat16)],
        scratch_shapes=[
            pltpu.SMEM((2,), jnp.int32),
            pltpu.VMEM((heads, BQ, seq), jnp.float32),
            pltpu.VMEM((heads, BQ, seq), jnp.float32),
            pltpu.VMEM((heads, seq, D), jnp.float32),
            pltpu.VMEM((heads, seq, D), jnp.float32),
        ],
        compiler_params=pltpu.CompilerParams(dimension_semantics=("arbitrary",), vmem_limit_bytes=60 * 1024 * 1024),
    )(seg_row, qkv, d_attn)


MESH = pl.DeviceIdType.MESH
NC = 2


def place():
    y = lax.axis_index('col')
    r = lax.axis_index('row')
    c = lax.rem(r, 2)
    r_s = r + 1 - 2 * c
    return y, r, c, r_s, lax.rem(r + 2, 4), lax.rem(r_s + 2, 4)


def mult(i, n):
    return pl.multiple_of(i * n, n)


def gather_kernel(x_ref, w_ref, wo_ref, seg_ref, dy_ref, xg, dyg, wg, segg, qkv_ref, do_ref,
                  stage, wstage, wh, woh, tok, ssem, rsem, lsem):
    y, r, c, r_s, r_x, r_xs = place()
    x = r // 2
    t_loc, h_loc = x_ref.shape
    hw = wh.shape[1]
    ow = woh.shape[0]
    sib, xn, yn = {'row': r_s}, {'row': r_x}, {'col': 1 - y}
    ct = t_loc // NC
    started = []

    def send(i, src, dst, dev):
        cp = pltpu.make_async_remote_copy(src, dst, ssem.at[i], rsem.at[i], device_id=dev, device_id_type=MESH)
        cp.start()
        started.append(cp)

    def recv(i, dst):
        pltpu.make_async_remote_copy(dst, dst, ssem.at[i], rsem.at[i], device_id=sib, device_id_type=MESH).wait_recv()

    def local(i, src, dst):
        cp = pltpu.make_async_copy(src, dst, lsem.at[i])
        cp.start()
        return cp

    def slot(g, yy, rr, j):
        return g.at[pl.ds(pl.multiple_of(rr * t_loc + j * ct, ct), ct), pl.ds(mult(yy, h_loc), h_loc)]

    def own(a, j):
        return a.at[pl.ds(j * ct, ct)]

    def tid(base, kind, j):
        return base + kind * NC + j

    XB, YB = 0, 7 * NC
    WB = 14 * NC
    WOB = WB + 12
    SGB = WOB + 2

    def got_from(kind):
        return ((y, r_s), (y, r_x), (1 - y, r), (y, r_xs), (1 - y, r_x), (1 - y, r_s), (1 - y, r_xs))[kind]

    def send_own(a, g, base, kind, dev):
        for j in range(NC):
            send(tid(base, kind, j), own(a, j), slot(g, y, r, j), dev)

    def forward(g, base, kind_in, outs, j):
        yy, rr = got_from(kind_in)
        recv(tid(base, kind_in, j), slot(g, yy, rr, j))
        for kind_out, dev in outs:
            send(tid(base, kind_out, j), slot(g, yy, rr, j), slot(g, yy, rr, j), dev)

    def take(g, base, kind):
        yy, rr = got_from(kind)
        for j in range(NC):
            recv(tid(base, kind, j), slot(g, yy, rr, j))

    def wslot(rr, q):
        return wg.at[pl.ds(mult(rr, t_loc), t_loc), pl.ds(mult(q, hw), hw)]

    def wq(t, xx):
        return lax.rem(2 * xx + t, 4)

    def w_own(t, kind, xx, dev):
        q = wq(t, xx)
        send(WB + 4 * kind + t, w_ref.at[:, pl.ds(mult(q, hw), hw)], wslot(r, q), dev)

    def w_forward(t):
        q = wq(t, x)
        recv(WB + 4 + t, wslot(r_x, q))
        send(WB + 8 + t, wslot(r_x, q), wslot(r_x, q), sib)

    for i, (rr, dev) in enumerate(((r_s, sib), (r_x, xn), (r_xs, {'row': r_xs}))):
        send(SGB + i, seg_ref, segg.at[r], dev)
    send_own(x_ref, xg, XB, 1, xn)
    send_own(x_ref, xg, XB, 2, yn)
    for t in range(2):
        w_own(t, 1, 1 - x, xn)
    send_own(x_ref, xg, XB, 0, sib)
    for t in range(4):
        w_own(t, 0, x, sib)
    for k in range(2):
        row_to = 2 * c + k
        src = wo_ref.at[pl.ds(k * ow, ow)]
        dst = woh.at[:, pl.ds(mult(y, h_loc), h_loc)]
        mine = (x == y) & (row_to == r)

        @pl.when(mine)
        def _():
            pltpu.make_async_copy(src, dst, lsem.at[0]).start()

        @pl.when(jnp.logical_not(mine))
        def _():
            pltpu.make_async_remote_copy(src, dst, ssem.at[WOB + k], rsem.at[WOB + y],
                                         device_id={'col': x, 'row': row_to}, device_id_type=MESH).start()
    send_own(dy_ref, dyg, YB, 1, xn)
    send_own(dy_ref, dyg, YB, 0, sib)
    for t in range(2, 4):
        w_own(t, 1, 1 - x, xn)

    a = local(1, x_ref, stage.at[0])
    b = local(2, dy_ref, stage.at[1])
    d = local(3, w_ref, wstage)
    sg = local(4, seg_ref, segg.at[r])
    own_slot = lambda g: g.at[pl.ds(mult(r, t_loc), t_loc), pl.ds(mult(y, h_loc), h_loc)]
    a.wait()
    a = local(1, stage.at[0], own_slot(xg))
    b.wait()
    b = local(2, stage.at[1], own_slot(dyg))
    d.wait()
    d = local(3, wstage, wg.at[pl.ds(mult(r, t_loc), t_loc)])
    wh[pl.ds(mult(r, t_loc), t_loc), :] = wstage[:, pl.ds(mult(r, hw), hw)]

    for j in range(NC):
        forward(xg, XB, 1, ((4, yn), (3, sib)), j)
        forward(xg, XB, 2, ((5, sib),), j)
    send_own(dy_ref, dyg, YB, 2, yn)
    for j in range(NC):
        w_forward(j)
        forward(xg, XB, 4, ((6, sib),), j)
    a.wait()
    b.wait()
    d.wait()
    sg.wait()

    for t in range(4):
        recv(WB + t, wslot(r_s, wq(t, x)))
    for t in range(2):
        recv(WB + 8 + t, wslot(r_xs, wq(t, x)))
    loads = []
    for i, rr in enumerate((r_s, r_x, r_xs)):
        loads.append(local(5 + i, wslot(rr, r), wh.at[pl.ds(mult(rr, t_loc), t_loc)]))
    for kind in (0, 3, 5, 6):
        take(xg, XB, kind)

    def load_tok(g, rr, s):
        return local(8 + s, g.at[pl.ds(mult(rr, t_loc), t_loc)], tok.at[s])

    blocks = (r, r_s, r_x, r_xs)
    nxt = load_tok(xg, blocks[0], 0)
    for cp in loads:
        cp.wait()
    for i in range(4):
        nxt.wait()
        if i < 3:
            nxt = load_tok(xg, blocks[i + 1], (i + 1) % 2)
        rows = pl.ds(mult(blocks[i], t_loc), t_loc)
        for n in range(hw // 256):
            cols = slice(256 * n, 256 * n + 256)
            qkv_ref[rows, cols] = jnp.dot(tok[i % 2], wh[:, cols], preferred_element_type=jnp.float32).astype(jnp.bfloat16)

    for j in range(NC):
        forward(dyg, YB, 1, ((4, yn), (3, sib)), j)
        forward(dyg, YB, 2, ((5, sib),), j)
    for yy in range(2):
        piece = woh.at[:, pl.ds(yy * h_loc, h_loc)]
        mine = (y == yy) & (2 * y + x == r)

        @pl.when(mine)
        def _():
            pltpu.make_async_copy(wo_ref.at[pl.ds(0, ow)], piece, lsem.at[0]).wait()

        @pl.when(jnp.logical_not(mine))
        def _():
            recv(WOB + yy, piece)
    for kind in (0, 5):
        take(dyg, YB, kind)

    def d_out(i, s):
        rows = pl.ds(mult(blocks[i], t_loc), t_loc)
        do_ref[rows, :] = lax.dot_general(tok[s], woh[...], NT, preferred_element_type=jnp.float32).astype(jnp.bfloat16)

    one = load_tok(dyg, r, 0)
    two = load_tok(dyg, r_s, 1)
    one.wait()
    d_out(0, 0)
    two.wait()
    d_out(1, 1)
    for j in range(NC):
        forward(dyg, YB, 4, ((6, sib),), j)
    w_forward(2)
    take(dyg, YB, 3)
    one = load_tok(dyg, r_x, 0)
    take(dyg, YB, 6)
    two = load_tok(dyg, r_xs, 1)
    one.wait()
    d_out(2, 0)
    two.wait()
    d_out(3, 1)
    w_forward(3)
    for t in range(2, 4):
        recv(WB + 8 + t, wslot(r_xs, wq(t, x)))
    for i, rr in enumerate((r_s, r_x, r_xs)):
        recv(SGB + i, segg.at[rr])
    for cp in started:
        cp.wait_send()
    for k in range(2):
        mine = (x == y) & (2 * c + k == r)

        @pl.when(jnp.logical_not(mine))
        def _():
            pltpu.make_async_remote_copy(wo_ref.at[pl.ds(0, ow)], woh.at[:, pl.ds(0, h_loc)], ssem.at[WOB + k], rsem.at[WOB + k],
                                         device_id=sib, device_id_type=MESH).wait_send()


def gather_all(x_blk, w_blk, wo_blk, seg_blk, dy_blk):
    t_loc, h_loc = x_blk.shape
    w_loc = w_blk.shape[1]
    seq, hid = 4 * t_loc, 2 * h_loc
    hw, ow = w_loc // 4, w_loc // 12
    bf = jnp.bfloat16
    hbm = pl.BlockSpec(memory_space=pl.ANY)
    vmem = pl.BlockSpec(memory_space=pltpu.VMEM)
    n_sem = 14 * NC + 12 + 2 + 3
    return pl.pallas_call(
        gather_kernel,
        in_specs=[hbm] * 5,
        out_specs=[hbm] * 4 + [vmem] * 2,
        out_shape=[
            jax.ShapeDtypeStruct((seq, hid), bf), jax.ShapeDtypeStruct((seq, hid), bf),
            jax.ShapeDtypeStruct((hid, w_loc), bf), jax.ShapeDtypeStruct((4,) + seg_blk.shape, jnp.int32),
            jax.ShapeDtypeStruct((seq, hw), bf), jax.ShapeDtypeStruct((seq, ow), bf),
        ],
        scratch_shapes=[
            pltpu.VMEM((2, t_loc, h_loc), bf), pltpu.VMEM((t_loc, w_loc), bf), pltpu.VMEM((hid, hw), bf),
            pltpu.VMEM((ow, hid), bf), pltpu.VMEM((2, t_loc, hid), bf),
            pltpu.SemaphoreType.DMA((n_sem,)), pltpu.SemaphoreType.DMA((n_sem,)), pltpu.SemaphoreType.DMA((10,)),
        ],
        compiler_params=pltpu.CompilerParams(has_side_effects=True, vmem_limit_bytes=48 * 1024 * 1024),
        name='gather_project',
    )(x_blk, w_blk, wo_blk, seg_blk, dy_blk)


NJ = 2


def scatter_kernel(xg, dyg, wg, dqkv_ref, o_ref, dx_out, dw_out, dwo_out,
                   dtok, dq_v, w_v, o_v, col_v, dw_v, dwo_v, px_send, px_recv, px_own, dx_v, ssem, rsem, lsem):
    y, r, c, r_s, r_x, r_xs = place()
    x = r // 2
    t_loc, feat = dtok.shape
    hw = dq_v.shape[1]
    ow = o_v.shape[1]
    seq = dq_v.shape[0]
    h_loc = dx_v.shape[1]
    bt = t_loc // NJ
    f32 = jnp.float32
    others = (r_s, r_x, r_xs)
    started = []
    DQ, DW, DWO, PX = 0, 3 * NJ, 3 * NJ + 3, 3 * NJ + 5

    def copy(i, k, src, dst, dev):
        return pltpu.make_async_remote_copy(src, dst, ssem.at[i], rsem.at[k], device_id=dev, device_id_type=MESH)

    def send(i, src, dst, dev):
        cp = copy(i, i, src, dst, dev)
        cp.start()
        started.append(cp)

    def recv(i, dst):
        copy(i, i, dst, dst, {'row': r_s}).wait_recv()

    def local(i, src, dst):
        cp = pltpu.make_async_copy(src, dst, lsem.at[i])
        cp.start()
        return cp

    def tok_slot(rr, j):
        return dtok.at[pl.ds(j * bt, bt), pl.ds(mult(rr, hw), hw)]

    def dw_slot(rr):
        return dw_out.at[:, pl.ds(mult(rr, hw), hw)]

    for j in range(NJ):
        for k in (1, 2, 0):
            rr = others[k]
            src = dqkv_ref.at[pl.ds(pl.multiple_of(rr * t_loc + j * bt, bt), bt)]
            send(DQ + 3 * j + k, src, tok_slot(r, j), {'row': rr})
    own_tok = local(0, dqkv_ref.at[pl.ds(mult(r, t_loc), t_loc)], dtok.at[:, pl.ds(mult(r, hw), hw)])
    ld_o = local(1, o_ref, o_v)
    ld_dy = [local(2 + s, dyg.at[:, pl.ds(512 * s, 512)], col_v.at[s]) for s in range(2)]
    ld_dq = local(4, dqkv_ref, dq_v)
    ld_w = local(5, wg, w_v)

    ld_o.wait()
    ld_x = [None, None]
    blocks = (r_x, r_xs, r_s, r)
    for s in range(4):
        ld_dy[s].wait()
        dwo_v[:, 512 * s:512 * s + 512] = lax.dot_general(o_v[...], col_v[s % 2], TN, preferred_element_type=f32).astype(jnp.bfloat16)
        if s < 2:
            ld_dy.append(local(2 + s, dyg.at[:, pl.ds(512 * s + 1024, 512)], col_v.at[s]))
        else:
            ld_x[s - 2] = local(2 + s - 2, xg.at[:, pl.ds(mult(blocks[s - 2], t_loc), t_loc)], col_v.at[s - 2])
    row_to = 2 * y + x
    for k in range(2):
        src = dwo_v.at[:, pl.ds(k * h_loc, h_loc)]
        dst = dwo_out.at[pl.ds(mult(c, ow), ow)]
        mine = (y == k) & (row_to == r)

        @pl.when(mine)
        def _():
            pltpu.make_async_copy(src, dst, lsem.at[6]).start()

        @pl.when(jnp.logical_not(mine))
        def _():
            copy(DWO + k, DWO + c, src, dst, {'col': k, 'row': row_to}).start()

    ld_dq.wait()

    def d_w(i):
        s = i % 2
        ld_x[s].wait()
        dw_v[i] = lax.dot_general(col_v[s], dq_v[...], TN, preferred_element_type=f32).astype(jnp.bfloat16)
        if i < 2:
            ld_x[s] = local(2 + s, xg.at[:, pl.ds(mult(blocks[i + 2], t_loc), t_loc)], col_v.at[s])

    def d_x(j, half, dst):
        for n in range(h_loc // 256):
            rows = pl.ds(pl.multiple_of(half * h_loc + 256 * n, 256), 256)
            dst[pl.ds(j * bt, bt), 256 * n:256 * n + 256] = lax.dot_general(
                dtok[pl.ds(j * bt, bt), :], w_v[rows, :], NT, preferred_element_type=f32)

    def d_x_send(j):
        for k in range(3):
            recv(DQ + 3 * j + k, tok_slot(others[k], j))
        d_x(j, 1 - y, px_send)
        send(PX + j, px_send.at[pl.ds(j * bt, bt)], px_recv.at[pl.ds(j * bt, bt)], {'col': 1 - y})

    d_w(0)
    send(DW + 1, dw_v.at[0], dw_slot(r), {'row': r_x})
    d_w(1)
    send(DW + 2, dw_v.at[1], dw_slot(r), {'row': r_xs})
    ld_w.wait()
    own_tok.wait()
    d_x_send(0)
    d_w(2)
    send(DW + 0, dw_v.at[2], dw_slot(r), {'row': r_s})
    d_x(0, y, px_own)
    d_x_send(1)
    d_w(3)
    own_dw = local(0, dw_v.at[3], dw_slot(r))
    d_x(1, y, px_own)
    outs = []
    for j in range(NJ):
        rows = pl.ds(j * bt, bt)
        recv(PX + j, px_recv.at[rows])
        dx_v[rows, :] = (px_own[rows, :] + px_recv[rows, :]).astype(jnp.bfloat16)
        outs.append(local(2 + j, dx_v.at[rows], dx_out.at[rows]))
    own_dw.wait()
    for k in range(3):
        recv(DW + k, dw_slot(others[k]))
    for k in range(2):
        piece = dwo_out.at[pl.ds(k * ow, ow)]
        mine = (r // 2 == y) & (2 * lax.rem(r, 2) + k == r)

        @pl.when(mine)
        def _():
            pltpu.make_async_copy(dwo_v.at[:, pl.ds(0, h_loc)], piece, lsem.at[6]).wait()

        @pl.when(jnp.logical_not(mine))
        def _():
            recv(DWO + k, piece)
    for cp in outs:
        cp.wait()
    for cp in started:
        cp.wait_send()
    for k in range(2):
        @pl.when(jnp.logical_not((y == k) & (row_to == r)))
        def _():
            copy(DWO + k, DWO + k, dwo_v.at[:, pl.ds(0, h_loc)], dwo_out.at[pl.ds(0, ow)], {'row': r_s}).wait_send()


def scatter_all(x_all, dy_all, w_col, d_qkv, attn_out, blocks):
    bf, f32 = jnp.bfloat16, jnp.float32
    t_loc, h_loc = blocks[0].shape
    seq, hw = d_qkv.shape
    ow = attn_out.shape[1]
    hid, feat = w_col.shape
    hbm = pl.BlockSpec(memory_space=pl.ANY)
    n_sem = 4 * NJ + 5
    return pl.pallas_call(
        scatter_kernel,
        in_specs=[hbm] * 5,
        out_specs=[hbm] * 3,
        out_shape=[jax.ShapeDtypeStruct(b.shape, bf) for b in blocks],
        scratch_shapes=[
            pltpu.VMEM((t_loc, feat), bf), pltpu.VMEM((seq, hw), bf), pltpu.VMEM((hid, feat), bf), pltpu.VMEM((seq, ow), bf),
            pltpu.VMEM((2, seq, t_loc), bf), pltpu.VMEM((4, t_loc, hw), bf), pltpu.VMEM((ow, hid), bf),
            pltpu.VMEM((t_loc, h_loc), f32), pltpu.VMEM((t_loc, h_loc), f32), pltpu.VMEM((t_loc, h_loc), f32),
            pltpu.VMEM((t_loc, h_loc), bf),
            pltpu.SemaphoreType.DMA((n_sem,)), pltpu.SemaphoreType.DMA((n_sem,)), pltpu.SemaphoreType.DMA((7,)),
        ],
        compiler_params=pltpu.CompilerParams(has_side_effects=True, vmem_limit_bytes=60 * 1024 * 1024),
        name='project_scatter',
    )(x_all, dy_all, w_col, d_qkv, attn_out)


def solution(mesh):
    tok_spec = P(('dp', 'row'), 'col')
    mat_spec = P('row', 'col')
    seg_spec = P(('dp', 'row'))

    def grad_step(x_blk, wqkv_blk, wout_blk, seg_blk, dy_blk):
        x_all, dy_all, w_col, seg_all, qkv, d_attn = gather_all(x_blk, wqkv_blk, wout_blk, seg_blk.reshape(4, -1), dy_blk)
        d_qkv, attn_out = attention(seg_all, qkv, d_attn)
        grad_x, grad_wqkv, grad_wout = scatter_all(x_all, dy_all, w_col, d_qkv, attn_out, (x_blk, wqkv_blk, wout_blk))
        return grad_x, grad_wqkv, grad_wout

    return jax.shard_map(grad_step, mesh=mesh, in_specs=(tok_spec, mat_spec, mat_spec, seg_spec, tok_spec), out_specs=(tok_spec, tok_spec, tok_spec), check_vma=False)
```

```python
import jax
import jax.numpy as jnp
from jax import lax
from jax.experimental import pallas as pl
from jax.experimental.pallas import tpu as pltpu
from jax.sharding import PartitionSpec as P

NT = (((1,), (1,)), ((), ()))
TN = (((0,), (0,)), ((), ()))
BK = 512
D = 128
LOW = -3.0e38
VMEM_LIMIT = 66_000_000


def attention_block(q0, bq, c1, c2, qkv_v, do_v, p_scr, dp_scr, m_scr, kt, vt, dk_acc, dv_acc, dqkv_v, o_v):
    seq = qkv_v.shape[0]
    heads = do_v.shape[1] // D
    scale = D ** -0.5
    to_exp2 = scale * 1.4426950408889634
    f32 = jnp.float32
    rows = pl.ds(q0, bq)
    iq = q0 + lax.broadcasted_iota(jnp.int32, (1, bq), 1)
    q_doc = (iq >= c1).astype(jnp.int32) + (iq >= c2).astype(jnp.int32)
    q = [qkv_v[rows, 3 * D * h:3 * D * h + D] for h in range(heads)]
    do = [do_v[rows, D * h:D * h + D] for h in range(heads)]

    def first(kb, carry):
        k0 = pl.multiple_of(kb * BK, BK)
        keys = pl.ds(k0, BK)
        ik = k0 + lax.broadcasted_iota(jnp.int32, (BK, 1), 0)
        k_doc = (ik >= c1).astype(jnp.int32) + (ik >= c2).astype(jnp.int32)
        same = q_doc == k_doc
        out = []
        for h in range(heads):
            m, l, dd = carry[h]
            k = qkv_v[keys, 3 * D * h + D:3 * D * h + 2 * D]
            v = qkv_v[keys, 3 * D * h + 2 * D:3 * D * h + 3 * D]
            s = lax.dot_general(k, q[h], NT, preferred_element_type=f32)
            s = jnp.where(same, s, LOW)
            dp = lax.dot_general(v, do[h], NT, preferred_element_type=f32)
            dp_scr[h, keys, :] = dp
            m_new = jnp.maximum(m, jnp.max(s, axis=0, keepdims=True))
            p = jnp.exp2((s - m_new) * to_exp2)
            p_scr[h, keys, :] = p
            m_scr[kb, h] = m_new
            alpha = jnp.exp2((m - m_new) * to_exp2)
            out.append((m_new, alpha * l + jnp.sum(p, axis=0, keepdims=True), alpha * dd + jnp.sum(p * dp, axis=0, keepdims=True)))
        return tuple(out)

    zero = jnp.zeros((1, bq), f32)
    low = jnp.full((1, bq), LOW, f32)
    mld = lax.fori_loop(0, seq // BK, first, tuple((low, zero, zero) for _ in range(heads)))
    inv = [1.0 / mld[h][1] for h in range(heads)]
    row_dot = [mld[h][2] * inv[h] for h in range(heads)]

    def second(kb, acc):
        keys = pl.ds(pl.multiple_of(kb * BK, BK), BK)
        out = []
        for h in range(heads):
            f = jnp.exp2((m_scr[kb, h] - mld[h][0]) * to_exp2) * inv[h]
            p = p_scr[h, keys, :]
            p_bf = (p * f).astype(jnp.bfloat16)
            ds = ((p * (f * scale)) * (dp_scr[h, keys, :] - row_dot[h])).astype(jnp.bfloat16)
            o, dq = acc[h]
            o = o + jnp.dot(vt[h, :, keys], p_bf, preferred_element_type=f32)
            dq = dq + jnp.dot(kt[h, :, keys], ds, preferred_element_type=f32)
            dk_acc[h, keys, :] += jnp.dot(ds, q[h], preferred_element_type=f32)
            dv_acc[h, keys, :] += jnp.dot(p_bf, do[h], preferred_element_type=f32)
            out.append((o, dq))
        return tuple(out)

    zacc = jnp.zeros((D, bq), f32)
    acc = lax.fori_loop(0, seq // BK, second, tuple((zacc, zacc) for _ in range(heads)))
    for h in range(heads):
        o_v[rows, D * h:D * h + D] = acc[h][0].T.astype(jnp.bfloat16)
        dqkv_v[rows, 3 * D * h:3 * D * h + D] = acc[h][1].T.astype(jnp.bfloat16)


MESH = pl.DeviceIdType.MESH
NC = 2


def place():
    y = lax.axis_index('col')
    r = lax.axis_index('row')
    c = lax.rem(r, 2)
    r_s = r + 1 - 2 * c
    return y, r, c, r_s, lax.rem(r + 2, 4), lax.rem(r_s + 2, 4)


def mult(i, n):
    return pl.multiple_of(i * n, n)


def forward_kernel(x_ref, w_ref, wo_ref, seg_ref, dy_ref, xg, dyg, wg, segg, dqkv_ref, o_ref,
                   stage, wstage, wh, woh, tok, qkv_v, do_v, seg_v, p_scr, dp_scr, m_scr, kt, vt, dk_acc, dv_acc, dqkv_v, o_v,
                   ssem, rsem, lsem):
    y, r, c, r_s, r_x, r_xs = place()
    x = r // 2
    t_loc, h_loc = x_ref.shape
    heads = woh.shape[0] // D
    hw = wh.shape[1]
    ow = woh.shape[0]
    sib, xn, yn = {'row': r_s}, {'row': r_x}, {'col': 1 - y}
    ct = t_loc // NC
    started = []

    def send(i, src, dst, dev):
        cp = pltpu.make_async_remote_copy(src, dst, ssem.at[i], rsem.at[i], device_id=dev, device_id_type=MESH)
        cp.start()
        started.append(cp)

    def recv(i, dst):
        pltpu.make_async_remote_copy(dst, dst, ssem.at[i], rsem.at[i], device_id=sib, device_id_type=MESH).wait_recv()

    def local(i, src, dst):
        cp = pltpu.make_async_copy(src, dst, lsem.at[i])
        cp.start()
        return cp

    def slot(g, yy, rr, j):
        return g.at[pl.ds(pl.multiple_of(rr * t_loc + j * ct, ct), ct), pl.ds(mult(yy, h_loc), h_loc)]

    def own(a, j):
        return a.at[pl.ds(j * ct, ct)]

    def tid(base, kind, j):
        return base + kind * NC + j

    XB, YB = 0, 7 * NC
    WB = 14 * NC
    WOB = WB + 12
    SGB = WOB + 2

    def got_from(kind):
        return ((y, r_s), (y, r_x), (1 - y, r), (y, r_xs), (1 - y, r_x), (1 - y, r_s), (1 - y, r_xs))[kind]

    def send_own(a, g, base, kind, dev):
        for j in range(NC):
            send(tid(base, kind, j), own(a, j), slot(g, y, r, j), dev)

    def forward(g, base, kind_in, outs, j):
        yy, rr = got_from(kind_in)
        recv(tid(base, kind_in, j), slot(g, yy, rr, j))
        for kind_out, dev in outs:
            send(tid(base, kind_out, j), slot(g, yy, rr, j), slot(g, yy, rr, j), dev)

    def take(g, base, kind):
        yy, rr = got_from(kind)
        for j in range(NC):
            recv(tid(base, kind, j), slot(g, yy, rr, j))

    def wslot(rr, q):
        return wg.at[pl.ds(mult(rr, t_loc), t_loc), pl.ds(mult(q, hw), hw)]

    def wq(t, xx):
        return lax.rem(2 * xx + t, 4)

    def w_own(t, kind, xx, dev):
        q = wq(t, xx)
        send(WB + 4 * kind + t, w_ref.at[:, pl.ds(mult(q, hw), hw)], wslot(r, q), dev)

    def w_forward(t):
        q = wq(t, x)
        recv(WB + 4 + t, wslot(r_x, q))
        send(WB + 8 + t, wslot(r_x, q), wslot(r_x, q), sib)

    for i, (rr, dev) in enumerate(((r_s, sib), (r_x, xn), (r_xs, {'row': r_xs}))):
        send(SGB + i, seg_ref, segg.at[r], dev)
    send_own(x_ref, xg, XB, 1, xn)
    send_own(x_ref, xg, XB, 2, yn)
    for t in range(2):
        w_own(t, 1, 1 - x, xn)
    send_own(x_ref, xg, XB, 0, sib)
    for t in range(4):
        w_own(t, 0, x, sib)
    for k in range(2):
        row_to = 2 * c + k
        src = wo_ref.at[pl.ds(k * ow, ow)]
        dst = woh.at[:, pl.ds(mult(y, h_loc), h_loc)]
        mine = (x == y) & (row_to == r)

        @pl.when(mine)
        def _():
            pltpu.make_async_copy(src, dst, lsem.at[0]).start()

        @pl.when(jnp.logical_not(mine))
        def _():
            pltpu.make_async_remote_copy(src, dst, ssem.at[WOB + k], rsem.at[WOB + y],
                                         device_id={'col': x, 'row': row_to}, device_id_type=MESH).start()
    send_own(dy_ref, dyg, YB, 1, xn)
    send_own(dy_ref, dyg, YB, 0, sib)
    for t in range(2, 4):
        w_own(t, 1, 1 - x, xn)

    a = local(1, x_ref, stage.at[0])
    b = local(2, dy_ref, stage.at[1])
    d = local(3, w_ref, wstage)
    sg = local(4, seg_ref, segg.at[r])
    own_slot = lambda g: g.at[pl.ds(mult(r, t_loc), t_loc), pl.ds(mult(y, h_loc), h_loc)]
    a.wait()
    a = local(1, stage.at[0], own_slot(xg))
    b.wait()
    b = local(2, stage.at[1], own_slot(dyg))
    d.wait()
    d = local(3, wstage, wg.at[pl.ds(mult(r, t_loc), t_loc)])
    wh[pl.ds(mult(r, t_loc), t_loc), :] = wstage[:, pl.ds(mult(r, hw), hw)]

    for j in range(NC):
        forward(xg, XB, 1, ((4, yn), (3, sib)), j)
        forward(xg, XB, 2, ((5, sib),), j)
    send_own(dy_ref, dyg, YB, 2, yn)
    for j in range(NC):
        w_forward(j)
        forward(xg, XB, 4, ((6, sib),), j)
    a.wait()
    b.wait()
    d.wait()
    sg.wait()

    for t in range(4):
        recv(WB + t, wslot(r_s, wq(t, x)))
    for t in range(2):
        recv(WB + 8 + t, wslot(r_xs, wq(t, x)))
    loads = []
    for i, rr in enumerate((r_s, r_x, r_xs)):
        loads.append(local(5 + i, wslot(rr, r), wh.at[pl.ds(mult(rr, t_loc), t_loc)]))
    for kind in (0, 3, 5, 6):
        take(xg, XB, kind)

    def load_tok(g, rr, s):
        return local(8 + s, g.at[pl.ds(mult(rr, t_loc), t_loc)], tok.at[s])

    blocks = (r, r_s, r_x, r_xs)
    nxt = load_tok(xg, blocks[0], 0)
    for cp in loads:
        cp.wait()
    for i in range(4):
        nxt.wait()
        if i < 3:
            nxt = load_tok(xg, blocks[i + 1], (i + 1) % 2)
        rows = pl.ds(mult(blocks[i], t_loc), t_loc)
        for n in range(hw // 256):
            cols = slice(256 * n, 256 * n + 256)
            qkv_v[rows, cols] = jnp.dot(tok[i % 2], wh[:, cols], preferred_element_type=jnp.float32).astype(jnp.bfloat16)

        for h in range(heads):
            kt[h, :, rows] = qkv_v[rows, 3 * D * h + D:3 * D * h + 2 * D].T
            vt[h, :, rows] = qkv_v[rows, 3 * D * h + 2 * D:3 * D * h + 3 * D].T

    for i, rr in enumerate((r_s, r_x, r_xs)):
        recv(SGB + i, segg.at[rr])
    local(4, segg, seg_v).wait()
    c1 = jnp.sum((seg_v[...] < 1).astype(jnp.int32))
    c2 = jnp.sum((seg_v[...] < 2).astype(jnp.int32))
    dk_acc[...] = jnp.zeros_like(dk_acc)
    dv_acc[...] = jnp.zeros_like(dv_acc)

    for j in range(NC):
        forward(dyg, YB, 1, ((4, yn), (3, sib)), j)
        forward(dyg, YB, 2, ((5, sib),), j)
    for yy in range(2):
        piece = woh.at[:, pl.ds(yy * h_loc, h_loc)]
        mine = (y == yy) & (2 * y + x == r)

        @pl.when(mine)
        def _():
            pltpu.make_async_copy(wo_ref.at[pl.ds(0, ow)], piece, lsem.at[0]).wait()

        @pl.when(jnp.logical_not(mine))
        def _():
            recv(WOB + yy, piece)
    for kind in (0, 5):
        take(dyg, YB, kind)

    def d_out(i, s):
        rows = pl.ds(mult(blocks[i], t_loc), t_loc)
        do_v[rows, :] = lax.dot_general(tok[s], woh[...], NT, preferred_element_type=jnp.float32).astype(jnp.bfloat16)

    def attend(i):
        q0 = mult(blocks[i], t_loc)
        attention_block(q0, t_loc, c1, c2, qkv_v, do_v, p_scr, dp_scr, m_scr, kt, vt, dk_acc, dv_acc, dqkv_v, o_v)

    one = load_tok(dyg, r, 0)
    two = load_tok(dyg, r_s, 1)
    one.wait()
    d_out(0, 0)
    attend(0)
    for j in range(NC):
        forward(dyg, YB, 4, ((6, sib),), j)
    two.wait()
    d_out(1, 1)
    attend(1)
    w_forward(2)
    take(dyg, YB, 3)
    one = load_tok(dyg, r_x, 0)
    take(dyg, YB, 6)
    two = load_tok(dyg, r_xs, 1)
    one.wait()
    d_out(2, 0)
    attend(2)
    two.wait()
    d_out(3, 1)
    attend(3)
    w_forward(3)
    for t in range(2, 4):
        recv(WB + 8 + t, wslot(r_xs, wq(t, x)))
    for h in range(heads):
        dqkv_v[:, 3 * D * h + D:3 * D * h + 2 * D] = dk_acc[h].astype(jnp.bfloat16)
        dqkv_v[:, 3 * D * h + 2 * D:3 * D * h + 3 * D] = dv_acc[h].astype(jnp.bfloat16)
    out_a = local(0, dqkv_v, dqkv_ref)
    out_b = local(1, o_v, o_ref)
    out_a.wait()
    out_b.wait()
    for cp in started:
        cp.wait_send()
    for k in range(2):
        mine = (x == y) & (2 * c + k == r)

        @pl.when(jnp.logical_not(mine))
        def _():
            pltpu.make_async_remote_copy(wo_ref.at[pl.ds(0, ow)], woh.at[:, pl.ds(0, h_loc)], ssem.at[WOB + k], rsem.at[WOB + k],
                                         device_id=sib, device_id_type=MESH).wait_send()


def forward_all(x_blk, w_blk, wo_blk, seg_blk, dy_blk):
    t_loc, h_loc = x_blk.shape
    w_loc = w_blk.shape[1]
    seq, hid = 4 * t_loc, 2 * h_loc
    hw, ow = w_loc // 4, w_loc // 12
    heads = ow // D
    bf, f32 = jnp.bfloat16, jnp.float32
    hbm = pl.BlockSpec(memory_space=pl.ANY)
    n_sem = 14 * NC + 12 + 2 + 3
    seg_shape = (4,) + seg_blk.shape
    return pl.pallas_call(
        forward_kernel,
        in_specs=[hbm] * 5,
        out_specs=[hbm] * 6,
        out_shape=[
            jax.ShapeDtypeStruct((seq, hid), bf), jax.ShapeDtypeStruct((seq, hid), bf),
            jax.ShapeDtypeStruct((hid, w_loc), bf), jax.ShapeDtypeStruct(seg_shape, jnp.int32),
            jax.ShapeDtypeStruct((seq, hw), bf), jax.ShapeDtypeStruct((seq, ow), bf),
        ],
        scratch_shapes=[
            pltpu.VMEM((2, t_loc, h_loc), bf), pltpu.VMEM((t_loc, w_loc), bf), pltpu.VMEM((hid, hw), bf),
            pltpu.VMEM((ow, hid), bf), pltpu.VMEM((2, t_loc, hid), bf),
            pltpu.VMEM((seq, hw), bf), pltpu.VMEM((seq, ow), bf), pltpu.VMEM(seg_shape, jnp.int32),
            pltpu.VMEM((heads, seq, t_loc), f32), pltpu.VMEM((heads, seq, t_loc), f32),
            pltpu.VMEM((seq // BK, heads, 1, t_loc), f32),
            pltpu.VMEM((heads, D, seq), bf), pltpu.VMEM((heads, D, seq), bf),
            pltpu.VMEM((heads, seq, D), f32), pltpu.VMEM((heads, seq, D), f32),
            pltpu.VMEM((seq, hw), bf), pltpu.VMEM((seq, ow), bf),
            pltpu.SemaphoreType.DMA((n_sem,)), pltpu.SemaphoreType.DMA((n_sem,)), pltpu.SemaphoreType.DMA((10,)),
        ],
        compiler_params=pltpu.CompilerParams(has_side_effects=True, vmem_limit_bytes=VMEM_LIMIT),
        name='gather_attend',
    )(x_blk, w_blk, wo_blk, seg_blk, dy_blk)


NJ = 2


def scatter_kernel(xg, dyg, wg, dqkv_ref, o_ref, dx_out, dw_out, dwo_out,
                   dtok, dq_v, w_v, o_v, col_v, dw_v, dwo_v, px_send, px_recv, px_own, dx_v, ssem, rsem, lsem):
    y, r, c, r_s, r_x, r_xs = place()
    x = r // 2
    t_loc, feat = dtok.shape
    hw = dq_v.shape[1]
    ow = o_v.shape[1]
    seq = dq_v.shape[0]
    h_loc = dx_v.shape[1]
    bt = t_loc // NJ
    f32 = jnp.float32
    others = (r_s, r_x, r_xs)
    started = []
    DQ, DW, DWO, PX = 0, 3 * NJ, 3 * NJ + 3, 3 * NJ + 5

    def copy(i, k, src, dst, dev):
        return pltpu.make_async_remote_copy(src, dst, ssem.at[i], rsem.at[k], device_id=dev, device_id_type=MESH)

    def send(i, src, dst, dev):
        cp = copy(i, i, src, dst, dev)
        cp.start()
        started.append(cp)

    def recv(i, dst):
        copy(i, i, dst, dst, {'row': r_s}).wait_recv()

    def local(i, src, dst):
        cp = pltpu.make_async_copy(src, dst, lsem.at[i])
        cp.start()
        return cp

    def tok_slot(rr, j):
        return dtok.at[pl.ds(j * bt, bt), pl.ds(mult(rr, hw), hw)]

    def dw_slot(rr):
        return dw_out.at[:, pl.ds(mult(rr, hw), hw)]

    for j in range(NJ):
        for k in (1, 2, 0):
            rr = others[k]
            src = dqkv_ref.at[pl.ds(pl.multiple_of(rr * t_loc + j * bt, bt), bt)]
            send(DQ + 3 * j + k, src, tok_slot(r, j), {'row': rr})
    own_tok = local(0, dqkv_ref.at[pl.ds(mult(r, t_loc), t_loc)], dtok.at[:, pl.ds(mult(r, hw), hw)])
    ld_o = local(1, o_ref, o_v)
    ld_dy = [local(2 + s, dyg.at[:, pl.ds(512 * s, 512)], col_v.at[s]) for s in range(2)]
    ld_dq = local(4, dqkv_ref, dq_v)
    ld_w = local(5, wg, w_v)

    ld_o.wait()
    ld_x = [None, None]
    blocks = (r_x, r_xs, r_s, r)
    for s in range(4):
        ld_dy[s].wait()
        dwo_v[:, 512 * s:512 * s + 512] = lax.dot_general(o_v[...], col_v[s % 2], TN, preferred_element_type=f32).astype(jnp.bfloat16)
        if s < 2:
            ld_dy.append(local(2 + s, dyg.at[:, pl.ds(512 * s + 1024, 512)], col_v.at[s]))
        else:
            ld_x[s - 2] = local(2 + s - 2, xg.at[:, pl.ds(mult(blocks[s - 2], t_loc), t_loc)], col_v.at[s - 2])
    row_to = 2 * y + x
    for k in range(2):
        src = dwo_v.at[:, pl.ds(k * h_loc, h_loc)]
        dst = dwo_out.at[pl.ds(mult(c, ow), ow)]
        mine = (y == k) & (row_to == r)

        @pl.when(mine)
        def _():
            pltpu.make_async_copy(src, dst, lsem.at[6]).start()

        @pl.when(jnp.logical_not(mine))
        def _():
            copy(DWO + k, DWO + c, src, dst, {'col': k, 'row': row_to}).start()

    ld_dq.wait()

    def d_w(i):
        s = i % 2
        ld_x[s].wait()
        dw_v[i] = lax.dot_general(col_v[s], dq_v[...], TN, preferred_element_type=f32).astype(jnp.bfloat16)
        if i < 2:
            ld_x[s] = local(2 + s, xg.at[:, pl.ds(mult(blocks[i + 2], t_loc), t_loc)], col_v.at[s])

    def d_x(j, half, dst):
        for n in range(h_loc // 256):
            rows = pl.ds(pl.multiple_of(half * h_loc + 256 * n, 256), 256)
            dst[pl.ds(j * bt, bt), 256 * n:256 * n + 256] = lax.dot_general(
                dtok[pl.ds(j * bt, bt), :], w_v[rows, :], NT, preferred_element_type=f32)

    def d_x_send(j):
        for k in range(3):
            recv(DQ + 3 * j + k, tok_slot(others[k], j))
        d_x(j, 1 - y, px_send)
        send(PX + j, px_send.at[pl.ds(j * bt, bt)], px_recv.at[pl.ds(j * bt, bt)], {'col': 1 - y})

    d_w(0)
    send(DW + 1, dw_v.at[0], dw_slot(r), {'row': r_x})
    d_w(1)
    send(DW + 2, dw_v.at[1], dw_slot(r), {'row': r_xs})
    ld_w.wait()
    own_tok.wait()
    d_x_send(0)
    d_w(2)
    send(DW + 0, dw_v.at[2], dw_slot(r), {'row': r_s})
    d_x(0, y, px_own)
    d_x_send(1)
    d_w(3)
    own_dw = local(0, dw_v.at[3], dw_slot(r))
    d_x(1, y, px_own)
    outs = []
    for j in range(NJ):
        rows = pl.ds(j * bt, bt)
        recv(PX + j, px_recv.at[rows])
        dx_v[rows, :] = (px_own[rows, :] + px_recv[rows, :]).astype(jnp.bfloat16)
        outs.append(local(2 + j, dx_v.at[rows], dx_out.at[rows]))
    own_dw.wait()
    for k in range(3):
        recv(DW + k, dw_slot(others[k]))
    for k in range(2):
        piece = dwo_out.at[pl.ds(k * ow, ow)]
        mine = (r // 2 == y) & (2 * lax.rem(r, 2) + k == r)

        @pl.when(mine)
        def _():
            pltpu.make_async_copy(dwo_v.at[:, pl.ds(0, h_loc)], piece, lsem.at[6]).wait()

        @pl.when(jnp.logical_not(mine))
        def _():
            recv(DWO + k, piece)
    for cp in outs:
        cp.wait()
    for cp in started:
        cp.wait_send()
    for k in range(2):
        @pl.when(jnp.logical_not((y == k) & (row_to == r)))
        def _():
            copy(DWO + k, DWO + k, dwo_v.at[:, pl.ds(0, h_loc)], dwo_out.at[pl.ds(0, ow)], {'row': r_s}).wait_send()


def scatter_all(x_all, dy_all, w_col, d_qkv, attn_out, blocks):
    bf, f32 = jnp.bfloat16, jnp.float32
    t_loc, h_loc = blocks[0].shape
    seq, hw = d_qkv.shape
    ow = attn_out.shape[1]
    hid, feat = w_col.shape
    hbm = pl.BlockSpec(memory_space=pl.ANY)
    n_sem = 4 * NJ + 5
    return pl.pallas_call(
        scatter_kernel,
        in_specs=[hbm] * 5,
        out_specs=[hbm] * 3,
        out_shape=[jax.ShapeDtypeStruct(b.shape, bf) for b in blocks],
        scratch_shapes=[
            pltpu.VMEM((t_loc, feat), bf), pltpu.VMEM((seq, hw), bf), pltpu.VMEM((hid, feat), bf), pltpu.VMEM((seq, ow), bf),
            pltpu.VMEM((2, seq, t_loc), bf), pltpu.VMEM((4, t_loc, hw), bf), pltpu.VMEM((ow, hid), bf),
            pltpu.VMEM((t_loc, h_loc), f32), pltpu.VMEM((t_loc, h_loc), f32), pltpu.VMEM((t_loc, h_loc), f32),
            pltpu.VMEM((t_loc, h_loc), bf),
            pltpu.SemaphoreType.DMA((n_sem,)), pltpu.SemaphoreType.DMA((n_sem,)), pltpu.SemaphoreType.DMA((7,)),
        ],
        compiler_params=pltpu.CompilerParams(has_side_effects=True, vmem_limit_bytes=VMEM_LIMIT),
        name='project_scatter',
    )(x_all, dy_all, w_col, d_qkv, attn_out)


def solution(mesh):
    tok_spec = P(('dp', 'row'), 'col')
    mat_spec = P('row', 'col')
    seg_spec = P(('dp', 'row'))

    def grad_step(x_blk, wqkv_blk, wout_blk, seg_blk, dy_blk):
        x_all, dy_all, w_col, _, d_qkv, attn_out = forward_all(x_blk, wqkv_blk, wout_blk, seg_blk.reshape(4, -1), dy_blk)
        grad_x, grad_wqkv, grad_wout = scatter_all(x_all, dy_all, w_col, d_qkv, attn_out, (x_blk, wqkv_blk, wout_blk))
        return grad_x, grad_wqkv, grad_wout

    return jax.shard_map(grad_step, mesh=mesh, in_specs=(tok_spec, mat_spec, mat_spec, seg_spec, tok_spec), out_specs=(tok_spec, tok_spec, tok_spec), check_vma=False)
```

```python
import jax
import jax.numpy as jnp
from jax import lax
from jax.experimental import pallas as pl
from jax.experimental.pallas import tpu as pltpu
from jax.sharding import PartitionSpec as P

NT = (((1,), (1,)), ((), ()))
TN = (((0,), (0,)), ((), ()))
BK = 512
D = 128
LOW = -3.0e38
VMEM_LIMIT = 66_000_000


def attention_block(q0, bq, c1, c2, qkv_v, do_v, p_scr, dp_scr, m_scr, kt, vt, dk_acc, dv_acc, dqkv_v, o_v, between=None):
    seq = qkv_v.shape[0]
    heads = do_v.shape[1] // D
    scale = D ** -0.5
    to_exp2 = scale * 1.4426950408889634
    f32 = jnp.float32
    rows = pl.ds(q0, bq)
    iq = q0 + lax.broadcasted_iota(jnp.int32, (1, bq), 1)
    q_doc = (iq >= c1).astype(jnp.int32) + (iq >= c2).astype(jnp.int32)
    q = [qkv_v[rows, 3 * D * h:3 * D * h + D] for h in range(heads)]
    do = [do_v[rows, D * h:D * h + D] for h in range(heads)]

    def first(kb, carry):
        k0 = pl.multiple_of(kb * BK, BK)
        keys = pl.ds(k0, BK)
        ik = k0 + lax.broadcasted_iota(jnp.int32, (BK, 1), 0)
        k_doc = (ik >= c1).astype(jnp.int32) + (ik >= c2).astype(jnp.int32)
        same = q_doc == k_doc
        out = []
        for h in range(heads):
            m, l, dd = carry[h]
            k = qkv_v[keys, 3 * D * h + D:3 * D * h + 2 * D]
            v = qkv_v[keys, 3 * D * h + 2 * D:3 * D * h + 3 * D]
            s = lax.dot_general(k, q[h], NT, preferred_element_type=f32)
            s = jnp.where(same, s, LOW)
            dp = lax.dot_general(v, do[h], NT, preferred_element_type=f32)
            dp_scr[h, keys, :] = dp
            m_new = jnp.maximum(m, jnp.max(s, axis=0, keepdims=True))
            p = jnp.exp2((s - m_new) * to_exp2)
            p_scr[h, keys, :] = p
            m_scr[kb, h] = m_new
            alpha = jnp.exp2((m - m_new) * to_exp2)
            out.append((m_new, alpha * l + jnp.sum(p, axis=0, keepdims=True), alpha * dd + jnp.sum(p * dp, axis=0, keepdims=True)))
        return tuple(out)

    zero = jnp.zeros((1, bq), f32)
    low = jnp.full((1, bq), LOW, f32)
    mld = lax.fori_loop(0, seq // BK, first, tuple((low, zero, zero) for _ in range(heads)))
    if between is not None:
        between()
    inv = [1.0 / mld[h][1] for h in range(heads)]
    row_dot = [mld[h][2] * inv[h] for h in range(heads)]

    def second(kb, acc):
        keys = pl.ds(pl.multiple_of(kb * BK, BK), BK)
        out = []
        for h in range(heads):
            f = jnp.exp2((m_scr[kb, h] - mld[h][0]) * to_exp2) * inv[h]
            p = p_scr[h, keys, :]
            p_bf = (p * f).astype(jnp.bfloat16)
            ds = ((p * (f * scale)) * (dp_scr[h, keys, :] - row_dot[h])).astype(jnp.bfloat16)
            o, dq = acc[h]
            o = o + jnp.dot(vt[h, :, keys], p_bf, preferred_element_type=f32)
            dq = dq + jnp.dot(kt[h, :, keys], ds, preferred_element_type=f32)
            dk_acc[h, keys, :] += jnp.dot(ds, q[h], preferred_element_type=f32)
            dv_acc[h, keys, :] += jnp.dot(p_bf, do[h], preferred_element_type=f32)
            out.append((o, dq))
        return tuple(out)

    zacc = jnp.zeros((D, bq), f32)
    acc = lax.fori_loop(0, seq // BK, second, tuple((zacc, zacc) for _ in range(heads)))
    for h in range(heads):
        o_v[rows, D * h:D * h + D] = acc[h][0].T.astype(jnp.bfloat16)
        dqkv_v[rows, 3 * D * h:3 * D * h + D] = acc[h][1].T.astype(jnp.bfloat16)


MESH = pl.DeviceIdType.MESH
NC = 2


def place():
    y = lax.axis_index('col')
    r = lax.axis_index('row')
    c = lax.rem(r, 2)
    r_s = r + 1 - 2 * c
    return y, r, c, r_s, lax.rem(r + 2, 4), lax.rem(r_s + 2, 4)


def mult(i, n):
    return pl.multiple_of(i * n, n)


def forward_kernel(x_ref, w_ref, wo_ref, seg_ref, dy_ref, xg, dyg, wg, segg, dqkv_ref, o_ref,
                   stage, wstage, wh, woh, tok, qkv_v, do_v, seg_v, p_scr, dp_scr, m_scr, kt, vt, dk_acc, dv_acc, dqkv_v, o_v,
                   ssem, rsem, lsem):
    y, r, c, r_s, r_x, r_xs = place()
    x = r // 2
    t_loc, h_loc = x_ref.shape
    heads = woh.shape[0] // D
    hw = wh.shape[1]
    ow = woh.shape[0]
    sib, xn, yn = {'row': r_s}, {'row': r_x}, {'col': 1 - y}
    ct = t_loc // NC
    started = []

    def send(i, src, dst, dev):
        cp = pltpu.make_async_remote_copy(src, dst, ssem.at[i], rsem.at[i], device_id=dev, device_id_type=MESH)
        cp.start()
        started.append(cp)

    def recv(i, dst):
        pltpu.make_async_remote_copy(dst, dst, ssem.at[i], rsem.at[i], device_id=sib, device_id_type=MESH).wait_recv()

    def local(i, src, dst):
        cp = pltpu.make_async_copy(src, dst, lsem.at[i])
        cp.start()
        return cp

    def slot(g, yy, rr, j):
        return g.at[pl.ds(pl.multiple_of(rr * t_loc + j * ct, ct), ct), pl.ds(mult(yy, h_loc), h_loc)]

    def own(a, j):
        return a.at[pl.ds(j * ct, ct)]

    def tid(base, kind, j):
        return base + kind * NC + j

    XB, YB = 0, 7 * NC
    WB = 14 * NC
    WOB = WB + 12
    SGB = WOB + 2

    def got_from(kind):
        return ((y, r_s), (y, r_x), (1 - y, r), (y, r_xs), (1 - y, r_x), (1 - y, r_s), (1 - y, r_xs))[kind]

    def send_own(a, g, base, kind, dev):
        for j in range(NC):
            send(tid(base, kind, j), own(a, j), slot(g, y, r, j), dev)

    def forward(g, base, kind_in, outs, j):
        yy, rr = got_from(kind_in)
        recv(tid(base, kind_in, j), slot(g, yy, rr, j))
        for kind_out, dev in outs:
            send(tid(base, kind_out, j), slot(g, yy, rr, j), slot(g, yy, rr, j), dev)

    def take(g, base, kind):
        yy, rr = got_from(kind)
        for j in range(NC):
            recv(tid(base, kind, j), slot(g, yy, rr, j))

    def wslot(rr, q):
        return wg.at[pl.ds(mult(rr, t_loc), t_loc), pl.ds(mult(q, hw), hw)]

    def wq(t, xx):
        return lax.rem(2 * xx + t, 4)

    def w_own(t, kind, xx, dev):
        q = wq(t, xx)
        send(WB + 4 * kind + t, w_ref.at[:, pl.ds(mult(q, hw), hw)], wslot(r, q), dev)

    def w_forward(t):
        q = wq(t, x)
        recv(WB + 4 + t, wslot(r_x, q))
        send(WB + 8 + t, wslot(r_x, q), wslot(r_x, q), sib)

    for i, (rr, dev) in enumerate(((r_s, sib), (r_x, xn), (r_xs, {'row': r_xs}))):
        send(SGB + i, seg_ref, segg.at[r], dev)
    send_own(x_ref, xg, XB, 1, xn)
    send_own(x_ref, xg, XB, 2, yn)
    for t in range(2):
        w_own(t, 1, 1 - x, xn)
    send_own(x_ref, xg, XB, 0, sib)
    for t in range(4):
        w_own(t, 0, x, sib)
    a = local(1, x_ref, stage.at[0])
    b = local(2, dy_ref, stage.at[1])
    d = local(3, w_ref, wstage)
    sg = local(4, seg_ref, segg.at[r])
    own_slot = lambda g: g.at[pl.ds(mult(r, t_loc), t_loc), pl.ds(mult(y, h_loc), h_loc)]
    a.wait()
    a = local(1, stage.at[0], own_slot(xg))
    b.wait()
    b = local(2, stage.at[1], own_slot(dyg))
    d.wait()
    d = local(3, wstage, wg.at[pl.ds(mult(r, t_loc), t_loc)])
    wh[pl.ds(mult(r, t_loc), t_loc), :] = wstage[:, pl.ds(mult(r, hw), hw)]

    for j in range(NC):
        forward(xg, XB, 1, ((4, yn), (3, sib)), j)
        forward(xg, XB, 2, ((5, sib),), j)
    for k in range(2):
        row_to = 2 * c + k
        src = wo_ref.at[pl.ds(k * ow, ow)]
        dst = woh.at[:, pl.ds(mult(y, h_loc), h_loc)]
        mine = (x == y) & (row_to == r)

        @pl.when(mine)
        def _():
            pltpu.make_async_copy(src, dst, lsem.at[0]).start()

        @pl.when(jnp.logical_not(mine))
        def _():
            pltpu.make_async_remote_copy(src, dst, ssem.at[WOB + k], rsem.at[WOB + y],
                                         device_id={'col': x, 'row': row_to}, device_id_type=MESH).start()
    send_own(dy_ref, dyg, YB, 2, yn)
    send_own(dy_ref, dyg, YB, 1, xn)
    send_own(dy_ref, dyg, YB, 0, sib)
    w_forward(0)
    forward(xg, XB, 4, ((6, sib),), 0)
    forward(xg, XB, 4, ((6, sib),), 1)
    w_forward(1)
    a.wait()
    b.wait()
    d.wait()
    sg.wait()

    for t in range(4):
        recv(WB + t, wslot(r_s, wq(t, x)))
    for t in range(2):
        recv(WB + 8 + t, wslot(r_xs, wq(t, x)))
    loads = []
    for i, rr in enumerate((r_s, r_x, r_xs)):
        loads.append(local(5 + i, wslot(rr, r), wh.at[pl.ds(mult(rr, t_loc), t_loc)]))
    for kind in (0, 3, 5, 6):
        take(xg, XB, kind)

    def load_tok(g, rr, s):
        return local(8 + s, g.at[pl.ds(mult(rr, t_loc), t_loc)], tok.at[s])

    blocks = (r, r_s, r_x, r_xs)
    nxt = load_tok(xg, blocks[0], 0)
    for cp in loads:
        cp.wait()
    for i in range(4):
        nxt.wait()
        if i < 3:
            nxt = load_tok(xg, blocks[i + 1], (i + 1) % 2)
        rows = pl.ds(mult(blocks[i], t_loc), t_loc)
        for n in range(hw // 256):
            cols = slice(256 * n, 256 * n + 256)
            qkv_v[rows, cols] = jnp.dot(tok[i % 2], wh[:, cols], preferred_element_type=jnp.float32).astype(jnp.bfloat16)

        for h in range(heads):
            kt[h, :, rows] = qkv_v[rows, 3 * D * h + D:3 * D * h + 2 * D].T
            vt[h, :, rows] = qkv_v[rows, 3 * D * h + 2 * D:3 * D * h + 3 * D].T

    for i, rr in enumerate((r_s, r_x, r_xs)):
        recv(SGB + i, segg.at[rr])
    local(4, segg, seg_v).wait()
    c1 = jnp.sum((seg_v[...] < 1).astype(jnp.int32))
    c2 = jnp.sum((seg_v[...] < 2).astype(jnp.int32))
    dk_acc[...] = jnp.zeros_like(dk_acc)
    dv_acc[...] = jnp.zeros_like(dv_acc)

    for j in range(NC):
        forward(dyg, YB, 2, ((5, sib),), j)
    for yy in range(2):
        piece = woh.at[:, pl.ds(yy * h_loc, h_loc)]
        mine = (y == yy) & (2 * y + x == r)

        @pl.when(mine)
        def _():
            pltpu.make_async_copy(wo_ref.at[pl.ds(0, ow)], piece, lsem.at[0]).wait()

        @pl.when(jnp.logical_not(mine))
        def _():
            recv(WOB + yy, piece)

    def d_out(i, s):
        rows = pl.ds(mult(blocks[i], t_loc), t_loc)
        do_v[rows, :] = lax.dot_general(tok[s], woh[...], NT, preferred_element_type=jnp.float32).astype(jnp.bfloat16)

    def attend(i, between=None):
        q0 = mult(blocks[i], t_loc)
        attention_block(q0, t_loc, c1, c2, qkv_v, do_v, p_scr, dp_scr, m_scr, kt, vt, dk_acc, dv_acc, dqkv_v, o_v, between)

    def dy_forward(j):
        forward(dyg, YB, 1, ((4, yn), (3, sib)), j)

    def w_rest():
        for t in range(2, 4):
            w_own(t, 1, 1 - x, xn)

    load_tok(dyg, r, 0).wait()
    d_out(0, 0)
    attend(0, lambda: dy_forward(0))
    dy_forward(1)
    w_rest()
    for kind in (0, 5):
        take(dyg, YB, kind)
    load_tok(dyg, r_s, 1).wait()
    d_out(1, 1)
    attend(1, lambda: forward(dyg, YB, 4, ((6, sib),), 0))
    forward(dyg, YB, 4, ((6, sib),), 1)
    one = load_tok(dyg, r_x, 0)
    one.wait()
    d_out(2, 0)
    take(dyg, YB, 3)
    attend(2)
    w_forward(2)
    take(dyg, YB, 6)
    load_tok(dyg, r_xs, 1).wait()
    d_out(3, 1)
    attend(3)
    w_forward(3)
    for t in range(2, 4):
        recv(WB + 8 + t, wslot(r_xs, wq(t, x)))
    for h in range(heads):
        dqkv_v[:, 3 * D * h + D:3 * D * h + 2 * D] = dk_acc[h].astype(jnp.bfloat16)
        dqkv_v[:, 3 * D * h + 2 * D:3 * D * h + 3 * D] = dv_acc[h].astype(jnp.bfloat16)
    out_a = local(0, dqkv_v, dqkv_ref)
    out_b = local(1, o_v, o_ref)
    out_a.wait()
    out_b.wait()
    for cp in started:
        cp.wait_send()
    for k in range(2):
        mine = (x == y) & (2 * c + k == r)

        @pl.when(jnp.logical_not(mine))
        def _():
            pltpu.make_async_remote_copy(wo_ref.at[pl.ds(0, ow)], woh.at[:, pl.ds(0, h_loc)], ssem.at[WOB + k], rsem.at[WOB + k],
                                         device_id=sib, device_id_type=MESH).wait_send()


def forward_all(x_blk, w_blk, wo_blk, seg_blk, dy_blk):
    t_loc, h_loc = x_blk.shape
    w_loc = w_blk.shape[1]
    seq, hid = 4 * t_loc, 2 * h_loc
    hw, ow = w_loc // 4, w_loc // 12
    heads = ow // D
    bf, f32 = jnp.bfloat16, jnp.float32
    hbm = pl.BlockSpec(memory_space=pl.ANY)
    n_sem = 14 * NC + 12 + 2 + 3
    seg_shape = (4,) + seg_blk.shape
    return pl.pallas_call(
        forward_kernel,
        in_specs=[hbm] * 5,
        out_specs=[hbm] * 6,
        out_shape=[
            jax.ShapeDtypeStruct((seq, hid), bf), jax.ShapeDtypeStruct((seq, hid), bf),
            jax.ShapeDtypeStruct((hid, w_loc), bf), jax.ShapeDtypeStruct(seg_shape, jnp.int32),
            jax.ShapeDtypeStruct((seq, hw), bf), jax.ShapeDtypeStruct((seq, ow), bf),
        ],
        scratch_shapes=[
            pltpu.VMEM((2, t_loc, h_loc), bf), pltpu.VMEM((t_loc, w_loc), bf), pltpu.VMEM((hid, hw), bf),
            pltpu.VMEM((ow, hid), bf), pltpu.VMEM((2, t_loc, hid), bf),
            pltpu.VMEM((seq, hw), bf), pltpu.VMEM((seq, ow), bf), pltpu.VMEM(seg_shape, jnp.int32),
            pltpu.VMEM((heads, seq, t_loc), f32), pltpu.VMEM((heads, seq, t_loc), f32),
            pltpu.VMEM((seq // BK, heads, 1, t_loc), f32),
            pltpu.VMEM((heads, D, seq), bf), pltpu.VMEM((heads, D, seq), bf),
            pltpu.VMEM((heads, seq, D), f32), pltpu.VMEM((heads, seq, D), f32),
            pltpu.VMEM((seq, hw), bf), pltpu.VMEM((seq, ow), bf),
            pltpu.SemaphoreType.DMA((n_sem,)), pltpu.SemaphoreType.DMA((n_sem,)), pltpu.SemaphoreType.DMA((10,)),
        ],
        compiler_params=pltpu.CompilerParams(has_side_effects=True, vmem_limit_bytes=VMEM_LIMIT),
        name='gather_attend',
    )(x_blk, w_blk, wo_blk, seg_blk, dy_blk)


NJ = 2


def scatter_kernel(xg, dyg, wg, dqkv_ref, o_ref, dx_out, dw_out, dwo_out,
                   dtok, dq_v, w_v, o_v, col_v, dw_v, dwo_v, px_send, px_recv, px_own, dx_v, relay, ssem, rsem, lsem):
    y, r, c, r_s, r_x, r_xs = place()
    x = r // 2
    t_loc, feat = dtok.shape
    hw = dq_v.shape[1]
    ow = o_v.shape[1]
    seq = dq_v.shape[0]
    h_loc = dx_v.shape[1]
    bt = t_loc // NJ
    f32 = jnp.float32
    others = (r_s, r_x, r_xs)
    started = []
    DQ, DW, DWO, PX = 0, 3 * NJ, 3 * NJ + 3, 3 * NJ + 5
    DWF = PX + NJ
    DWG = DWF + 1

    def copy(i, k, src, dst, dev):
        return pltpu.make_async_remote_copy(src, dst, ssem.at[i], rsem.at[k], device_id=dev, device_id_type=MESH)

    def send(i, src, dst, dev):
        cp = copy(i, i, src, dst, dev)
        cp.start()
        started.append(cp)

    def recv(i, dst):
        copy(i, i, dst, dst, {'row': r_s}).wait_recv()

    def local(i, src, dst):
        cp = pltpu.make_async_copy(src, dst, lsem.at[i])
        cp.start()
        return cp

    def tok_slot(rr, j):
        return dtok.at[pl.ds(j * bt, bt), pl.ds(mult(rr, hw), hw)]

    def dw_slot(rr):
        return dw_out.at[:, pl.ds(mult(rr, hw), hw)]

    for j in range(NJ):
        for k in (1, 2, 0):
            rr = others[k]
            src = dqkv_ref.at[pl.ds(pl.multiple_of(rr * t_loc + j * bt, bt), bt)]
            send(DQ + 3 * j + k, src, tok_slot(r, j), {'row': rr})
    own_tok = local(0, dqkv_ref.at[pl.ds(mult(r, t_loc), t_loc)], dtok.at[:, pl.ds(mult(r, hw), hw)])
    ld_o = local(1, o_ref, o_v)
    ld_dy = [local(2 + s, dyg.at[:, pl.ds(512 * s, 512)], col_v.at[s]) for s in range(2)]
    ld_dq = local(4, dqkv_ref, dq_v)

    ld_o.wait()
    ld_x = [None, None]
    blocks = (r_x, r_xs, r_s, r)
    for s in range(4):
        ld_dy[s].wait()
        dwo_v[:, 512 * s:512 * s + 512] = lax.dot_general(o_v[...], col_v[s % 2], TN, preferred_element_type=f32).astype(jnp.bfloat16)
        if s == 1:
            ld_w = local(5, wg, w_v)
        if s < 2:
            ld_dy.append(local(2 + s, dyg.at[:, pl.ds(512 * s + 1024, 512)], col_v.at[s]))
        else:
            ld_x[s - 2] = local(2 + s - 2, xg.at[:, pl.ds(mult(blocks[s - 2], t_loc), t_loc)], col_v.at[s - 2])
    row_to = 2 * y + x
    near = x == y
    for k in range(2):
        src = dwo_v.at[:, pl.ds(k * h_loc, h_loc)]
        dst = dwo_out.at[pl.ds(mult(c, ow), ow)]
        mine = (y == k) & (row_to == r)
        far = (y != k) & (x != y)

        @pl.when(mine)
        def _():
            pltpu.make_async_copy(src, dst, lsem.at[6]).start()

        @pl.when(far)
        def _():
            copy(DWF, DWF, src, relay, {'col': k}).start()

        @pl.when(jnp.logical_not(mine | far))
        def _():
            copy(DWO + k, DWO + c, src, dst, {'col': k, 'row': row_to}).start()

    ld_dq.wait()

    def d_w(i):
        s = i % 2
        ld_x[s].wait()
        dw_v[i] = lax.dot_general(col_v[s], dq_v[...], TN, preferred_element_type=f32).astype(jnp.bfloat16)
        if i < 2:
            ld_x[s] = local(2 + s, xg.at[:, pl.ds(mult(blocks[i + 2], t_loc), t_loc)], col_v.at[s])

    def d_x(j, half, dst):
        for n in range(h_loc // 256):
            rows = pl.ds(pl.multiple_of(half * h_loc + 256 * n, 256), 256)
            dst[pl.ds(j * bt, bt), 256 * n:256 * n + 256] = lax.dot_general(
                dtok[pl.ds(j * bt, bt), :], w_v[rows, :], NT, preferred_element_type=f32)

    def d_x_send(j):
        for k in range(3):
            recv(DQ + 3 * j + k, tok_slot(others[k], j))
        d_x(j, 1 - y, px_send)
        send(PX + j, px_send.at[pl.ds(j * bt, bt)], px_recv.at[pl.ds(j * bt, bt)], {'col': 1 - y})

    d_w(0)
    send(DW + 1, dw_v.at[0], dw_slot(r), {'row': r_x})
    d_w(1)
    send(DW + 2, dw_v.at[1], dw_slot(r), {'row': r_xs})
    ld_w.wait()
    own_tok.wait()
    d_x_send(0)

    @pl.when(near)
    def _():
        recv(DWF, relay)
        copy(DWG, DWG + c, relay, dwo_out.at[pl.ds(mult(c, ow), ow)], {'row': 2 * (1 - y) + x}).start()

    d_w(2)
    send(DW + 0, dw_v.at[2], dw_slot(r), {'row': r_s})
    d_x(0, y, px_own)
    d_x_send(1)
    d_w(3)
    own_dw = local(0, dw_v.at[3], dw_slot(r))
    d_x(1, y, px_own)
    outs = []
    for j in range(NJ):
        rows = pl.ds(j * bt, bt)
        recv(PX + j, px_recv.at[rows])
        dx_v[rows, :] = (px_own[rows, :] + px_recv[rows, :]).astype(jnp.bfloat16)
        outs.append(local(2 + j, dx_v.at[rows], dx_out.at[rows]))
    own_dw.wait()
    for k in range(3):
        recv(DW + k, dw_slot(others[k]))
    src_col, src_x = r // 2, lax.rem(r, 2)
    for k in range(2):
        piece = dwo_out.at[pl.ds(k * ow, ow)]
        mine = (src_col == y) & (2 * src_x + k == r)
        far = (src_col != y) & (src_x != src_col)

        @pl.when(mine)
        def _():
            pltpu.make_async_copy(dwo_v.at[:, pl.ds(0, h_loc)], piece, lsem.at[6]).wait()

        @pl.when(far)
        def _():
            recv(DWG + k, piece)

        @pl.when(jnp.logical_not(mine | far))
        def _():
            recv(DWO + k, piece)
    for cp in outs:
        cp.wait()
    for cp in started:
        cp.wait_send()
    half = dwo_v.at[:, pl.ds(0, h_loc)]
    for k in range(2):
        far = (y != k) & (x != y)

        @pl.when(jnp.logical_not(((y == k) & (row_to == r)) | far))
        def _():
            copy(DWO + k, DWO + k, half, relay, {'row': r_s}).wait_send()

    @pl.when(jnp.logical_not(near))
    def _():
        copy(DWF, DWF, half, relay, {'col': 1 - y}).wait_send()

    @pl.when(near)
    def _():
        copy(DWG, DWG, relay, relay, {'row': r_s}).wait_send()


def scatter_all(x_all, dy_all, w_col, d_qkv, attn_out, blocks):
    bf, f32 = jnp.bfloat16, jnp.float32
    t_loc, h_loc = blocks[0].shape
    seq, hw = d_qkv.shape
    ow = attn_out.shape[1]
    hid, feat = w_col.shape
    hbm = pl.BlockSpec(memory_space=pl.ANY)
    n_sem = 4 * NJ + 9
    return pl.pallas_call(
        scatter_kernel,
        in_specs=[hbm] * 5,
        out_specs=[hbm] * 3,
        out_shape=[jax.ShapeDtypeStruct(b.shape, bf) for b in blocks],
        scratch_shapes=[
            pltpu.VMEM((t_loc, feat), bf), pltpu.VMEM((seq, hw), bf), pltpu.VMEM((hid, feat), bf), pltpu.VMEM((seq, ow), bf),
            pltpu.VMEM((2, seq, t_loc), bf), pltpu.VMEM((4, t_loc, hw), bf), pltpu.VMEM((ow, hid), bf),
            pltpu.VMEM((t_loc, h_loc), f32), pltpu.VMEM((t_loc, h_loc), f32), pltpu.VMEM((t_loc, h_loc), f32),
            pltpu.VMEM((t_loc, h_loc), bf), pltpu.VMEM((ow, h_loc), bf),
            pltpu.SemaphoreType.DMA((n_sem,)), pltpu.SemaphoreType.DMA((n_sem,)), pltpu.SemaphoreType.DMA((7,)),
        ],
        compiler_params=pltpu.CompilerParams(has_side_effects=True, vmem_limit_bytes=VMEM_LIMIT),
        name='project_scatter',
    )(x_all, dy_all, w_col, d_qkv, attn_out)


def solution(mesh):
    tok_spec = P(('dp', 'row'), 'col')
    mat_spec = P('row', 'col')
    seg_spec = P(('dp', 'row'))

    def grad_step(x_blk, wqkv_blk, wout_blk, seg_blk, dy_blk):
        x_all, dy_all, w_col, _, d_qkv, attn_out = forward_all(x_blk, wqkv_blk, wout_blk, seg_blk.reshape(4, -1), dy_blk)
        grad_x, grad_wqkv, grad_wout = scatter_all(x_all, dy_all, w_col, d_qkv, attn_out, (x_blk, wqkv_blk, wout_blk))
        return grad_x, grad_wqkv, grad_wout

    return jax.shard_map(grad_step, mesh=mesh, in_specs=(tok_spec, mat_spec, mat_spec, seg_spec, tok_spec), out_specs=(tok_spec, tok_spec, tok_spec), check_vma=False)
```

```python
import jax
import jax.numpy as jnp
from jax import lax
from jax.experimental import pallas as pl
from jax.experimental.pallas import tpu as pltpu
from jax.sharding import PartitionSpec as P

NT = (((1,), (1,)), ((), ()))
TN = (((0,), (0,)), ((), ()))
MESH = pl.DeviceIdType.MESH
BK = 512
D = 128
NC = 2
NJ = 2
LOW = -3.0e38
VMEM_LIMIT = 66_000_000


def mult(i, n):
    return pl.multiple_of(i * n, n)


def attention_block(q0, bq, h, c1, c2, qkv_v, do_v, p_scr, dp_scr, m_scr, kt, vt, dk_acc, dv_acc, dqkv_v, o_v):
    seq = qkv_v.shape[0]
    scale = D ** -0.5
    to_exp2 = scale * 1.4426950408889634
    f32 = jnp.float32
    rows = pl.ds(q0, bq)
    c0 = 3 * D * h
    iq = q0 + lax.broadcasted_iota(jnp.int32, (1, bq), 1)
    q_doc = (iq >= c1).astype(jnp.int32) + (iq >= c2).astype(jnp.int32)
    q = qkv_v[rows, c0:c0 + D]
    do = do_v[rows, D * h:D * h + D]

    def first(kb, carry):
        m, l, dd = carry
        k0 = pl.multiple_of(kb * BK, BK)
        keys = pl.ds(k0, BK)
        ik = k0 + lax.broadcasted_iota(jnp.int32, (BK, 1), 0)
        k_doc = (ik >= c1).astype(jnp.int32) + (ik >= c2).astype(jnp.int32)
        s = lax.dot_general(qkv_v[keys, c0 + D:c0 + 2 * D], q, NT, preferred_element_type=f32)
        s = jnp.where(q_doc == k_doc, s, LOW)
        dp = lax.dot_general(qkv_v[keys, c0 + 2 * D:c0 + 3 * D], do, NT, preferred_element_type=f32)
        dp_scr[keys, :] = dp
        m_new = jnp.maximum(m, jnp.max(s, axis=0, keepdims=True))
        p = jnp.exp2((s - m_new) * to_exp2)
        p_scr[keys, :] = p
        m_scr[kb] = m_new
        alpha = jnp.exp2((m - m_new) * to_exp2)
        return m_new, alpha * l + jnp.sum(p, axis=0, keepdims=True), alpha * dd + jnp.sum(p * dp, axis=0, keepdims=True)

    zero = jnp.zeros((1, bq), f32)
    m, l, dd = lax.fori_loop(0, seq // BK, first, (jnp.full((1, bq), LOW, f32), zero, zero))
    inv = 1.0 / l
    row_dot = dd * inv

    def second(kb, acc):
        o, dq = acc
        keys = pl.ds(pl.multiple_of(kb * BK, BK), BK)
        f = jnp.exp2((m_scr[kb] - m) * to_exp2) * inv
        p = p_scr[keys, :]
        p_bf = (p * f).astype(jnp.bfloat16)
        ds = ((p * (f * scale)) * (dp_scr[keys, :] - row_dot)).astype(jnp.bfloat16)
        o = o + jnp.dot(vt[h, :, keys], p_bf, preferred_element_type=f32)
        dq = dq + jnp.dot(kt[h, :, keys], ds, preferred_element_type=f32)
        dk_acc[h, keys, :] += jnp.dot(ds, q, preferred_element_type=f32)
        dv_acc[h, keys, :] += jnp.dot(p_bf, do, preferred_element_type=f32)
        return o, dq

    zacc = jnp.zeros((D, bq), f32)
    o, dq = lax.fori_loop(0, seq // BK, second, (zacc, zacc))
    o_v[rows, D * h:D * h + D] = o.T.astype(jnp.bfloat16)
    dqkv_v[rows, c0:c0 + D] = dq.T.astype(jnp.bfloat16)


def step_kernel(x_ref, w_ref, wo_ref, seg_ref, dy_ref, xg, dyg, dx_out, dw_out, dwo_out,
                w_v, tok, col_v, woh, qkv_v, do_v, seg_v, p_scr, dp_scr, m_scr, kt, vt, dk_acc, dv_acc, dqkv_v, o_v,
                dtok, dwo_v, px_recv, dx_v, relay, ssem, rsem, lsem):
    y = lax.axis_index('col')
    r = lax.axis_index('row')
    x = r // 2
    c = lax.rem(r, 2)
    r_s = r + 1 - 2 * c
    r_x = lax.rem(r + 2, 4)
    r_xs = lax.rem(r_s + 2, 4)
    sib, xn, yn = {'row': r_s}, {'row': r_x}, {'col': 1 - y}
    t_loc, h_loc = x_ref.shape
    hw = qkv_v.shape[1]
    ow = woh.shape[0]
    heads = ow // D
    ct, bt = t_loc // NC, t_loc // NJ
    f32, bf = jnp.float32, jnp.bfloat16
    started = []
    XB, YB, WB = 0, 7 * NC, 14 * NC
    WOB = WB + 12
    SGB = WOB + 2
    DQ = SGB + 3
    DW = DQ + 3 + 3 * NJ
    DWO = DW + 3
    PX = DWO + 2
    DWF = PX + NJ
    DWG = DWF + 1

    def copy(i, k, src, dst, dev):
        return pltpu.make_async_remote_copy(src, dst, ssem.at[i], rsem.at[k], device_id=dev, device_id_type=MESH)

    def send(i, src, dst, dev):
        cp = copy(i, i, src, dst, dev)
        cp.start()
        started.append(cp)

    def recv(i, dst):
        copy(i, i, dst, dst, sib).wait_recv()

    def local(i, src, dst):
        cp = pltpu.make_async_copy(src, dst, lsem.at[i])
        cp.start()
        return cp

    def slot(g, yy, rr, j):
        return g.at[pl.ds(pl.multiple_of(rr * t_loc + j * ct, ct), ct), pl.ds(mult(yy, h_loc), h_loc)]

    def tid(base, kind, j):
        return base + kind * NC + j

    def got_from(kind):
        return ((y, r_s), (y, r_x), (1 - y, r), (y, r_xs), (1 - y, r_x), (1 - y, r_s), (1 - y, r_xs))[kind]

    def send_own(a, g, base, kind, dev):
        for j in range(NC):
            send(tid(base, kind, j), a.at[pl.ds(j * ct, ct)], slot(g, y, r, j), dev)

    def forward(g, base, kind_in, outs, j):
        yy, rr = got_from(kind_in)
        recv(tid(base, kind_in, j), slot(g, yy, rr, j))
        for kind_out, dev in outs:
            send(tid(base, kind_out, j), slot(g, yy, rr, j), slot(g, yy, rr, j), dev)

    def take(g, base, kind):
        yy, rr = got_from(kind)
        for j in range(NC):
            recv(tid(base, kind, j), slot(g, yy, rr, j))

    def wslot(rr, q):
        return w_v.at[pl.ds(mult(rr, t_loc), t_loc), pl.ds(mult(q, hw), hw)]

    def wq(t, xx):
        return lax.rem(2 * xx + t, 4)

    def w_own(t, kind, xx, dev):
        q = wq(t, xx)
        send(WB + 4 * kind + t, w_ref.at[:, pl.ds(mult(q, hw), hw)], wslot(r, q), dev)

    def w_forward(t):
        q = wq(t, x)
        recv(WB + 4 + t, wslot(r_x, q))
        send(WB + 8 + t, wslot(r_x, q), wslot(r_x, q), sib)

    send_own(x_ref, xg, XB, 1, xn)
    send_own(x_ref, xg, XB, 2, yn)
    for t in range(2):
        w_own(t, 1, 1 - x, xn)
    send_own(x_ref, xg, XB, 0, sib)
    for t in range(4):
        w_own(t, 0, x, sib)
    for i, (rr, dev) in enumerate(((r_s, sib), (r_x, xn), (r_xs, {'row': r_xs}))):
        send(SGB + i, seg_ref, seg_v.at[r], dev)

    a = local(1, x_ref, tok.at[0, :, pl.ds(0, h_loc)])
    b = local(2, dy_ref, tok.at[1, :, pl.ds(0, h_loc)])
    d = local(3, w_ref, w_v.at[pl.ds(mult(r, t_loc), t_loc)])
    sg = local(4, seg_ref, seg_v.at[r])
    own_slot = lambda g: g.at[pl.ds(mult(r, t_loc), t_loc), pl.ds(mult(y, h_loc), h_loc)]
    a.wait()
    a = local(1, tok.at[0, :, pl.ds(0, h_loc)], own_slot(xg))
    b.wait()
    b = local(2, tok.at[1, :, pl.ds(0, h_loc)], own_slot(dyg))
    dk_acc[...] = jnp.zeros_like(dk_acc)
    dv_acc[...] = jnp.zeros_like(dv_acc)

    for j in range(NC):
        forward(xg, XB, 1, ((4, yn), (3, sib)), j)
        forward(xg, XB, 2, ((5, sib),), j)
    for k in range(2):
        row_to = 2 * c + k
        src = wo_ref.at[pl.ds(k * ow, ow)]
        dst = woh.at[:, pl.ds(mult(y, h_loc), h_loc)]
        mine = (x == y) & (row_to == r)

        @pl.when(mine)
        def _():
            pltpu.make_async_copy(src, dst, lsem.at[0]).start()

        @pl.when(jnp.logical_not(mine))
        def _():
            copy(WOB + k, WOB + y, src, dst, {'col': x, 'row': row_to}).start()
    send_own(dy_ref, dyg, YB, 2, yn)
    send_own(dy_ref, dyg, YB, 1, xn)
    send_own(dy_ref, dyg, YB, 0, sib)
    w_forward(0)
    for j in range(NC):
        forward(xg, XB, 4, ((6, sib),), j)
    a.wait()
    b.wait()
    d.wait()
    sg.wait()

    def load_tok(g, rr, s):
        return local(8 + s, g.at[pl.ds(mult(rr, t_loc), t_loc)], tok.at[s])

    blocks = (r, r_s, r_x, r_xs)
    for kind in (0, 3, 5, 6):
        take(xg, XB, kind)
    loads = [load_tok(xg, blocks[i], i) for i in range(2)]
    w_forward(1)
    for t in range(4):
        recv(WB + t, wslot(r_s, wq(t, x)))
    for t in range(2):
        recv(WB + 8 + t, wslot(r_xs, wq(t, x)))
    for i in range(4):
        loads[i].wait()
        rows = pl.ds(mult(blocks[i], t_loc), t_loc)
        for n in range(hw // 256):
            mine = w_v[:, pl.ds(pl.multiple_of(r * hw + 256 * n, 256), 256)]
            qkv_v[rows, 256 * n:256 * n + 256] = jnp.dot(tok[i % 2], mine, preferred_element_type=f32).astype(bf)
        if i < 2:
            loads.append(load_tok(xg, blocks[i + 2], i))
        for h in range(heads):
            kt[h, :, rows] = qkv_v[rows, 3 * D * h + D:3 * D * h + 2 * D].T
            vt[h, :, rows] = qkv_v[rows, 3 * D * h + 2 * D:3 * D * h + 3 * D].T

    for i, rr in enumerate((r_s, r_x, r_xs)):
        recv(SGB + i, seg_v.at[rr])
    c1 = jnp.sum((seg_v[...] < 1).astype(jnp.int32))
    c2 = jnp.sum((seg_v[...] < 2).astype(jnp.int32))
    for j in range(NC):
        forward(dyg, YB, 2, ((5, sib),), j)
    for yy in range(2):
        piece = woh.at[:, pl.ds(yy * h_loc, h_loc)]
        mine = (y == yy) & (2 * y + x == r)

        @pl.when(mine)
        def _():
            pltpu.make_async_copy(wo_ref.at[pl.ds(0, ow)], piece, lsem.at[0]).wait()

        @pl.when(jnp.logical_not(mine))
        def _():
            recv(WOB + yy, piece)

    def d_out(i, s):
        rows = pl.ds(mult(blocks[i], t_loc), t_loc)
        do_v[rows, :] = lax.dot_general(tok[s], woh[...], NT, preferred_element_type=f32).astype(bf)

    def attend(i, h):
        attention_block(mult(blocks[i], t_loc), t_loc, h, c1, c2, qkv_v, do_v, p_scr, dp_scr, m_scr, kt, vt, dk_acc, dv_acc, dqkv_v, o_v)

    def dy_forward(j):
        forward(dyg, YB, 1, ((4, yn), (3, sib)), j)

    load_tok(dyg, r, 0).wait()
    d_out(0, 0)
    attend(0, 0)
    dy_forward(0)
    attend(0, 1)
    dy_forward(1)
    for t in range(2, 4):
        w_own(t, 1, 1 - x, xn)
    for kind in (0, 5):
        take(dyg, YB, kind)
    load_tok(dyg, r_s, 1).wait()
    d_out(1, 1)
    attend(1, 0)
    forward(dyg, YB, 4, ((6, sib),), 0)
    attend(1, 1)
    forward(dyg, YB, 4, ((6, sib),), 1)
    load_tok(dyg, r_x, 0).wait()
    d_out(2, 0)
    attend(2, 0)
    w_forward(2)
    take(dyg, YB, 3)
    take(dyg, YB, 6)
    load_tok(dyg, r_xs, 1).wait()
    d_out(3, 1)
    ld = [local(5 + s, dyg.at[:, pl.ds(512 * s, 512)], col_v.at[s]) for s in range(2)]
    attend(3, 0)

    others = (r_s, r_x, r_xs)

    def finish(h):
        c0 = 3 * D * h
        dqkv_v[:, c0 + D:c0 + 2 * D] = dk_acc[h].astype(bf)
        dqkv_v[:, c0 + 2 * D:c0 + 3 * D] = dv_acc[h].astype(bf)

    def tok_slot(rr, h, j, n):
        return dtok.at[pl.ds(j * n, n), pl.ds(pl.multiple_of(rr * hw + 3 * D * h, 3 * D), 3 * D)]

    def send_dqkv(i, h, j, n):
        for k in (1, 2, 0):
            src = dqkv_v.at[pl.ds(pl.multiple_of(others[k] * t_loc + j * n, n), n), pl.ds(3 * D * h, 3 * D)]
            send(i + k, src, tok_slot(r, h, j, n), {'row': others[k]})

    finish(0)
    send_dqkv(DQ, 0, 0, t_loc)
    attend(2, 1)
    w_forward(3)
    attend(3, 1)
    finish(1)
    for j in range(NJ):
        send_dqkv(DQ + 3 + 3 * j, 1, j, bt)
    dtok[:, pl.ds(mult(r, hw), hw)] = dqkv_v[pl.ds(mult(r, t_loc), t_loc), :]

    order = (r_x, r_xs, r_s, r)
    for s in range(4):
        ld[s].wait()
        dwo_v[:, 512 * s:512 * s + 512] = lax.dot_general(o_v[...], col_v[s % 2], TN, preferred_element_type=f32).astype(bf)
        if s < 2:
            ld.append(local(5 + s, dyg.at[:, pl.ds(512 * s + 1024, 512)], col_v.at[s]))
        else:
            ld.append(local(5 + s - 2, xg.at[:, pl.ds(mult(order[s - 2], t_loc), t_loc)], col_v.at[s - 2]))
    ld = ld[4:]
    row_to = 2 * y + x
    near = x == y
    for k in range(2):
        src = dwo_v.at[:, pl.ds(k * h_loc, h_loc)]
        dst = dwo_out.at[pl.ds(mult(c, ow), ow)]
        mine = (y == k) & (row_to == r)
        far = (y != k) & (x != y)

        @pl.when(mine)
        def _():
            pltpu.make_async_copy(src, dst, lsem.at[0]).start()

        @pl.when(far)
        def _():
            copy(DWF, DWF, src, relay, {'col': k}).start()

        @pl.when(jnp.logical_not(mine | far))
        def _():
            copy(DWO + k, DWO + c, src, dst, {'col': k, 'row': row_to}).start()

    def dw_slot(rr):
        return dw_out.at[:, pl.ds(mult(rr, hw), hw)]

    def d_w(i):
        s = i % 2
        ld[i].wait()
        qkv_v[t_loc * i:t_loc * i + t_loc, :] = lax.dot_general(col_v[s], dqkv_v[...], TN, preferred_element_type=f32).astype(bf)
        if i < 2:
            ld.append(local(5 + s, xg.at[:, pl.ds(mult(order[i + 2], t_loc), t_loc)], col_v.at[s]))

    def send_dw(i, k):
        send(DW + k, qkv_v.at[pl.ds(t_loc * i, t_loc)], dw_slot(r), {'row': others[k]})

    def d_x(j, half, dst):
        for n in range(h_loc // 256):
            rows = pl.ds(pl.multiple_of(half * h_loc + 256 * n, 256), 256)
            dst[pl.ds(2 * bt * j + bt * (n // 2), bt), 256 * (n % 2):256 * (n % 2) + 256] = lax.dot_general(
                dtok[pl.ds(j * bt, bt), :], w_v[rows, :], NT, preferred_element_type=f32)

    def d_x_send(j):
        for k in range(3):
            recv(DQ + 3 + 3 * j + k, tok_slot(others[k], 1, j, bt))
        d_x(j, 1 - y, dp_scr)
        part = pl.ds(2 * bt * j, 2 * bt)
        send(PX + j, dp_scr.at[part], px_recv.at[part], yn)

    d_w(0)
    send_dw(0, 1)
    d_w(1)
    send_dw(1, 2)
    for t in range(2, 4):
        recv(WB + 8 + t, wslot(r_xs, wq(t, x)))
    for k in range(3):
        recv(DQ + k, tok_slot(others[k], 0, 0, t_loc))
    d_x_send(0)

    @pl.when(near)
    def _():
        recv(DWF, relay)
        copy(DWG, DWG + c, relay, dwo_out.at[pl.ds(mult(c, ow), ow)], {'row': 2 * (1 - y) + x}).start()

    d_w(2)
    send_dw(2, 0)
    d_x_send(1)
    d_x(0, y, p_scr)
    d_w(3)
    own_dw = local(7, qkv_v.at[pl.ds(3 * t_loc, t_loc)], dw_slot(r))
    d_x(1, y, p_scr)
    outs = []
    for j in range(NJ):
        recv(PX + j, px_recv.at[pl.ds(2 * bt * j, 2 * bt)])
        for q in range(2):
            part = pl.ds(2 * bt * j + bt * q, bt)
            dx_v[pl.ds(j * bt, bt), 512 * q:512 * q + 512] = (p_scr[part, :] + px_recv[part, :]).astype(bf)
        outs.append(local(8 + j, dx_v.at[pl.ds(j * bt, bt)], dx_out.at[pl.ds(j * bt, bt)]))
    own_dw.wait()
    for k in range(3):
        recv(DW + k, dw_slot(others[k]))
    src_col, src_x = r // 2, lax.rem(r, 2)
    for k in range(2):
        piece = dwo_out.at[pl.ds(k * ow, ow)]
        mine = (src_col == y) & (2 * src_x + k == r)
        far = (src_col != y) & (src_x != src_col)

        @pl.when(mine)
        def _():
            pltpu.make_async_copy(dwo_v.at[:, pl.ds(0, h_loc)], piece, lsem.at[0]).wait()

        @pl.when(far)
        def _():
            recv(DWG + k, piece)

        @pl.when(jnp.logical_not(mine | far))
        def _():
            recv(DWO + k, piece)
    for cp in outs:
        cp.wait()
    for cp in started:
        cp.wait_send()
    half = dwo_v.at[:, pl.ds(0, h_loc)]
    for k in range(2):
        @pl.when(jnp.logical_not((x == y) & (2 * c + k == r)))
        def _():
            copy(WOB + k, WOB + k, wo_ref.at[pl.ds(0, ow)], half, sib).wait_send()

        @pl.when(jnp.logical_not(((y == k) & (row_to == r)) | ((y != k) & (x != y))))
        def _():
            copy(DWO + k, DWO + k, half, relay, sib).wait_send()

    @pl.when(jnp.logical_not(near))
    def _():
        copy(DWF, DWF, half, relay, yn).wait_send()

    @pl.when(near)
    def _():
        copy(DWG, DWG, relay, relay, sib).wait_send()


def step_all(x_blk, w_blk, wo_blk, seg_blk, dy_blk):
    t_loc, h_loc = x_blk.shape
    w_loc = w_blk.shape[1]
    seq, hid = 4 * t_loc, 2 * h_loc
    hw, ow = w_loc // 4, w_loc // 12
    heads = ow // D
    bf, f32 = jnp.bfloat16, jnp.float32
    hbm = pl.BlockSpec(memory_space=pl.ANY)
    n_sem = 14 * NC + 12 + 2 + 3 + 3 + 3 * NJ + 3 + 2 + NJ + 1 + 2
    return pl.pallas_call(
        step_kernel,
        in_specs=[hbm] * 5,
        out_specs=[hbm] * 5,
        out_shape=[jax.ShapeDtypeStruct((seq, hid), bf)] * 2 + [jax.ShapeDtypeStruct(b.shape, bf) for b in (x_blk, w_blk, wo_blk)],
        scratch_shapes=[
            pltpu.VMEM((hid, w_loc), bf), pltpu.VMEM((2, t_loc, hid), bf), pltpu.VMEM((2, seq, t_loc), bf),
            pltpu.VMEM((ow, hid), bf), pltpu.VMEM((seq, hw), bf), pltpu.VMEM((seq, ow), bf),
            pltpu.VMEM((4,) + seg_blk.shape, jnp.int32),
            pltpu.VMEM((seq, t_loc), f32), pltpu.VMEM((seq, t_loc), f32), pltpu.VMEM((seq // BK, 1, t_loc), f32),
            pltpu.VMEM((heads, D, seq), bf), pltpu.VMEM((heads, D, seq), bf),
            pltpu.VMEM((heads, seq, D), f32), pltpu.VMEM((heads, seq, D), f32),
            pltpu.VMEM((seq, hw), bf), pltpu.VMEM((seq, ow), bf),
            pltpu.VMEM((t_loc, w_loc), bf), pltpu.VMEM((ow, hid), bf), pltpu.VMEM((2 * t_loc, t_loc), f32),
            pltpu.VMEM((t_loc, h_loc), bf), pltpu.VMEM((ow, h_loc), bf),
            pltpu.SemaphoreType.DMA((n_sem,)), pltpu.SemaphoreType.DMA((n_sem,)), pltpu.SemaphoreType.DMA((10,)),
        ],
        compiler_params=pltpu.CompilerParams(has_side_effects=True, vmem_limit_bytes=VMEM_LIMIT),
        name='mega_step',
    )(x_blk, w_blk, wo_blk, seg_blk, dy_blk)


def solution(mesh):
    tok_spec = P(('dp', 'row'), 'col')
    mat_spec = P('row', 'col')
    seg_spec = P(('dp', 'row'))

    def grad_step(x_blk, wqkv_blk, wout_blk, seg_blk, dy_blk):
        _, _, grad_x, grad_wqkv, grad_wout = step_all(x_blk, wqkv_blk, wout_blk, seg_blk.reshape(4, -1), dy_blk)
        return grad_x, grad_wqkv, grad_wout

    return jax.shard_map(grad_step, mesh=mesh, in_specs=(tok_spec, mat_spec, mat_spec, seg_spec, tok_spec), out_specs=(tok_spec, tok_spec, tok_spec), check_vma=False)
```

```python
import functools

import jax
import jax.numpy as jnp
from jax import lax
from jax.experimental import pallas as pl
from jax.experimental.pallas import tpu as pltpu
from jax.sharding import PartitionSpec as P

NT = (((1,), (1,)), ((), ()))
TN = (((0,), (0,)), ((), ()))
MESH = pl.DeviceIdType.MESH
BK = 512
D = 128
NC = 2
NJ = 2
LOW = -3.0e38
VMEM_LIMIT = 66_000_000


def mult(i, n):
    return pl.multiple_of(i * n, n)


def attention_block(q0, bq, h, c1, c2, qkv_v, do_v, p_scr, dp_scr, m_scr, kt, vt, dk_acc, dv_acc, dqkv_v, o_v, between):
    seq = qkv_v.shape[0]
    scale = D ** -0.5
    to_exp2 = scale * 1.4426950408889634
    f32 = jnp.float32
    rows = pl.ds(q0, bq)
    c0 = 3 * D * h
    iq = q0 + lax.broadcasted_iota(jnp.int32, (1, bq), 1)
    q_doc = (iq >= c1).astype(jnp.int32) + (iq >= c2).astype(jnp.int32)
    q = qkv_v[rows, c0:c0 + D]
    do = do_v[rows, D * h:D * h + D]

    def first(kb, carry):
        m, l, dd = carry
        k0 = pl.multiple_of(kb * BK, BK)
        keys = pl.ds(k0, BK)
        ik = k0 + lax.broadcasted_iota(jnp.int32, (BK, 1), 0)
        k_doc = (ik >= c1).astype(jnp.int32) + (ik >= c2).astype(jnp.int32)
        s = lax.dot_general(qkv_v[keys, c0 + D:c0 + 2 * D], q, NT, preferred_element_type=f32)
        s = jnp.where(q_doc == k_doc, s, LOW)
        dp = lax.dot_general(qkv_v[keys, c0 + 2 * D:c0 + 3 * D], do, NT, preferred_element_type=f32)
        dp_scr[keys, :] = dp
        m_new = jnp.maximum(m, jnp.max(s, axis=0, keepdims=True))
        p = jnp.exp2((s - m_new) * to_exp2)
        p_scr[keys, :] = p
        m_scr[kb] = m_new
        alpha = jnp.exp2((m - m_new) * to_exp2)
        return m_new, alpha * l + jnp.sum(p, axis=0, keepdims=True), alpha * dd + jnp.sum(p * dp, axis=0, keepdims=True)

    zero = jnp.zeros((1, bq), f32)
    m, l, dd = lax.fori_loop(0, seq // BK, first, (jnp.full((1, bq), LOW, f32), zero, zero))
    if between is not None:
        between()
    inv = 1.0 / l
    row_dot = dd * inv

    def second(kb, acc):
        o, dq = acc
        keys = pl.ds(pl.multiple_of(kb * BK, BK), BK)
        f = jnp.exp2((m_scr[kb] - m) * to_exp2) * inv
        p = p_scr[keys, :]
        p_bf = (p * f).astype(jnp.bfloat16)
        ds = ((p * (f * scale)) * (dp_scr[keys, :] - row_dot)).astype(jnp.bfloat16)
        o = o + jnp.dot(vt[h, :, keys], p_bf, preferred_element_type=f32)
        dq = dq + jnp.dot(kt[h, :, keys], ds, preferred_element_type=f32)
        dk_acc[h, keys, :] += jnp.dot(ds, q, preferred_element_type=f32)
        dv_acc[h, keys, :] += jnp.dot(p_bf, do, preferred_element_type=f32)
        return o, dq

    zacc = jnp.zeros((D, bq), f32)
    o, dq = lax.fori_loop(0, seq // BK, second, (zacc, zacc))
    o_v[rows, D * h:D * h + D] = o.T.astype(jnp.bfloat16)
    dqkv_v[rows, c0:c0 + D] = dq.T.astype(jnp.bfloat16)


def step_kernel(x_ref, w_ref, wo_ref, seg_ref, dy_ref, xg, dyg, dx_out, dw_out, dwo_out,
                w_v, tok, col_v, woh, qkv_v, do_v, seg_v, p_scr, dp_scr, m_scr, kt, vt, dk_acc, dv_acc, dqkv_v, o_v,
                dtok, dwo_v, px_recv, dx_v, relay, ssem, rsem, lsem):
    y = lax.axis_index('col')
    r = lax.axis_index('row')
    x = r // 2
    c = lax.rem(r, 2)
    r_s = r + 1 - 2 * c
    r_x = lax.rem(r + 2, 4)
    r_xs = lax.rem(r_s + 2, 4)
    sib, xn, yn = {'row': r_s}, {'row': r_x}, {'col': 1 - y}
    t_loc, h_loc = x_ref.shape
    hw = qkv_v.shape[1]
    ow = woh.shape[0]
    heads = ow // D
    ct, bt = t_loc // NC, t_loc // NJ
    f32, bf = jnp.float32, jnp.bfloat16
    started = []
    XB, YB, WB = 0, 7 * NC, 14 * NC
    WOB = WB + 12
    SGB = WOB + 2
    DQ = SGB + 3
    DW = DQ + 3 + 3 * NJ
    DWO = DW + 3
    PX = DWO + 2
    DWF = PX + NJ
    DWG = DWF + 1

    def copy(i, k, src, dst, dev):
        return pltpu.make_async_remote_copy(src, dst, ssem.at[i], rsem.at[k], device_id=dev, device_id_type=MESH)

    def send(i, src, dst, dev):
        cp = copy(i, i, src, dst, dev)
        cp.start()
        started.append(cp)

    def recv(i, dst):
        copy(i, i, dst, dst, sib).wait_recv()

    def local(i, src, dst):
        cp = pltpu.make_async_copy(src, dst, lsem.at[i])
        cp.start()
        return cp

    def slot(g, yy, rr, j):
        return g.at[pl.ds(pl.multiple_of(rr * t_loc + j * ct, ct), ct), pl.ds(mult(yy, h_loc), h_loc)]

    def tid(base, kind, j):
        return base + kind * NC + j

    def got_from(kind):
        return ((y, r_s), (y, r_x), (1 - y, r), (y, r_xs), (1 - y, r_x), (1 - y, r_s), (1 - y, r_xs))[kind]

    def send_own(a, g, base, kind, dev):
        for j in range(NC):
            send(tid(base, kind, j), a.at[pl.ds(j * ct, ct)], slot(g, y, r, j), dev)

    def forward(g, base, kind_in, outs, j):
        yy, rr = got_from(kind_in)
        recv(tid(base, kind_in, j), slot(g, yy, rr, j))
        for kind_out, dev in outs:
            send(tid(base, kind_out, j), slot(g, yy, rr, j), slot(g, yy, rr, j), dev)

    def take(g, base, kind):
        yy, rr = got_from(kind)
        for j in range(NC):
            recv(tid(base, kind, j), slot(g, yy, rr, j))

    def wslot(rr, q):
        return w_v.at[pl.ds(mult(rr, t_loc), t_loc), pl.ds(mult(q, hw), hw)]

    def wq(t, xx):
        return lax.rem(2 * xx + t, 4)

    def w_own(t, kind, xx, dev):
        q = wq(t, xx)
        send(WB + 4 * kind + t, w_ref.at[:, pl.ds(mult(q, hw), hw)], wslot(r, q), dev)

    def w_forward(t):
        q = wq(t, x)
        recv(WB + 4 + t, wslot(r_x, q))
        send(WB + 8 + t, wslot(r_x, q), wslot(r_x, q), sib)

    barrier = pltpu.get_barrier_semaphore()
    for i in range(1, 8):
        pl.semaphore_signal(barrier, inc=1, device_id={'row': lax.rem(r + i, 4), 'col': lax.rem(y + i // 4, 2)}, device_id_type=MESH)
    pl.semaphore_wait(barrier, 7)

    send_own(x_ref, xg, XB, 1, xn)
    send_own(x_ref, xg, XB, 2, yn)
    for t in range(2):
        w_own(t, 1, 1 - x, xn)
    send_own(x_ref, xg, XB, 0, sib)
    for t in range(4):
        w_own(t, 0, x, sib)
    for i, (rr, dev) in enumerate(((r_s, sib), (r_x, xn), (r_xs, {'row': r_xs}))):
        send(SGB + i, seg_ref, seg_v.at[r], dev)

    a = local(1, x_ref, tok.at[0, :, pl.ds(0, h_loc)])
    b = local(2, dy_ref, tok.at[1, :, pl.ds(0, h_loc)])
    d = local(3, w_ref, w_v.at[pl.ds(mult(r, t_loc), t_loc)])
    sg = local(4, seg_ref, seg_v.at[r])
    own_slot = lambda g: g.at[pl.ds(mult(r, t_loc), t_loc), pl.ds(mult(y, h_loc), h_loc)]
    a.wait()
    a = local(1, tok.at[0, :, pl.ds(0, h_loc)], own_slot(xg))
    b.wait()
    b = local(2, tok.at[1, :, pl.ds(0, h_loc)], own_slot(dyg))
    dk_acc[...] = jnp.zeros_like(dk_acc)
    dv_acc[...] = jnp.zeros_like(dv_acc)

    for j in range(NC):
        forward(xg, XB, 1, ((4, yn), (3, sib)), j)
        forward(xg, XB, 2, ((5, sib),), j)
    for k in range(2):
        row_to = 2 * c + k
        src = wo_ref.at[pl.ds(k * ow, ow)]
        dst = woh.at[:, pl.ds(mult(y, h_loc), h_loc)]
        mine = (x == y) & (row_to == r)

        @pl.when(mine)
        def _():
            pltpu.make_async_copy(src, dst, lsem.at[0]).start()

        @pl.when(jnp.logical_not(mine))
        def _():
            copy(WOB + k, WOB + y, src, dst, {'col': x, 'row': row_to}).start()
    send_own(dy_ref, dyg, YB, 2, yn)
    send_own(dy_ref, dyg, YB, 1, xn)
    send_own(dy_ref, dyg, YB, 0, sib)
    w_forward(0)
    for j in range(NC):
        forward(xg, XB, 4, ((6, sib),), j)
    a.wait()
    b.wait()
    d.wait()
    sg.wait()

    def load_tok(g, rr, s):
        return local(8 + s, g.at[pl.ds(mult(rr, t_loc), t_loc)], tok.at[s])

    blocks = (r, r_s, r_x, r_xs)
    for kind in (0, 3, 5, 6):
        take(xg, XB, kind)
    loads = [load_tok(xg, blocks[i], i) for i in range(2)]
    w_forward(1)
    for t in range(4):
        recv(WB + t, wslot(r_s, wq(t, x)))
    for t in range(2):
        recv(WB + 8 + t, wslot(r_xs, wq(t, x)))
    for i in range(4):
        loads[i].wait()
        rows = pl.ds(mult(blocks[i], t_loc), t_loc)
        for n in range(hw // 256):
            mine = w_v[:, pl.ds(pl.multiple_of(r * hw + 256 * n, 256), 256)]
            qkv_v[rows, 256 * n:256 * n + 256] = jnp.dot(tok[i % 2], mine, preferred_element_type=f32).astype(bf)
        if i < 2:
            loads.append(load_tok(xg, blocks[i + 2], i))
        for h in range(heads):
            kt[h, :, rows] = qkv_v[rows, 3 * D * h + D:3 * D * h + 2 * D].T
            vt[h, :, rows] = qkv_v[rows, 3 * D * h + 2 * D:3 * D * h + 3 * D].T

    for i, rr in enumerate((r_s, r_x, r_xs)):
        recv(SGB + i, seg_v.at[rr])
    c1 = jnp.sum((seg_v[...] < 1).astype(jnp.int32))
    c2 = jnp.sum((seg_v[...] < 2).astype(jnp.int32))
    for j in range(NC):
        forward(dyg, YB, 2, ((5, sib),), j)
    for yy in range(2):
        piece = woh.at[:, pl.ds(yy * h_loc, h_loc)]
        mine = (y == yy) & (2 * y + x == r)

        @pl.when(mine)
        def _():
            pltpu.make_async_copy(wo_ref.at[pl.ds(0, ow)], piece, lsem.at[0]).wait()

        @pl.when(jnp.logical_not(mine))
        def _():
            recv(WOB + yy, piece)

    def d_out(i, s):
        rows = pl.ds(mult(blocks[i], t_loc), t_loc)
        do_v[rows, :] = lax.dot_general(tok[s], woh[...], NT, preferred_element_type=f32).astype(bf)

    def attend(i, h, between=None):
        attention_block(mult(blocks[i], t_loc), t_loc, h, c1, c2, qkv_v, do_v, p_scr, dp_scr, m_scr, kt, vt, dk_acc, dv_acc, dqkv_v, o_v, between)

    def dy_forward(j):
        forward(dyg, YB, 1, ((4, yn), (3, sib)), j)

    load_tok(dyg, r, 0).wait()
    d_out(0, 0)
    attend(0, 0, lambda: dy_forward(0))
    for t in range(2, 4):
        w_own(t, 1, 1 - x, xn)
    attend(0, 1, lambda: dy_forward(1))
    for kind in (0, 5):
        take(dyg, YB, kind)
    load_tok(dyg, r_s, 1).wait()
    d_out(1, 1)
    attend(1, 0)
    forward(dyg, YB, 4, ((6, sib),), 0)
    attend(1, 1)
    forward(dyg, YB, 4, ((6, sib),), 1)
    load_tok(dyg, r_x, 0).wait()
    d_out(2, 0)
    attend(2, 0)
    w_forward(2)
    take(dyg, YB, 3)
    take(dyg, YB, 6)
    load_tok(dyg, r_xs, 1).wait()
    d_out(3, 1)
    ld = [local(5 + s, dyg.at[:, pl.ds(512 * s, 512)], col_v.at[s]) for s in range(2)]
    attend(3, 0)

    others = (r_s, r_x, r_xs)

    def finish(h):
        c0 = 3 * D * h
        dqkv_v[:, c0 + D:c0 + 2 * D] = dk_acc[h].astype(bf)
        dqkv_v[:, c0 + 2 * D:c0 + 3 * D] = dv_acc[h].astype(bf)

    def tok_slot(rr, h, j, n):
        return dtok.at[pl.ds(j * n, n), pl.ds(pl.multiple_of(rr * hw + 3 * D * h, 3 * D), 3 * D)]

    def send_dqkv(i, h, j, n):
        for k in (1, 2, 0):
            src = dqkv_v.at[pl.ds(pl.multiple_of(others[k] * t_loc + j * n, n), n), pl.ds(3 * D * h, 3 * D)]
            send(i + k, src, tok_slot(r, h, j, n), {'row': others[k]})

    finish(0)
    send_dqkv(DQ, 0, 0, t_loc)
    attend(2, 1)
    w_forward(3)
    attend(3, 1)
    finish(1)
    for j in range(NJ):
        send_dqkv(DQ + 3 + 3 * j, 1, j, bt)
    dtok[:, pl.ds(mult(r, hw), hw)] = dqkv_v[pl.ds(mult(r, t_loc), t_loc), :]

    order = (r_x, r_xs, r_s, r)
    for s in range(4):
        ld[s].wait()
        dwo_v[:, 512 * s:512 * s + 512] = lax.dot_general(o_v[...], col_v[s % 2], TN, preferred_element_type=f32).astype(bf)
        if s < 2:
            ld.append(local(5 + s, dyg.at[:, pl.ds(512 * s + 1024, 512)], col_v.at[s]))
        else:
            ld.append(local(5 + s - 2, xg.at[:, pl.ds(mult(order[s - 2], t_loc), t_loc)], col_v.at[s - 2]))
    ld = ld[4:]
    row_to = 2 * y + x
    near = x == y
    for k in range(2):
        src = dwo_v.at[:, pl.ds(k * h_loc, h_loc)]
        dst = dwo_out.at[pl.ds(mult(c, ow), ow)]
        mine = (y == k) & (row_to == r)
        far = (y != k) & (x != y)

        @pl.when(mine)
        def _():
            pltpu.make_async_copy(src, dst, lsem.at[0]).start()

        @pl.when(far)
        def _():
            copy(DWF, DWF, src, relay, {'col': k}).start()

        @pl.when(jnp.logical_not(mine | far))
        def _():
            copy(DWO + k, DWO + c, src, dst, {'col': k, 'row': row_to}).start()

    def dw_slot(rr):
        return dw_out.at[:, pl.ds(mult(rr, hw), hw)]

    def d_w(i):
        s = i % 2
        ld[i].wait()
        qkv_v[t_loc * i:t_loc * i + t_loc, :] = lax.dot_general(col_v[s], dqkv_v[...], TN, preferred_element_type=f32).astype(bf)
        if i < 2:
            ld.append(local(5 + s, xg.at[:, pl.ds(mult(order[i + 2], t_loc), t_loc)], col_v.at[s]))

    def send_dw(i, k):
        send(DW + k, qkv_v.at[pl.ds(t_loc * i, t_loc)], dw_slot(r), {'row': others[k]})

    def d_x(j, half, dst):
        for n in range(h_loc // 256):
            rows = pl.ds(pl.multiple_of(half * h_loc + 256 * n, 256), 256)
            dst[pl.ds(2 * bt * j + bt * (n // 2), bt), 256 * (n % 2):256 * (n % 2) + 256] = lax.dot_general(
                dtok[pl.ds(j * bt, bt), :], w_v[rows, :], NT, preferred_element_type=f32)

    def d_x_send(j):
        for k in range(3):
            recv(DQ + 3 + 3 * j + k, tok_slot(others[k], 1, j, bt))
        d_x(j, 1 - y, dp_scr)
        part = pl.ds(2 * bt * j, 2 * bt)
        send(PX + j, dp_scr.at[part], px_recv.at[part], yn)

    d_w(0)
    send_dw(0, 1)
    d_w(1)
    send_dw(1, 2)
    for t in range(2, 4):
        recv(WB + 8 + t, wslot(r_xs, wq(t, x)))
    for k in range(3):
        recv(DQ + k, tok_slot(others[k], 0, 0, t_loc))
    d_x_send(0)

    @pl.when(near)
    def _():
        recv(DWF, relay)
        copy(DWG, DWG + c, relay, dwo_out.at[pl.ds(mult(c, ow), ow)], {'row': 2 * (1 - y) + x}).start()

    d_w(2)
    send_dw(2, 0)
    d_x_send(1)
    d_x(0, y, p_scr)
    d_w(3)
    own_dw = local(7, qkv_v.at[pl.ds(3 * t_loc, t_loc)], dw_slot(r))
    d_x(1, y, p_scr)
    outs = []
    for j in range(NJ):
        recv(PX + j, px_recv.at[pl.ds(2 * bt * j, 2 * bt)])
        for q in range(2):
            part = pl.ds(2 * bt * j + bt * q, bt)
            dx_v[pl.ds(j * bt, bt), 512 * q:512 * q + 512] = (p_scr[part, :] + px_recv[part, :]).astype(bf)
        outs.append(local(8 + j, dx_v.at[pl.ds(j * bt, bt)], dx_out.at[pl.ds(j * bt, bt)]))
    own_dw.wait()
    for k in range(3):
        recv(DW + k, dw_slot(others[k]))
    src_col, src_x = r // 2, lax.rem(r, 2)
    for k in range(2):
        piece = dwo_out.at[pl.ds(k * ow, ow)]
        mine = (src_col == y) & (2 * src_x + k == r)
        far = (src_col != y) & (src_x != src_col)

        @pl.when(mine)
        def _():
            pltpu.make_async_copy(dwo_v.at[:, pl.ds(0, h_loc)], piece, lsem.at[0]).wait()

        @pl.when(far)
        def _():
            recv(DWG + k, piece)

        @pl.when(jnp.logical_not(mine | far))
        def _():
            recv(DWO + k, piece)
    for cp in outs:
        cp.wait()
    for cp in started:
        cp.wait_send()
    half = dwo_v.at[:, pl.ds(0, h_loc)]
    for k in range(2):
        @pl.when(jnp.logical_not((x == y) & (2 * c + k == r)))
        def _():
            copy(WOB + k, WOB + k, wo_ref.at[pl.ds(0, ow)], half, sib).wait_send()

        @pl.when(jnp.logical_not(((y == k) & (row_to == r)) | ((y != k) & (x != y))))
        def _():
            copy(DWO + k, DWO + k, half, relay, sib).wait_send()

    @pl.when(jnp.logical_not(near))
    def _():
        copy(DWF, DWF, half, relay, yn).wait_send()

    @pl.when(near)
    def _():
        copy(DWG, DWG, relay, relay, sib).wait_send()


def step_all(x_blk, w_blk, wo_blk, seg_blk, dy_blk):
    t_loc, h_loc = x_blk.shape
    w_loc = w_blk.shape[1]
    seq, hid = 4 * t_loc, 2 * h_loc
    hw, ow = w_loc // 4, w_loc // 12
    heads = ow // D
    bf, f32 = jnp.bfloat16, jnp.float32
    hbm = pl.BlockSpec(memory_space=pl.ANY)
    n_sem = 14 * NC + 12 + 2 + 3 + 3 + 3 * NJ + 3 + 2 + NJ + 1 + 2
    return pl.pallas_call(
        step_kernel,
        in_specs=[hbm] * 5,
        out_specs=[hbm] * 5,
        out_shape=[jax.ShapeDtypeStruct((seq, hid), bf)] * 2 + [jax.ShapeDtypeStruct(b.shape, bf) for b in (x_blk, w_blk, wo_blk)],
        scratch_shapes=[
            pltpu.VMEM((hid, w_loc), bf), pltpu.VMEM((2, t_loc, hid), bf), pltpu.VMEM((2, seq, t_loc), bf),
            pltpu.VMEM((ow, hid), bf), pltpu.VMEM((seq, hw), bf), pltpu.VMEM((seq, ow), bf),
            pltpu.VMEM((4,) + seg_blk.shape, jnp.int32),
            pltpu.VMEM((seq, t_loc), f32), pltpu.VMEM((seq, t_loc), f32), pltpu.VMEM((seq // BK, 1, t_loc), f32),
            pltpu.VMEM((heads, D, seq), bf), pltpu.VMEM((heads, D, seq), bf),
            pltpu.VMEM((heads, seq, D), f32), pltpu.VMEM((heads, seq, D), f32),
            pltpu.VMEM((seq, hw), bf), pltpu.VMEM((seq, ow), bf),
            pltpu.VMEM((t_loc, w_loc), bf), pltpu.VMEM((ow, hid), bf), pltpu.VMEM((2 * t_loc, t_loc), f32),
            pltpu.VMEM((t_loc, h_loc), bf), pltpu.VMEM((ow, h_loc), bf),
            pltpu.SemaphoreType.DMA((n_sem,)), pltpu.SemaphoreType.DMA((n_sem,)), pltpu.SemaphoreType.DMA((16,)),
        ],
        compiler_params=pltpu.CompilerParams(collective_id=0, has_side_effects=True, vmem_limit_bytes=VMEM_LIMIT),
        name='mega_step',
    )(x_blk, w_blk, wo_blk, seg_blk, dy_blk)


def copy_kernel(parts, *refs):
    n = len(parts)
    ins, outs, bufs, sem_in, sem_out = refs[:n], refs[n:2 * n], refs[2 * n:3 * n], refs[3 * n], refs[3 * n + 1]
    moves = []
    for i in range(n):
        step = ins[i].shape[0] // parts[i]
        for j in range(parts[i]):
            rows = pl.ds(j * step, step)
            load = pltpu.make_async_copy(ins[i].at[rows], bufs[i].at[rows], sem_in.at[len(moves)])
            load.start()
            moves.append((load, pltpu.make_async_copy(bufs[i].at[rows], outs[i].at[rows], sem_out.at[len(moves)])))
    for load, store in moves:
        load.wait()
        store.start()
    for _, store in moves:
        store.wait()


def copy_out(*arrays):
    parts = [a.shape[0] // 128 for a in arrays]
    hbm = pl.BlockSpec(memory_space=pl.ANY)
    shapes = [jax.ShapeDtypeStruct(a.shape, a.dtype) for a in arrays]
    return pl.pallas_call(
        functools.partial(copy_kernel, parts),
        in_specs=[hbm] * len(arrays),
        out_specs=[hbm] * len(arrays),
        out_shape=shapes,
        scratch_shapes=[pltpu.VMEM(a.shape, a.dtype) for a in arrays] + [pltpu.SemaphoreType.DMA((sum(parts),))] * 2,
        compiler_params=pltpu.CompilerParams(vmem_limit_bytes=VMEM_LIMIT),
        name='copy_out',
    )(*arrays)


def solution(mesh):
    tok_spec = P(('dp', 'row'), 'col')
    mat_spec = P('row', 'col')
    seg_spec = P(('dp', 'row'))

    def grad_step(x_blk, wqkv_blk, wout_blk, seg_blk, dy_blk):
        _, _, grad_x, grad_wqkv, grad_wout = step_all(x_blk, wqkv_blk, wout_blk, seg_blk.reshape(4, -1), dy_blk)
        return copy_out(grad_x, grad_wqkv, grad_wout)

    return jax.shard_map(grad_step, mesh=mesh, in_specs=(tok_spec, mat_spec, mat_spec, seg_spec, tok_spec), out_specs=(tok_spec, tok_spec, tok_spec), check_vma=False)
```

```python
import functools

import jax
import jax.numpy as jnp
from jax import lax
from jax.experimental import pallas as pl
from jax.experimental.pallas import tpu as pltpu
from jax.sharding import PartitionSpec as P

NT = (((1,), (1,)), ((), ()))
TN = (((0,), (0,)), ((), ()))
MESH = pl.DeviceIdType.MESH
BK = 512
D = 128
NC = 2
NJ = 2
LOW = -3.0e38
VMEM_LIMIT = 66_000_000
STEP_LIMIT = 57_000_000


def mult(i, n):
    return pl.multiple_of(i * n, n)


def attention_block(q0, bq, h, c1, c2, qkv_v, do_v, p_scr, dp_scr, m_scr, kt, vt, dk_acc, dv_acc, dqkv_v, o_v, between):
    seq = qkv_v.shape[0]
    scale = D ** -0.5
    to_exp2 = scale * 1.4426950408889634
    f32 = jnp.float32
    rows = pl.ds(q0, bq)
    c0 = 3 * D * h
    iq = q0 + lax.broadcasted_iota(jnp.int32, (1, bq), 1)
    q_doc = (iq >= c1).astype(jnp.int32) + (iq >= c2).astype(jnp.int32)
    q = qkv_v[rows, c0:c0 + D]
    do = do_v[rows, D * h:D * h + D]

    def first(kb, carry):
        m, l, dd = carry
        k0 = pl.multiple_of(kb * BK, BK)
        keys = pl.ds(k0, BK)
        ik = k0 + lax.broadcasted_iota(jnp.int32, (BK, 1), 0)
        k_doc = (ik >= c1).astype(jnp.int32) + (ik >= c2).astype(jnp.int32)
        s = lax.dot_general(qkv_v[keys, c0 + D:c0 + 2 * D], q, NT, preferred_element_type=f32)
        s = jnp.where(q_doc == k_doc, s, LOW)
        dp = lax.dot_general(qkv_v[keys, c0 + 2 * D:c0 + 3 * D], do, NT, preferred_element_type=f32)
        dp_scr[keys, :] = dp
        m_new = jnp.maximum(m, jnp.max(s, axis=0, keepdims=True))
        p = jnp.exp2((s - m_new) * to_exp2)
        p_scr[keys, :] = p
        m_scr[kb] = m_new
        alpha = jnp.exp2((m - m_new) * to_exp2)
        return m_new, alpha * l + jnp.sum(p, axis=0, keepdims=True), alpha * dd + jnp.sum(p * dp, axis=0, keepdims=True)

    zero = jnp.zeros((1, bq), f32)
    m, l, dd = lax.fori_loop(0, seq // BK, first, (jnp.full((1, bq), LOW, f32), zero, zero))
    if between is not None:
        between()
    inv = 1.0 / l
    row_dot = dd * inv

    def second(kb, acc):
        o, dq = acc
        keys = pl.ds(pl.multiple_of(kb * BK, BK), BK)
        f = jnp.exp2((m_scr[kb] - m) * to_exp2) * inv
        p = p_scr[keys, :]
        p_bf = (p * f).astype(jnp.bfloat16)
        ds = ((p * (f * scale)) * (dp_scr[keys, :] - row_dot)).astype(jnp.bfloat16)
        o = o + jnp.dot(vt[h, :, keys], p_bf, preferred_element_type=f32)
        dq = dq + jnp.dot(kt[h, :, keys], ds, preferred_element_type=f32)
        dk_acc[h, keys, :] += jnp.dot(ds, q, preferred_element_type=f32)
        dv_acc[h, keys, :] += jnp.dot(p_bf, do, preferred_element_type=f32)
        return o, dq

    zacc = jnp.zeros((D, bq), f32)
    o, dq = lax.fori_loop(0, seq // BK, second, (zacc, zacc))
    o_v[rows, D * h:D * h + D] = o.T.astype(jnp.bfloat16)
    dqkv_v[rows, c0:c0 + D] = dq.T.astype(jnp.bfloat16)


def step_kernel(x_ref, w_ref, wo_ref, seg_ref, dy_ref, xg, dyg, dx_out, dw_out, dwo_out,
                w_v, tok, col_v, woh, qkv_v, do_v, seg_v, p_scr, dp_scr, m_scr, kt, vt, dk_acc, dv_acc, dqkv_v, o_v,
                dtok, dwo_v, px_recv, relay, ssem, rsem, lsem):
    y = lax.axis_index('col')
    r = lax.axis_index('row')
    x = r // 2
    c = lax.rem(r, 2)
    r_s = r + 1 - 2 * c
    r_x = lax.rem(r + 2, 4)
    r_xs = lax.rem(r_s + 2, 4)
    sib, xn, yn = {'row': r_s}, {'row': r_x}, {'col': 1 - y}
    t_loc, h_loc = x_ref.shape
    hw = qkv_v.shape[1]
    ow = woh.shape[0]
    heads = ow // D
    ct, bt = t_loc // NC, t_loc // NJ
    f32, bf = jnp.float32, jnp.bfloat16
    started = []
    XB, YB, WB = 0, 7 * NC, 14 * NC
    WOB = WB + 12
    SGB = WOB + 2
    DQ = SGB + 3
    DW = DQ + 3 + 3 * NJ
    DWO = DW + 3
    PX = DWO + 2
    DWF = PX + NJ
    DWG = DWF + 1
    DQE = DWG + 2

    def copy(i, k, src, dst, dev):
        return pltpu.make_async_remote_copy(src, dst, ssem.at[i], rsem.at[k], device_id=dev, device_id_type=MESH)

    def send(i, src, dst, dev):
        cp = copy(i, i, src, dst, dev)
        cp.start()
        started.append(cp)

    def recv(i, dst):
        copy(i, i, dst, dst, sib).wait_recv()

    def local(i, src, dst):
        cp = pltpu.make_async_copy(src, dst, lsem.at[i])
        cp.start()
        return cp

    def slot(g, yy, rr, j):
        return g.at[pl.ds(pl.multiple_of(rr * t_loc + j * ct, ct), ct), pl.ds(mult(yy, h_loc), h_loc)]

    def tid(base, kind, j):
        return base + kind * NC + j

    def got_from(kind):
        return ((y, r_s), (y, r_x), (1 - y, r), (y, r_xs), (1 - y, r_x), (1 - y, r_s), (1 - y, r_xs))[kind]

    def send_own(a, g, base, kind, dev):
        for j in range(NC):
            send(tid(base, kind, j), a.at[pl.ds(j * ct, ct)], slot(g, y, r, j), dev)

    def forward(g, base, kind_in, outs, j):
        yy, rr = got_from(kind_in)
        recv(tid(base, kind_in, j), slot(g, yy, rr, j))
        for kind_out, dev in outs:
            send(tid(base, kind_out, j), slot(g, yy, rr, j), slot(g, yy, rr, j), dev)

    def take(g, base, kind):
        yy, rr = got_from(kind)
        for j in range(NC):
            recv(tid(base, kind, j), slot(g, yy, rr, j))

    def wslot(rr, q):
        return w_v.at[pl.ds(mult(rr, t_loc), t_loc), pl.ds(mult(q, hw), hw)]

    def wq(t, xx):
        return lax.rem(2 * xx + t, 4)

    def w_own(t, kind, xx, dev):
        q = wq(t, xx)
        send(WB + 4 * kind + t, w_ref.at[:, pl.ds(mult(q, hw), hw)], wslot(r, q), dev)

    def w_forward(t):
        q = wq(t, x)
        recv(WB + 4 + t, wslot(r_x, q))
        send(WB + 8 + t, wslot(r_x, q), wslot(r_x, q), sib)

    barrier = pltpu.get_barrier_semaphore()
    for i in range(1, 8):
        pl.semaphore_signal(barrier, inc=1, device_id={'row': lax.rem(r + i, 4), 'col': lax.rem(y + i // 4, 2)}, device_id_type=MESH)
    pl.semaphore_wait(barrier, 7)

    send_own(x_ref, xg, XB, 1, xn)
    send_own(x_ref, xg, XB, 2, yn)
    for t in range(2):
        w_own(t, 1, 1 - x, xn)
    send_own(x_ref, xg, XB, 0, sib)
    for t in range(4):
        w_own(t, 0, x, sib)
    for i, (rr, dev) in enumerate(((r_s, sib), (r_x, xn), (r_xs, {'row': r_xs}))):
        send(SGB + i, seg_ref, seg_v.at[r], dev)

    a = local(1, x_ref, tok.at[0, :, pl.ds(0, h_loc)])
    b = local(2, dy_ref, tok.at[1, :, pl.ds(0, h_loc)])
    d = local(3, w_ref, w_v.at[pl.ds(mult(r, t_loc), t_loc)])
    sg = local(4, seg_ref, seg_v.at[r])
    own_slot = lambda g: g.at[pl.ds(mult(r, t_loc), t_loc), pl.ds(mult(y, h_loc), h_loc)]
    a.wait()
    a = local(1, tok.at[0, :, pl.ds(0, h_loc)], own_slot(xg))
    b.wait()
    b = local(2, tok.at[1, :, pl.ds(0, h_loc)], own_slot(dyg))
    dk_acc[...] = jnp.zeros_like(dk_acc)
    dv_acc[...] = jnp.zeros_like(dv_acc)

    for j in range(NC):
        forward(xg, XB, 1, ((4, yn), (3, sib)), j)
        forward(xg, XB, 2, ((5, sib),), j)
    for k in range(2):
        row_to = 2 * c + k
        src = wo_ref.at[pl.ds(k * ow, ow)]
        dst = woh.at[:, pl.ds(mult(y, h_loc), h_loc)]
        mine = (x == y) & (row_to == r)

        @pl.when(mine)
        def _():
            pltpu.make_async_copy(src, dst, lsem.at[0]).start()

        @pl.when(jnp.logical_not(mine))
        def _():
            copy(WOB + k, WOB + y, src, dst, {'col': x, 'row': row_to}).start()
    send_own(dy_ref, dyg, YB, 2, yn)
    send_own(dy_ref, dyg, YB, 1, xn)
    send_own(dy_ref, dyg, YB, 0, sib)
    w_forward(0)
    for j in range(NC):
        forward(xg, XB, 4, ((6, sib),), j)
    a.wait()
    b.wait()
    d.wait()
    sg.wait()

    def load_tok(g, rr, s):
        return local(8 + s, g.at[pl.ds(mult(rr, t_loc), t_loc)], tok.at[s])

    def load_half(g, yy, rr, s, i):
        cols = pl.ds(mult(yy, h_loc), h_loc)
        return local(i, g.at[pl.ds(mult(rr, t_loc), t_loc), cols], tok.at[s, :, cols])

    blocks = (r, r_s, r_x, r_xs)
    for kind in (0, 3, 5, 6):
        take(xg, XB, kind)
    loads = [load_tok(xg, blocks[i], i) for i in range(2)]
    w_forward(1)
    for t in range(4):
        recv(WB + t, wslot(r_s, wq(t, x)))
    for t in range(2):
        recv(WB + 8 + t, wslot(r_xs, wq(t, x)))
    for i in range(4):
        loads[i].wait()
        rows = pl.ds(mult(blocks[i], t_loc), t_loc)
        for n in range(hw // 256):
            mine = w_v[:, pl.ds(pl.multiple_of(r * hw + 256 * n, 256), 256)]
            qkv_v[rows, 256 * n:256 * n + 256] = jnp.dot(tok[i % 2], mine, preferred_element_type=f32).astype(bf)
        if i < 2:
            loads.append(load_tok(xg, blocks[i + 2], i))
        for h in range(heads):
            kt[h, :, rows] = qkv_v[rows, 3 * D * h + D:3 * D * h + 2 * D].T
            vt[h, :, rows] = qkv_v[rows, 3 * D * h + 2 * D:3 * D * h + 3 * D].T

    near_half = load_half(dyg, y, r, 0, 10)
    for i, rr in enumerate((r_s, r_x, r_xs)):
        recv(SGB + i, seg_v.at[rr])
    c1 = jnp.sum((seg_v[...] < 1).astype(jnp.int32))
    c2 = jnp.sum((seg_v[...] < 2).astype(jnp.int32))
    for j in range(NC):
        forward(dyg, YB, 2, ((5, sib),), j)
    far_half = load_half(dyg, 1 - y, r, 0, 11)
    for yy in range(2):
        piece = woh.at[:, pl.ds(yy * h_loc, h_loc)]
        mine = (y == yy) & (2 * y + x == r)

        @pl.when(mine)
        def _():
            pltpu.make_async_copy(wo_ref.at[pl.ds(0, ow)], piece, lsem.at[0]).wait()

        @pl.when(jnp.logical_not(mine))
        def _():
            recv(WOB + yy, piece)

    def d_out(i, s):
        rows = pl.ds(mult(blocks[i], t_loc), t_loc)
        do_v[rows, :] = lax.dot_general(tok[s], woh[...], NT, preferred_element_type=f32).astype(bf)

    def attend(i, h, between=None):
        attention_block(mult(blocks[i], t_loc), t_loc, h, c1, c2, qkv_v, do_v, p_scr, dp_scr, m_scr, kt, vt, dk_acc, dv_acc, dqkv_v, o_v, between)

    def dy_forward(j):
        forward(dyg, YB, 1, ((4, yn), (3, sib)), j)

    near_half.wait()
    far_half.wait()
    d_out(0, 0)
    attend(0, 0, lambda: dy_forward(0))
    for t in range(2, 4):
        w_own(t, 1, 1 - x, xn)
    others = (r_s, r_x, r_xs)

    def finish(h):
        c0 = 3 * D * h
        dqkv_v[:, c0 + D:c0 + 2 * D] = dk_acc[h].astype(bf)
        dqkv_v[:, c0 + 2 * D:c0 + 3 * D] = dv_acc[h].astype(bf)

    def tok_slot(rr, h, j, n, c0=0, c1=3 * D):
        return dtok.at[pl.ds(j * n, n), pl.ds(pl.multiple_of(rr * hw + 3 * D * h + c0, D), c1 - c0)]

    def send_dqkv(i, h, j, n):
        for k in (1, 2, 0):
            c0 = D if (h, k) == (0, 1) else 0
            src = dqkv_v.at[pl.ds(pl.multiple_of(others[k] * t_loc + j * n, n), n), pl.ds(3 * D * h + c0, 3 * D - c0)]
            send(i + k, src, tok_slot(r, h, j, n, c0), {'row': others[k]})

    def send_early_dq():
        src = dqkv_v.at[pl.ds(mult(r_x, t_loc), t_loc), pl.ds(0, D)]
        send(DQE, src, tok_slot(r, 0, 0, t_loc, 0, D), xn)

    loading = []

    def second_block():
        dy_forward(1)
        for kind in (0, 5):
            take(dyg, YB, kind)
        loading.append(load_tok(dyg, r_s, 1))

    def last_block():
        take(dyg, YB, 3)
        take(dyg, YB, 6)
        loading.append(load_tok(dyg, r_xs, 1))

    attend(0, 1, second_block)
    loading.pop().wait()
    d_out(1, 1)
    attend(1, 0)
    forward(dyg, YB, 4, ((6, sib),), 0)
    near_half = load_half(dyg, y, r_x, 0, 10)
    attend(1, 1)
    forward(dyg, YB, 4, ((6, sib),), 1)
    far_half = load_half(dyg, 1 - y, r_x, 0, 11)
    near_half.wait()
    far_half.wait()
    d_out(2, 0)
    attend(2, 0, last_block)
    send_early_dq()
    w_forward(2)
    loading.pop().wait()
    d_out(3, 1)
    ld = [local(5 + s, dyg.at[:, pl.ds(512 * s, 512)], col_v.at[s]) for s in range(2)]
    attend(3, 0)

    finish(0)
    send_dqkv(DQ, 0, 0, t_loc)
    attend(2, 1)
    w_forward(3)
    attend(3, 1)
    finish(1)
    for j in range(NJ):
        send_dqkv(DQ + 3 + 3 * j, 1, j, bt)
    dtok[:, pl.ds(mult(r, hw), hw)] = dqkv_v[pl.ds(mult(r, t_loc), t_loc), :]

    order = (r_x, r_xs, r_s, r)
    for s in range(4):
        ld[s].wait()
        dwo_v[:, 512 * s:512 * s + 512] = lax.dot_general(o_v[...], col_v[s % 2], TN, preferred_element_type=f32).astype(bf)
        if s < 2:
            ld.append(local(5 + s, dyg.at[:, pl.ds(512 * s + 1024, 512)], col_v.at[s]))
        else:
            ld.append(local(5 + s - 2, xg.at[:, pl.ds(mult(order[s - 2], t_loc), t_loc)], col_v.at[s - 2]))
    ld = ld[4:]
    row_to = 2 * y + x
    near = x == y
    for k in range(2):
        src = dwo_v.at[:, pl.ds(k * h_loc, h_loc)]
        dst = dwo_out.at[pl.ds(mult(c, ow), ow)]
        mine = (y == k) & (row_to == r)
        far = (y != k) & (x != y)

        @pl.when(mine)
        def _():
            pltpu.make_async_copy(src, dst, lsem.at[0]).start()

        @pl.when(far)
        def _():
            copy(DWF, DWF, src, relay, {'col': k}).start()

        @pl.when(jnp.logical_not(mine | far))
        def _():
            copy(DWO + k, DWO + c, src, dst, {'col': k, 'row': row_to}).start()

    def dw_slot(rr):
        return dw_out.at[:, pl.ds(mult(rr, hw), hw)]

    def d_w(i):
        s = i % 2
        ld[i].wait()
        part = lax.dot_general(col_v[s], dqkv_v[...], TN, preferred_element_type=f32).astype(bf)
        if i < 3:
            qkv_v[t_loc * i:t_loc * i + t_loc, :] = part
        else:
            dw_out[:, pl.ds(mult(r, hw), hw)] = part
        if i < 2:
            ld.append(local(5 + s, xg.at[:, pl.ds(mult(order[i + 2], t_loc), t_loc)], col_v.at[s]))

    def send_dw(i, k):
        send(DW + k, qkv_v.at[pl.ds(t_loc * i, t_loc)], dw_slot(r), {'row': others[k]})

    def d_x(j, half, dst):
        for n in range(h_loc // 256):
            rows = pl.ds(pl.multiple_of(half * h_loc + 256 * n, 256), 256)
            dst[pl.ds(2 * bt * j + bt * (n // 2), bt), 256 * (n % 2):256 * (n % 2) + 256] = lax.dot_general(
                dtok[pl.ds(j * bt, bt), :], w_v[rows, :], NT, preferred_element_type=f32)

    def d_x_send(j):
        for k in range(3):
            recv(DQ + 3 + 3 * j + k, tok_slot(others[k], 1, j, bt))
        d_x(j, 1 - y, dp_scr)
        part = pl.ds(2 * bt * j, 2 * bt)
        send(PX + j, dp_scr.at[part], px_recv.at[part], yn)

    d_w(0)
    send_dw(0, 1)
    d_w(1)
    send_dw(1, 2)
    for t in range(2, 4):
        recv(WB + 8 + t, wslot(r_xs, wq(t, x)))
    recv(DQE, tok_slot(r_x, 0, 0, t_loc, 0, D))
    for k in range(3):
        recv(DQ + k, tok_slot(others[k], 0, 0, t_loc, D if k == 1 else 0))
    d_x_send(0)

    @pl.when(near)
    def _():
        recv(DWF, relay)
        copy(DWG, DWG + c, relay, dwo_out.at[pl.ds(mult(c, ow), ow)], {'row': 2 * (1 - y) + x}).start()

    d_w(2)
    send_dw(2, 0)
    d_x_send(1)
    d_x(0, y, p_scr)
    d_w(3)
    d_x(1, y, p_scr)
    for j in range(NJ):
        recv(PX + j, px_recv.at[pl.ds(2 * bt * j, 2 * bt)])
        for q in range(2):
            part = pl.ds(2 * bt * j + bt * q, bt)
            dx_out[pl.ds(j * bt, bt), 512 * q:512 * q + 512] = (p_scr[part, :] + px_recv[part, :]).astype(bf)
    for k in range(3):
        recv(DW + k, dw_slot(others[k]))
    src_col, src_x = r // 2, lax.rem(r, 2)
    for k in range(2):
        piece = dwo_out.at[pl.ds(k * ow, ow)]
        mine = (src_col == y) & (2 * src_x + k == r)
        far = (src_col != y) & (src_x != src_col)

        @pl.when(mine)
        def _():
            pltpu.make_async_copy(dwo_v.at[:, pl.ds(0, h_loc)], piece, lsem.at[0]).wait()

        @pl.when(far)
        def _():
            recv(DWG + k, piece)

        @pl.when(jnp.logical_not(mine | far))
        def _():
            recv(DWO + k, piece)
    for cp in started:
        cp.wait_send()
    half = dwo_v.at[:, pl.ds(0, h_loc)]
    for k in range(2):
        @pl.when(jnp.logical_not((x == y) & (2 * c + k == r)))
        def _():
            copy(WOB + k, WOB + k, wo_ref.at[pl.ds(0, ow)], half, sib).wait_send()

        @pl.when(jnp.logical_not(((y == k) & (row_to == r)) | ((y != k) & (x != y))))
        def _():
            copy(DWO + k, DWO + k, half, relay, sib).wait_send()

    @pl.when(jnp.logical_not(near))
    def _():
        copy(DWF, DWF, half, relay, yn).wait_send()

    @pl.when(near)
    def _():
        copy(DWG, DWG, relay, relay, sib).wait_send()


def step_all(x_blk, w_blk, wo_blk, seg_blk, dy_blk):
    t_loc, h_loc = x_blk.shape
    w_loc = w_blk.shape[1]
    seq, hid = 4 * t_loc, 2 * h_loc
    hw, ow = w_loc // 4, w_loc // 12
    heads = ow // D
    bf, f32 = jnp.bfloat16, jnp.float32
    hbm = pl.BlockSpec(memory_space=pl.ANY)
    n_sem = 14 * NC + 12 + 2 + 3 + 3 + 3 * NJ + 3 + 2 + NJ + 1 + 2 + 1
    return pl.pallas_call(
        step_kernel,
        in_specs=[hbm] * 5,
        out_specs=[hbm] * 2 + [pl.BlockSpec(memory_space=pltpu.VMEM)] * 3,
        out_shape=[jax.ShapeDtypeStruct((seq, hid), bf)] * 2 + [pltpu.VMEM(b.shape, bf) for b in (x_blk, w_blk, wo_blk)],
        scratch_shapes=[
            pltpu.VMEM((hid, w_loc), bf), pltpu.VMEM((2, t_loc, hid), bf), pltpu.VMEM((2, seq, t_loc), bf),
            pltpu.VMEM((ow, hid), bf), pltpu.VMEM((seq, hw), bf), pltpu.VMEM((seq, ow), bf),
            pltpu.VMEM((4,) + seg_blk.shape, jnp.int32),
            pltpu.VMEM((seq, t_loc), f32), pltpu.VMEM((seq, t_loc), f32), pltpu.VMEM((seq // BK, 1, t_loc), f32),
            pltpu.VMEM((heads, D, seq), bf), pltpu.VMEM((heads, D, seq), bf),
            pltpu.VMEM((heads, seq, D), f32), pltpu.VMEM((heads, seq, D), f32),
            pltpu.VMEM((seq, hw), bf), pltpu.VMEM((seq, ow), bf),
            pltpu.VMEM((t_loc, w_loc), bf), pltpu.VMEM((ow, hid), bf), pltpu.VMEM((2 * t_loc, t_loc), f32),
            pltpu.VMEM((ow, h_loc), bf),
            pltpu.SemaphoreType.DMA((n_sem,)), pltpu.SemaphoreType.DMA((n_sem,)), pltpu.SemaphoreType.DMA((16,)),
        ],
        compiler_params=pltpu.CompilerParams(collective_id=0, has_side_effects=True, vmem_limit_bytes=STEP_LIMIT),
        name='mega_step',
    )(x_blk, w_blk, wo_blk, seg_blk, dy_blk)


def copy_kernel(parts, *refs):
    n = len(parts)
    ins, outs, sem = refs[:n], refs[n:2 * n], refs[2 * n]
    moves = []
    for i in range(n):
        step = ins[i].shape[0] // parts[i]
        for j in range(parts[i]):
            rows = pl.ds(j * step, step)
            move = pltpu.make_async_copy(ins[i].at[rows], outs[i].at[rows], sem.at[len(moves)])
            move.start()
            moves.append(move)
    for move in moves:
        move.wait()


def copy_out(*arrays):
    parts = [a.shape[0] // 128 for a in arrays]
    return pl.pallas_call(
        functools.partial(copy_kernel, parts),
        in_specs=[pl.BlockSpec(memory_space=pltpu.VMEM)] * len(arrays),
        out_specs=[pl.BlockSpec(memory_space=pl.ANY)] * len(arrays),
        out_shape=[jax.ShapeDtypeStruct(a.shape, a.dtype) for a in arrays],
        scratch_shapes=[pltpu.SemaphoreType.DMA((sum(parts),))],
        compiler_params=pltpu.CompilerParams(vmem_limit_bytes=1_000_000),
        name='copy_out',
    )(*arrays)


def solution(mesh):
    tok_spec = P(('dp', 'row'), 'col')
    mat_spec = P('row', 'col')
    seg_spec = P(('dp', 'row'))

    def grad_step(x_blk, wqkv_blk, wout_blk, seg_blk, dy_blk):
        _, _, grad_x, grad_wqkv, grad_wout = step_all(x_blk, wqkv_blk, wout_blk, seg_blk.reshape(4, -1), dy_blk)
        return copy_out(grad_x, grad_wqkv, grad_wout)

    return jax.shard_map(grad_step, mesh=mesh, in_specs=(tok_spec, mat_spec, mat_spec, seg_spec, tok_spec), out_specs=(tok_spec, tok_spec, tok_spec), check_vma=False)
```

```python
import functools

import jax
import jax.numpy as jnp
from jax import lax
from jax.experimental import pallas as pl
from jax.experimental.pallas import tpu as pltpu
from jax.sharding import PartitionSpec as P

NT = (((1,), (1,)), ((), ()))
TN = (((0,), (0,)), ((), ()))
MESH = pl.DeviceIdType.MESH
BK = 512
D = 128
NC = 2
NJ = 2
LOW = -3.0e38
VMEM_LIMIT = 66_000_000
STEP_LIMIT = 57_000_000


def mult(i, n):
    return pl.multiple_of(i * n, n)


def attention_block(q0, bq, h, c1, c2, qkv_v, do_v, p_scr, dp_scr, m_scr, kt, vt, dk_acc, dv_acc, dqkv_v, o_v, between):
    seq = qkv_v.shape[0]
    scale = D ** -0.5
    to_exp2 = scale * 1.4426950408889634
    f32 = jnp.float32
    rows = pl.ds(q0, bq)
    c0 = 3 * D * h
    iq = q0 + lax.broadcasted_iota(jnp.int32, (1, bq), 1)
    q_doc = (iq >= c1).astype(jnp.int32) + (iq >= c2).astype(jnp.int32)
    q = qkv_v[rows, c0:c0 + D]
    do = do_v[rows, D * h:D * h + D]

    def first(kb, carry):
        m, l, dd = carry
        k0 = pl.multiple_of(kb * BK, BK)
        keys = pl.ds(k0, BK)
        ik = k0 + lax.broadcasted_iota(jnp.int32, (BK, 1), 0)
        k_doc = (ik >= c1).astype(jnp.int32) + (ik >= c2).astype(jnp.int32)
        s = lax.dot_general(qkv_v[keys, c0 + D:c0 + 2 * D], q, NT, preferred_element_type=f32)
        s = jnp.where(q_doc == k_doc, s, LOW)
        dp = lax.dot_general(qkv_v[keys, c0 + 2 * D:c0 + 3 * D], do, NT, preferred_element_type=f32)
        dp_scr[keys, :] = dp
        m_new = jnp.maximum(m, jnp.max(s, axis=0, keepdims=True))
        p = jnp.exp2((s - m_new) * to_exp2)
        p_scr[keys, :] = p
        m_scr[kb] = m_new
        alpha = jnp.exp2((m - m_new) * to_exp2)
        return m_new, alpha * l + jnp.sum(p, axis=0, keepdims=True), alpha * dd + jnp.sum(p * dp, axis=0, keepdims=True)

    zero = jnp.zeros((1, bq), f32)
    m, l, dd = lax.fori_loop(0, seq // BK, first, (jnp.full((1, bq), LOW, f32), zero, zero))
    if between is not None:
        between()
    inv = 1.0 / l
    row_dot = dd * inv

    def second(kb, acc):
        o, dq = acc
        keys = pl.ds(pl.multiple_of(kb * BK, BK), BK)
        f = jnp.exp2((m_scr[kb] - m) * to_exp2) * inv
        p = p_scr[keys, :]
        p_bf = (p * f).astype(jnp.bfloat16)
        ds = ((p * (f * scale)) * (dp_scr[keys, :] - row_dot)).astype(jnp.bfloat16)
        o = o + jnp.dot(vt[h, :, keys], p_bf, preferred_element_type=f32)
        dq = dq + jnp.dot(kt[h, :, keys], ds, preferred_element_type=f32)
        dk_acc[h, keys, :] += jnp.dot(ds, q, preferred_element_type=f32)
        dv_acc[h, keys, :] += jnp.dot(p_bf, do, preferred_element_type=f32)
        return o, dq

    zacc = jnp.zeros((D, bq), f32)
    o, dq = lax.fori_loop(0, seq // BK, second, (zacc, zacc))
    o_v[rows, D * h:D * h + D] = o.T.astype(jnp.bfloat16)
    dqkv_v[rows, c0:c0 + D] = dq.T.astype(jnp.bfloat16)


def step_kernel(x_ref, w_ref, wo_ref, seg_ref, dy_ref, xg, dyg, dx_out, dw_out, dwo_out,
                w_v, tok, col_v, woh, qkv_v, do_v, seg_v, p_scr, dp_scr, m_scr, kt, vt, dk_acc, dv_acc, dqkv_v, o_v,
                dtok, dwo_v, px_recv, relay, ssem, rsem, lsem):
    y = lax.axis_index('col')
    r = lax.axis_index('row')
    x = r // 2
    c = lax.rem(r, 2)
    r_s = r + 1 - 2 * c
    r_x = lax.rem(r + 2, 4)
    r_xs = lax.rem(r_s + 2, 4)
    sib, xn, yn = {'row': r_s}, {'row': r_x}, {'col': 1 - y}
    t_loc, h_loc = x_ref.shape
    hw = qkv_v.shape[1]
    ow = woh.shape[0]
    heads = ow // D
    ct, bt = t_loc // NC, t_loc // NJ
    f32, bf = jnp.float32, jnp.bfloat16
    started = []
    XB, YB, WB = 0, 7 * NC, 14 * NC
    WOB = WB + 12
    SGB = WOB + 2
    DQ = SGB + 3
    DW = DQ + 3 + 3 * NJ
    DWO = DW + 3
    PX = DWO + 2
    DWF = PX + NJ
    DWG = DWF + 1
    DQE = DWG + 2

    def copy(i, k, src, dst, dev):
        return pltpu.make_async_remote_copy(src, dst, ssem.at[i], rsem.at[k], device_id=dev, device_id_type=MESH)

    def send(i, src, dst, dev):
        cp = copy(i, i, src, dst, dev)
        cp.start()
        started.append(cp)

    def recv(i, dst):
        copy(i, i, dst, dst, sib).wait_recv()

    def local(i, src, dst):
        cp = pltpu.make_async_copy(src, dst, lsem.at[i])
        cp.start()
        return cp

    def slot(g, yy, rr, j):
        return g.at[pl.ds(pl.multiple_of(rr * t_loc + j * ct, ct), ct), pl.ds(mult(yy, h_loc), h_loc)]

    def tid(base, kind, j):
        return base + kind * NC + j

    def got_from(kind):
        return ((y, r_s), (y, r_x), (1 - y, r), (y, r_xs), (1 - y, r_x), (1 - y, r_s), (1 - y, r_xs))[kind]

    def send_own(a, g, base, kind, dev):
        for j in range(NC):
            send(tid(base, kind, j), a.at[pl.ds(j * ct, ct)], slot(g, y, r, j), dev)

    def forward(g, base, kind_in, outs, j):
        yy, rr = got_from(kind_in)
        recv(tid(base, kind_in, j), slot(g, yy, rr, j))
        for kind_out, dev in outs:
            send(tid(base, kind_out, j), slot(g, yy, rr, j), slot(g, yy, rr, j), dev)

    def take(g, base, kind):
        yy, rr = got_from(kind)
        for j in range(NC):
            recv(tid(base, kind, j), slot(g, yy, rr, j))

    def wslot(rr, q):
        return w_v.at[pl.ds(mult(rr, t_loc), t_loc), pl.ds(mult(q, hw), hw)]

    def wq(t, xx):
        return lax.rem(2 * xx + t, 4)

    def w_own(t, kind, xx, dev):
        q = wq(t, xx)
        send(WB + 4 * kind + t, w_ref.at[:, pl.ds(mult(q, hw), hw)], wslot(r, q), dev)

    def w_forward(t):
        q = wq(t, x)
        recv(WB + 4 + t, wslot(r_x, q))
        send(WB + 8 + t, wslot(r_x, q), wslot(r_x, q), sib)

    barrier = pltpu.get_barrier_semaphore()
    for dev in (xn, yn, sib):
        pl.semaphore_signal(barrier, inc=1, device_id=dev, device_id_type=MESH)
    pl.semaphore_wait(barrier, 3)

    send_own(x_ref, xg, XB, 1, xn)
    send_own(x_ref, xg, XB, 2, yn)
    for t in range(2):
        w_own(t, 1, 1 - x, xn)
    send_own(x_ref, xg, XB, 0, sib)
    for t in range(4):
        w_own(t, 0, x, sib)
    send(SGB, seg_ref, seg_v.at[r], sib)
    send(SGB + 1, seg_ref, seg_v.at[r], xn)

    a = local(1, x_ref, tok.at[0, :, pl.ds(0, h_loc)])
    b = local(2, dy_ref, tok.at[1, :, pl.ds(0, h_loc)])
    d = local(3, w_ref, w_v.at[pl.ds(mult(r, t_loc), t_loc)])
    sg = local(4, seg_ref, seg_v.at[r])
    own_slot = lambda g: g.at[pl.ds(mult(r, t_loc), t_loc), pl.ds(mult(y, h_loc), h_loc)]
    a.wait()
    a = local(1, tok.at[0, :, pl.ds(0, h_loc)], own_slot(xg))
    b.wait()
    b = local(2, tok.at[1, :, pl.ds(0, h_loc)], own_slot(dyg))
    dk_acc[...] = jnp.zeros_like(dk_acc)
    dv_acc[...] = jnp.zeros_like(dv_acc)

    for j in range(NC):
        forward(xg, XB, 1, ((4, yn), (3, sib)), j)
        forward(xg, XB, 2, ((5, sib),), j)
    take(xg, XB, 5)
    send(SGB + 2, seg_ref, seg_v.at[r], {'row': r_xs})
    for k in range(2):
        row_to = 2 * c + k
        src = wo_ref.at[pl.ds(k * ow, ow)]
        dst = woh.at[:, pl.ds(mult(y, h_loc), h_loc)]
        mine = (x == y) & (row_to == r)

        @pl.when(mine)
        def _():
            pltpu.make_async_copy(src, dst, lsem.at[0]).start()

        @pl.when(jnp.logical_not(mine))
        def _():
            copy(WOB + k, WOB + y, src, dst, {'col': x, 'row': row_to}).start()
    send_own(dy_ref, dyg, YB, 2, yn)
    send_own(dy_ref, dyg, YB, 1, xn)
    send_own(dy_ref, dyg, YB, 0, sib)
    w_forward(0)
    for j in range(NC):
        forward(xg, XB, 4, ((6, sib),), j)
    a.wait()
    b.wait()
    d.wait()
    sg.wait()

    def load_tok(g, rr, s):
        return local(8 + s, g.at[pl.ds(mult(rr, t_loc), t_loc)], tok.at[s])

    def load_half(g, yy, rr, s, i):
        cols = pl.ds(mult(yy, h_loc), h_loc)
        return local(i, g.at[pl.ds(mult(rr, t_loc), t_loc), cols], tok.at[s, :, cols])

    blocks = (r, r_s, r_x, r_xs)
    for kind in (0, 3, 6):
        take(xg, XB, kind)
    loads = [load_tok(xg, blocks[i], i) for i in range(2)]
    w_forward(1)
    for t in range(4):
        recv(WB + t, wslot(r_s, wq(t, x)))
    for t in range(2):
        recv(WB + 8 + t, wslot(r_xs, wq(t, x)))
    for i in range(4):
        loads[i].wait()
        rows = pl.ds(mult(blocks[i], t_loc), t_loc)
        for n in range(hw // 256):
            mine = w_v[:, pl.ds(pl.multiple_of(r * hw + 256 * n, 256), 256)]
            qkv_v[rows, 256 * n:256 * n + 256] = jnp.dot(tok[i % 2], mine, preferred_element_type=f32).astype(bf)
        if i < 2:
            loads.append(load_tok(xg, blocks[i + 2], i))
        for h in range(heads):
            kt[h, :, rows] = qkv_v[rows, 3 * D * h + D:3 * D * h + 2 * D].T
            vt[h, :, rows] = qkv_v[rows, 3 * D * h + 2 * D:3 * D * h + 3 * D].T

    near_half = load_half(dyg, y, r, 0, 10)
    for i, rr in enumerate((r_s, r_x, r_xs)):
        recv(SGB + i, seg_v.at[rr])
    c1 = jnp.sum((seg_v[...] < 1).astype(jnp.int32))
    c2 = jnp.sum((seg_v[...] < 2).astype(jnp.int32))
    for j in range(NC):
        forward(dyg, YB, 2, ((5, sib),), j)
    far_half = load_half(dyg, 1 - y, r, 0, 11)
    for yy in range(2):
        piece = woh.at[:, pl.ds(yy * h_loc, h_loc)]
        mine = (y == yy) & (2 * y + x == r)

        @pl.when(mine)
        def _():
            pltpu.make_async_copy(wo_ref.at[pl.ds(0, ow)], piece, lsem.at[0]).wait()

        @pl.when(jnp.logical_not(mine))
        def _():
            recv(WOB + yy, piece)

    def d_out(i, s):
        rows = pl.ds(mult(blocks[i], t_loc), t_loc)
        do_v[rows, :] = lax.dot_general(tok[s], woh[...], NT, preferred_element_type=f32).astype(bf)

    def attend(i, h, between=None):
        attention_block(mult(blocks[i], t_loc), t_loc, h, c1, c2, qkv_v, do_v, p_scr, dp_scr, m_scr, kt, vt, dk_acc, dv_acc, dqkv_v, o_v, between)

    def dy_forward(j):
        forward(dyg, YB, 1, ((4, yn), (3, sib)), j)

    near_half.wait()
    far_half.wait()
    d_out(0, 0)
    attend(0, 0, lambda: dy_forward(0))
    for t in range(2, 4):
        w_own(t, 1, 1 - x, xn)
    others = (r_s, r_x, r_xs)

    def finish(h):
        c0 = 3 * D * h
        dqkv_v[:, c0 + D:c0 + 2 * D] = dk_acc[h].astype(bf)
        dqkv_v[:, c0 + 2 * D:c0 + 3 * D] = dv_acc[h].astype(bf)

    def tok_slot(rr, h, j, n, c0=0, c1=3 * D):
        return dtok.at[pl.ds(j * n, n), pl.ds(pl.multiple_of(rr * hw + 3 * D * h + c0, D), c1 - c0)]

    def send_dqkv(i, h, j, n):
        for k in (1, 2, 0):
            c0 = D if (h, k) == (0, 1) else 0
            src = dqkv_v.at[pl.ds(pl.multiple_of(others[k] * t_loc + j * n, n), n), pl.ds(3 * D * h + c0, 3 * D - c0)]
            send(i + k, src, tok_slot(r, h, j, n, c0), {'row': others[k]})

    def send_early_dq():
        src = dqkv_v.at[pl.ds(mult(r_x, t_loc), t_loc), pl.ds(0, D)]
        send(DQE, src, tok_slot(r, 0, 0, t_loc, 0, D), xn)

    loading = []

    def second_block():
        dy_forward(1)
        for kind in (0, 5):
            take(dyg, YB, kind)
        loading.append(load_tok(dyg, r_s, 1))

    def last_block():
        take(dyg, YB, 3)
        take(dyg, YB, 6)
        loading.append(load_tok(dyg, r_xs, 1))

    attend(0, 1, second_block)
    loading.pop().wait()
    d_out(1, 1)
    attend(1, 0)
    forward(dyg, YB, 4, ((6, sib),), 0)
    near_half = load_half(dyg, y, r_x, 0, 10)
    attend(1, 1)
    forward(dyg, YB, 4, ((6, sib),), 1)
    far_half = load_half(dyg, 1 - y, r_x, 0, 11)
    near_half.wait()
    far_half.wait()
    d_out(2, 0)
    attend(2, 0, last_block)
    send_early_dq()
    w_forward(2)
    loading.pop().wait()
    d_out(3, 1)
    ld = [local(5 + s, dyg.at[:, pl.ds(512 * s, 512)], col_v.at[s]) for s in range(2)]
    attend(3, 0)

    finish(0)
    send_dqkv(DQ, 0, 0, t_loc)
    attend(2, 1)
    w_forward(3)
    attend(3, 1)
    finish(1)
    for j in range(NJ):
        send_dqkv(DQ + 3 + 3 * j, 1, j, bt)
    dtok[:, pl.ds(mult(r, hw), hw)] = dqkv_v[pl.ds(mult(r, t_loc), t_loc), :]

    order = (r_x, r_xs, r_s, r)
    for s in range(4):
        ld[s].wait()
        dwo_v[:, 512 * s:512 * s + 512] = lax.dot_general(o_v[...], col_v[s % 2], TN, preferred_element_type=f32).astype(bf)
        if s < 2:
            ld.append(local(5 + s, dyg.at[:, pl.ds(512 * s + 1024, 512)], col_v.at[s]))
        else:
            ld.append(local(5 + s - 2, xg.at[:, pl.ds(mult(order[s - 2], t_loc), t_loc)], col_v.at[s - 2]))
    ld = ld[4:]
    row_to = 2 * y + x
    near = x == y
    for k in range(2):
        src = dwo_v.at[:, pl.ds(k * h_loc, h_loc)]
        dst = dwo_out.at[pl.ds(mult(c, ow), ow)]
        mine = (y == k) & (row_to == r)
        far = (y != k) & (x != y)

        @pl.when(mine)
        def _():
            pltpu.make_async_copy(src, dst, lsem.at[0]).start()

        @pl.when(far)
        def _():
            copy(DWF, DWF, src, relay, {'col': k}).start()

        @pl.when(jnp.logical_not(mine | far))
        def _():
            copy(DWO + k, DWO + c, src, dst, {'col': k, 'row': row_to}).start()

    def dw_slot(rr):
        return dw_out.at[:, pl.ds(mult(rr, hw), hw)]

    def d_w(i):
        s = i % 2
        ld[i].wait()
        part = lax.dot_general(col_v[s], dqkv_v[...], TN, preferred_element_type=f32).astype(bf)
        if i < 3:
            qkv_v[t_loc * i:t_loc * i + t_loc, :] = part
        else:
            dw_out[:, pl.ds(mult(r, hw), hw)] = part
        if i < 2:
            ld.append(local(5 + s, xg.at[:, pl.ds(mult(order[i + 2], t_loc), t_loc)], col_v.at[s]))

    def send_dw(i, k):
        send(DW + k, qkv_v.at[pl.ds(t_loc * i, t_loc)], dw_slot(r), {'row': others[k]})

    def d_x(j, half, dst):
        for n in range(h_loc // 256):
            rows = pl.ds(pl.multiple_of(half * h_loc + 256 * n, 256), 256)
            dst[pl.ds(2 * bt * j + bt * (n // 2), bt), 256 * (n % 2):256 * (n % 2) + 256] = lax.dot_general(
                dtok[pl.ds(j * bt, bt), :], w_v[rows, :], NT, preferred_element_type=f32)

    def d_x_send(j):
        for k in range(3):
            recv(DQ + 3 + 3 * j + k, tok_slot(others[k], 1, j, bt))
        d_x(j, 1 - y, dp_scr)
        part = pl.ds(2 * bt * j, 2 * bt)
        send(PX + j, dp_scr.at[part], px_recv.at[part], yn)

    d_w(0)
    send_dw(0, 1)
    d_w(1)
    send_dw(1, 2)
    for t in range(2, 4):
        recv(WB + 8 + t, wslot(r_xs, wq(t, x)))
    recv(DQE, tok_slot(r_x, 0, 0, t_loc, 0, D))
    for k in range(3):
        recv(DQ + k, tok_slot(others[k], 0, 0, t_loc, D if k == 1 else 0))
    d_x_send(0)

    @pl.when(near)
    def _():
        recv(DWF, relay)
        copy(DWG, DWG + c, relay, dwo_out.at[pl.ds(mult(c, ow), ow)], {'row': 2 * (1 - y) + x}).start()

    d_w(2)
    send_dw(2, 0)
    d_x_send(1)
    d_x(0, y, p_scr)
    d_w(3)
    d_x(1, y, p_scr)
    for j in range(NJ):
        recv(PX + j, px_recv.at[pl.ds(2 * bt * j, 2 * bt)])
        for q in range(2):
            part = pl.ds(2 * bt * j + bt * q, bt)
            dx_out[pl.ds(j * bt, bt), 512 * q:512 * q + 512] = (p_scr[part, :] + px_recv[part, :]).astype(bf)
    for k in range(3):
        recv(DW + k, dw_slot(others[k]))
    src_col, src_x = r // 2, lax.rem(r, 2)
    for k in range(2):
        piece = dwo_out.at[pl.ds(k * ow, ow)]
        mine = (src_col == y) & (2 * src_x + k == r)
        far = (src_col != y) & (src_x != src_col)

        @pl.when(mine)
        def _():
            pltpu.make_async_copy(dwo_v.at[:, pl.ds(0, h_loc)], piece, lsem.at[0]).wait()

        @pl.when(far)
        def _():
            recv(DWG + k, piece)

        @pl.when(jnp.logical_not(mine | far))
        def _():
            recv(DWO + k, piece)
    for cp in started:
        cp.wait_send()
    half = dwo_v.at[:, pl.ds(0, h_loc)]
    for k in range(2):
        @pl.when(jnp.logical_not((x == y) & (2 * c + k == r)))
        def _():
            copy(WOB + k, WOB + k, wo_ref.at[pl.ds(0, ow)], half, sib).wait_send()

        @pl.when(jnp.logical_not(((y == k) & (row_to == r)) | ((y != k) & (x != y))))
        def _():
            copy(DWO + k, DWO + k, half, relay, sib).wait_send()

    @pl.when(jnp.logical_not(near))
    def _():
        copy(DWF, DWF, half, relay, yn).wait_send()

    @pl.when(near)
    def _():
        copy(DWG, DWG, relay, relay, sib).wait_send()


def step_all(x_blk, w_blk, wo_blk, seg_blk, dy_blk):
    t_loc, h_loc = x_blk.shape
    w_loc = w_blk.shape[1]
    seq, hid = 4 * t_loc, 2 * h_loc
    hw, ow = w_loc // 4, w_loc // 12
    heads = ow // D
    bf, f32 = jnp.bfloat16, jnp.float32
    hbm = pl.BlockSpec(memory_space=pl.ANY)
    n_sem = 14 * NC + 12 + 2 + 3 + 3 + 3 * NJ + 3 + 2 + NJ + 1 + 2 + 1
    return pl.pallas_call(
        step_kernel,
        in_specs=[hbm] * 5,
        out_specs=[hbm] * 2 + [pl.BlockSpec(memory_space=pltpu.VMEM)] * 3,
        out_shape=[jax.ShapeDtypeStruct((seq, hid), bf)] * 2 + [pltpu.VMEM(b.shape, bf) for b in (x_blk, w_blk, wo_blk)],
        scratch_shapes=[
            pltpu.VMEM((hid, w_loc), bf), pltpu.VMEM((2, t_loc, hid), bf), pltpu.VMEM((2, seq, t_loc), bf),
            pltpu.VMEM((ow, hid), bf), pltpu.VMEM((seq, hw), bf), pltpu.VMEM((seq, ow), bf),
            pltpu.VMEM((4,) + seg_blk.shape, jnp.int32),
            pltpu.VMEM((seq, t_loc), f32), pltpu.VMEM((seq, t_loc), f32), pltpu.VMEM((seq // BK, 1, t_loc), f32),
            pltpu.VMEM((heads, D, seq), bf), pltpu.VMEM((heads, D, seq), bf),
            pltpu.VMEM((heads, seq, D), f32), pltpu.VMEM((heads, seq, D), f32),
            pltpu.VMEM((seq, hw), bf), pltpu.VMEM((seq, ow), bf),
            pltpu.VMEM((t_loc, w_loc), bf), pltpu.VMEM((ow, hid), bf), pltpu.VMEM((2 * t_loc, t_loc), f32),
            pltpu.VMEM((ow, h_loc), bf),
            pltpu.SemaphoreType.DMA((n_sem,)), pltpu.SemaphoreType.DMA((n_sem,)), pltpu.SemaphoreType.DMA((16,)),
        ],
        compiler_params=pltpu.CompilerParams(collective_id=0, has_side_effects=True, vmem_limit_bytes=STEP_LIMIT),
        name='mega_step',
    )(x_blk, w_blk, wo_blk, seg_blk, dy_blk)


def copy_kernel(parts, *refs):
    n = len(parts)
    ins, outs, sem = refs[:n], refs[n:2 * n], refs[2 * n]
    moves = []
    for i in range(n):
        step = ins[i].shape[0] // parts[i]
        for j in range(parts[i]):
            rows = pl.ds(j * step, step)
            move = pltpu.make_async_copy(ins[i].at[rows], outs[i].at[rows], sem.at[len(moves)])
            move.start()
            moves.append(move)
    for move in moves:
        move.wait()


def copy_out(*arrays):
    parts = [a.shape[0] // 128 for a in arrays]
    return pl.pallas_call(
        functools.partial(copy_kernel, parts),
        in_specs=[pl.BlockSpec(memory_space=pltpu.VMEM)] * len(arrays),
        out_specs=[pl.BlockSpec(memory_space=pl.ANY)] * len(arrays),
        out_shape=[jax.ShapeDtypeStruct(a.shape, a.dtype) for a in arrays],
        scratch_shapes=[pltpu.SemaphoreType.DMA((sum(parts),))],
        compiler_params=pltpu.CompilerParams(vmem_limit_bytes=1_000_000),
        name='copy_out',
    )(*arrays)


def solution(mesh):
    tok_spec = P(('dp', 'row'), 'col')
    mat_spec = P('row', 'col')
    seg_spec = P(('dp', 'row'))

    def grad_step(x_blk, wqkv_blk, wout_blk, seg_blk, dy_blk):
        _, _, grad_x, grad_wqkv, grad_wout = step_all(x_blk, wqkv_blk, wout_blk, seg_blk.reshape(4, -1), dy_blk)
        return copy_out(grad_x, grad_wqkv, grad_wout)

    return jax.shard_map(grad_step, mesh=mesh, in_specs=(tok_spec, mat_spec, mat_spec, seg_spec, tok_spec), out_specs=(tok_spec, tok_spec, tok_spec), check_vma=False)
```

```python
import functools

import jax
import jax.numpy as jnp
from jax import lax
from jax.experimental import pallas as pl
from jax.experimental.pallas import tpu as pltpu
from jax.sharding import PartitionSpec as P

NT = (((1,), (1,)), ((), ()))
TN = (((0,), (0,)), ((), ()))
MESH = pl.DeviceIdType.MESH
BK = 512
D = 128
NC = 2
NJ = 2
LOW = -3.0e38
VMEM_LIMIT = 66_000_000
STEP_LIMIT = 57_000_000


def mult(i, n):
    return pl.multiple_of(i * n, n)


def attention_block(q0, bq, h, c1, c2, qkv_v, do_v, p_scr, dp_scr, m_scr, kt, vt, dk_acc, dv_acc, dqkv_v, o_v, between):
    seq = qkv_v.shape[0]
    scale = D ** -0.5
    to_exp2 = scale * 1.4426950408889634
    f32 = jnp.float32
    rows = pl.ds(q0, bq)
    c0 = 3 * D * h
    iq = q0 + lax.broadcasted_iota(jnp.int32, (1, bq), 1)
    q_doc = (iq >= c1).astype(jnp.int32) + (iq >= c2).astype(jnp.int32)
    q = qkv_v[rows, c0:c0 + D]
    do = do_v[rows, D * h:D * h + D]

    def first(kb, carry):
        m, l, dd = carry
        k0 = pl.multiple_of(kb * BK, BK)
        keys = pl.ds(k0, BK)
        ik = k0 + lax.broadcasted_iota(jnp.int32, (BK, 1), 0)
        k_doc = (ik >= c1).astype(jnp.int32) + (ik >= c2).astype(jnp.int32)
        s = lax.dot_general(qkv_v[keys, c0 + D:c0 + 2 * D], q, NT, preferred_element_type=f32)
        s = jnp.where(q_doc == k_doc, s, LOW)
        dp = lax.dot_general(qkv_v[keys, c0 + 2 * D:c0 + 3 * D], do, NT, preferred_element_type=f32)
        dp_scr[keys, :] = dp
        m_new = jnp.maximum(m, jnp.max(s, axis=0, keepdims=True))
        p = jnp.exp2((s - m_new) * to_exp2)
        p_scr[keys, :] = p
        m_scr[kb] = m_new
        alpha = jnp.exp2((m - m_new) * to_exp2)
        return m_new, alpha * l + jnp.sum(p, axis=0, keepdims=True), alpha * dd + jnp.sum(p * dp, axis=0, keepdims=True)

    zero = jnp.zeros((1, bq), f32)
    m, l, dd = lax.fori_loop(0, seq // BK, first, (jnp.full((1, bq), LOW, f32), zero, zero))
    if between is not None:
        between()
    inv = 1.0 / l
    row_dot = dd * inv

    def second(kb, acc):
        o, dq = acc
        keys = pl.ds(pl.multiple_of(kb * BK, BK), BK)
        f = jnp.exp2((m_scr[kb] - m) * to_exp2) * inv
        p = p_scr[keys, :]
        p_bf = (p * f).astype(jnp.bfloat16)
        ds = ((p * (f * scale)) * (dp_scr[keys, :] - row_dot)).astype(jnp.bfloat16)
        o = o + jnp.dot(vt[h, :, keys], p_bf, preferred_element_type=f32)
        dq = dq + jnp.dot(kt[h, :, keys], ds, preferred_element_type=f32)
        dk_acc[h, keys, :] += jnp.dot(ds, q, preferred_element_type=f32)
        dv_acc[h, keys, :] += jnp.dot(p_bf, do, preferred_element_type=f32)
        return o, dq

    zacc = jnp.zeros((D, bq), f32)
    o, dq = lax.fori_loop(0, seq // BK, second, (zacc, zacc))
    o_v[rows, D * h:D * h + D] = o.T.astype(jnp.bfloat16)
    dqkv_v[rows, c0:c0 + D] = dq.T.astype(jnp.bfloat16)


def step_kernel(x_ref, w_ref, wo_ref, seg_ref, dy_ref, xg, dyg, dx_out, dw_out, dwo_out,
                w_v, tok, col_v, woh, qkv_v, do_v, seg_v, p_scr, dp_scr, m_scr, kt, vt, dk_acc, dv_acc, dqkv_v, o_v,
                dtok, dwo_v, px_recv, relay, ssem, rsem, lsem):
    y = lax.axis_index('col')
    r = lax.axis_index('row')
    x = r // 2
    c = lax.rem(r, 2)
    r_s = r + 1 - 2 * c
    r_x = lax.rem(r + 2, 4)
    r_xs = lax.rem(r_s + 2, 4)
    sib, xn, yn = {'row': r_s}, {'row': r_x}, {'col': 1 - y}
    t_loc, h_loc = x_ref.shape
    hw = qkv_v.shape[1]
    ow = woh.shape[0]
    heads = ow // D
    ct, bt = t_loc // NC, t_loc // NJ
    f32, bf = jnp.float32, jnp.bfloat16
    started = []
    XB, YB, WB = 0, 7 * NC, 14 * NC
    WOB = WB + 12
    SGB = WOB + 2
    DQ = SGB + 3
    DW = DQ + 3 + 3 * NJ
    DWO = DW + 3
    PX = DWO + 2
    DWF = PX + NJ
    DWG = DWF + 1
    DQE = DWG + 2

    def copy(i, k, src, dst, dev):
        return pltpu.make_async_remote_copy(src, dst, ssem.at[i], rsem.at[k], device_id=dev, device_id_type=MESH)

    def send(i, src, dst, dev):
        cp = copy(i, i, src, dst, dev)
        cp.start()
        started.append(cp)

    def recv(i, dst):
        copy(i, i, dst, dst, sib).wait_recv()

    def local(i, src, dst):
        cp = pltpu.make_async_copy(src, dst, lsem.at[i])
        cp.start()
        return cp

    def slot(g, yy, rr, j):
        return g.at[pl.ds(pl.multiple_of(rr * t_loc + j * ct, ct), ct), pl.ds(mult(yy, h_loc), h_loc)]

    def tid(base, kind, j):
        return base + kind * NC + j

    def got_from(kind):
        return ((y, r_s), (y, r_x), (1 - y, r), (y, r_xs), (1 - y, r_x), (1 - y, r_s), (1 - y, r_xs))[kind]

    def send_own(a, g, base, kind, dev):
        for j in range(NC):
            send(tid(base, kind, j), a.at[pl.ds(j * ct, ct)], slot(g, y, r, j), dev)

    def forward(g, base, kind_in, outs, j):
        yy, rr = got_from(kind_in)
        recv(tid(base, kind_in, j), slot(g, yy, rr, j))
        for kind_out, dev in outs:
            send(tid(base, kind_out, j), slot(g, yy, rr, j), slot(g, yy, rr, j), dev)

    def take(g, base, kind):
        yy, rr = got_from(kind)
        for j in range(NC):
            recv(tid(base, kind, j), slot(g, yy, rr, j))

    def wslot(rr, q):
        return w_v.at[pl.ds(mult(rr, t_loc), t_loc), pl.ds(mult(q, hw), hw)]

    def wq(t, xx):
        return lax.rem(2 * xx + t, 4)

    def w_own(t, kind, xx, dev):
        q = wq(t, xx)
        send(WB + 4 * kind + t, w_ref.at[:, pl.ds(mult(q, hw), hw)], wslot(r, q), dev)

    def w_forward(t):
        q = wq(t, x)
        recv(WB + 4 + t, wslot(r_x, q))
        send(WB + 8 + t, wslot(r_x, q), wslot(r_x, q), sib)

    barrier = pltpu.get_barrier_semaphore()
    for dev in (xn, yn, sib):
        pl.semaphore_signal(barrier, inc=1, device_id=dev, device_id_type=MESH)
    pl.semaphore_wait(barrier, 3)

    send_own(x_ref, xg, XB, 1, xn)
    send_own(x_ref, xg, XB, 2, yn)
    for t in range(2):
        w_own(t, 1, 1 - x, xn)
    send_own(x_ref, xg, XB, 0, sib)
    for t in range(4):
        w_own(t, 0, x, sib)
    send(SGB, seg_ref, seg_v.at[r], sib)
    send(SGB + 1, seg_ref, seg_v.at[r], xn)

    a = local(1, x_ref, tok.at[0, :, pl.ds(0, h_loc)])
    b = local(2, dy_ref, tok.at[1, :, pl.ds(0, h_loc)])
    d = local(3, w_ref, w_v.at[pl.ds(mult(r, t_loc), t_loc)])
    sg = local(4, seg_ref, seg_v.at[r])
    own_slot = lambda g: g.at[pl.ds(mult(r, t_loc), t_loc), pl.ds(mult(y, h_loc), h_loc)]
    a.wait()
    a = local(1, tok.at[0, :, pl.ds(0, h_loc)], own_slot(xg))
    b.wait()
    b = local(2, tok.at[1, :, pl.ds(0, h_loc)], own_slot(dyg))
    dk_acc[...] = jnp.zeros_like(dk_acc)
    dv_acc[...] = jnp.zeros_like(dv_acc)

    for j in range(NC):
        forward(xg, XB, 1, ((4, yn), (3, sib)), j)
        forward(xg, XB, 2, ((5, sib),), j)
    take(xg, XB, 5)
    send(SGB + 2, seg_ref, seg_v.at[r], {'row': r_xs})
    for k in range(2):
        row_to = 2 * c + k
        src = wo_ref.at[pl.ds(k * ow, ow)]
        dst = woh.at[:, pl.ds(mult(y, h_loc), h_loc)]
        mine = (x == y) & (row_to == r)

        @pl.when(mine)
        def _():
            pltpu.make_async_copy(src, dst, lsem.at[0]).start()

        @pl.when(jnp.logical_not(mine))
        def _():
            copy(WOB + k, WOB + y, src, dst, {'col': x, 'row': row_to}).start()
    send_own(dy_ref, dyg, YB, 2, yn)
    send_own(dy_ref, dyg, YB, 1, xn)
    send_own(dy_ref, dyg, YB, 0, sib)
    w_forward(0)
    for j in range(NC):
        forward(xg, XB, 4, ((6, sib),), j)
    a.wait()
    b.wait()
    d.wait()
    sg.wait()

    def load_tok(g, rr, s):
        return local(8 + s, g.at[pl.ds(mult(rr, t_loc), t_loc)], tok.at[s])

    def load_half(g, yy, rr, s, i):
        cols = pl.ds(mult(yy, h_loc), h_loc)
        return local(i, g.at[pl.ds(mult(rr, t_loc), t_loc), cols], tok.at[s, :, cols])

    blocks = (r, r_s, r_x, r_xs)
    for kind in (0, 3, 6):
        take(xg, XB, kind)
    loads = [load_tok(xg, blocks[i], i) for i in range(2)]
    w_forward(1)
    for t in range(4):
        recv(WB + t, wslot(r_s, wq(t, x)))
    for t in range(2):
        recv(WB + 8 + t, wslot(r_xs, wq(t, x)))
    for i in range(4):
        loads[i].wait()
        rows = pl.ds(mult(blocks[i], t_loc), t_loc)
        for n in range(hw // 256):
            mine = w_v[:, pl.ds(pl.multiple_of(r * hw + 256 * n, 256), 256)]
            qkv_v[rows, 256 * n:256 * n + 256] = jnp.dot(tok[i % 2], mine, preferred_element_type=f32).astype(bf)
        if i < 2:
            loads.append(load_tok(xg, blocks[i + 2], i))
        for h in range(heads):
            kt[h, :, rows] = qkv_v[rows, 3 * D * h + D:3 * D * h + 2 * D].T
            vt[h, :, rows] = qkv_v[rows, 3 * D * h + 2 * D:3 * D * h + 3 * D].T

    near_half = load_half(dyg, y, r, 0, 10)
    for i, rr in enumerate((r_s, r_x, r_xs)):
        recv(SGB + i, seg_v.at[rr])
    c1 = jnp.sum((seg_v[...] < 1).astype(jnp.int32))
    c2 = jnp.sum((seg_v[...] < 2).astype(jnp.int32))
    for j in range(NC):
        forward(dyg, YB, 2, ((5, sib),), j)
    far_half = load_half(dyg, 1 - y, r, 0, 11)
    for yy in range(2):
        piece = woh.at[:, pl.ds(yy * h_loc, h_loc)]
        mine = (y == yy) & (2 * y + x == r)

        @pl.when(mine)
        def _():
            pltpu.make_async_copy(wo_ref.at[pl.ds(0, ow)], piece, lsem.at[0]).wait()

        @pl.when(jnp.logical_not(mine))
        def _():
            recv(WOB + yy, piece)

    def d_out(i, s):
        rows = pl.ds(mult(blocks[i], t_loc), t_loc)
        do_v[rows, :] = lax.dot_general(tok[s], woh[...], NT, preferred_element_type=f32).astype(bf)

    def attend(i, h, between=None):
        attention_block(mult(blocks[i], t_loc), t_loc, h, c1, c2, qkv_v, do_v, p_scr, dp_scr, m_scr, kt, vt, dk_acc, dv_acc, dqkv_v, o_v, between)

    def dy_forward(j):
        forward(dyg, YB, 1, ((4, yn), (3, sib)), j)

    near_half.wait()
    far_half.wait()
    d_out(0, 0)
    attend(0, 0, lambda: dy_forward(0))
    for t in range(2, 4):
        w_own(t, 1, 1 - x, xn)
    others = (r_s, r_x, r_xs)

    def finish(h):
        c0 = 3 * D * h
        dqkv_v[:, c0 + D:c0 + 2 * D] = dk_acc[h].astype(bf)
        dqkv_v[:, c0 + 2 * D:c0 + 3 * D] = dv_acc[h].astype(bf)

    def tok_slot(rr, h, j, n, c0=0, c1=3 * D):
        return dtok.at[pl.ds(j * n, n), pl.ds(pl.multiple_of(rr * hw + 3 * D * h + c0, D), c1 - c0)]

    def send_dqkv(i, h, j, n):
        for k in (1, 2, 0):
            c0 = D if (h, k) == (0, 1) else 0
            src = dqkv_v.at[pl.ds(pl.multiple_of(others[k] * t_loc + j * n, n), n), pl.ds(3 * D * h + c0, 3 * D - c0)]
            send(i + k, src, tok_slot(r, h, j, n, c0), {'row': others[k]})

    def send_early_dq():
        src = dqkv_v.at[pl.ds(mult(r_x, t_loc), t_loc), pl.ds(0, D)]
        send(DQE, src, tok_slot(r, 0, 0, t_loc, 0, D), xn)

    loading = []

    def second_block():
        dy_forward(1)
        for kind in (0, 5):
            take(dyg, YB, kind)
        loading.append(load_tok(dyg, r_s, 1))

    def last_block():
        take(dyg, YB, 3)
        take(dyg, YB, 6)
        loading.append(load_tok(dyg, r_xs, 1))

    attend(0, 1, second_block)
    loading.pop().wait()
    d_out(1, 1)
    attend(1, 0)
    forward(dyg, YB, 4, ((6, sib),), 0)
    near_half = load_half(dyg, y, r_x, 0, 10)
    attend(1, 1)
    forward(dyg, YB, 4, ((6, sib),), 1)
    far_half = load_half(dyg, 1 - y, r_x, 0, 11)
    near_half.wait()
    far_half.wait()
    d_out(2, 0)
    attend(2, 0, last_block)
    send_early_dq()
    w_forward(2)
    loading.pop().wait()
    d_out(3, 1)
    ld = [local(5 + s, dyg.at[:, pl.ds(512 * s, 512)], col_v.at[s]) for s in range(2)]
    attend(3, 0)

    finish(0)
    send_dqkv(DQ, 0, 0, t_loc)
    attend(2, 1)
    w_forward(3)
    attend(3, 1)
    finish(1)
    for j in range(NJ):
        send_dqkv(DQ + 3 + 3 * j, 1, j, bt)
    dtok[:, pl.ds(mult(r, hw), hw)] = dqkv_v[pl.ds(mult(r, t_loc), t_loc), :]

    order = (r_x, r_xs, r_s, r)
    for s in range(4):
        ld[s].wait()
        dwo_v[:, 512 * s:512 * s + 512] = lax.dot_general(o_v[...], col_v[s % 2], TN, preferred_element_type=f32).astype(bf)
        if s < 2:
            ld.append(local(5 + s, dyg.at[:, pl.ds(512 * s + 1024, 512)], col_v.at[s]))
        else:
            ld.append(local(5 + s - 2, xg.at[:, pl.ds(mult(order[s - 2], t_loc), t_loc)], col_v.at[s - 2]))
    ld = ld[4:]
    row_to = 2 * y + x
    near = x == y
    for k in range(2):
        src = dwo_v.at[:, pl.ds(k * h_loc, h_loc)]
        dst = dwo_out.at[pl.ds(mult(c, ow), ow)]
        mine = (y == k) & (row_to == r)
        far = (y != k) & (x != y)

        @pl.when(mine)
        def _():
            pltpu.make_async_copy(src, dst, lsem.at[0]).start()

        @pl.when(far)
        def _():
            copy(DWF, DWF, src, relay, {'col': k}).start()

        @pl.when(jnp.logical_not(mine | far))
        def _():
            copy(DWO + k, DWO + c, src, dst, {'col': k, 'row': row_to}).start()

    def dw_slot(rr):
        return dw_out.at[:, pl.ds(mult(rr, hw), hw)]

    def d_w(i):
        s = i % 2
        ld[i].wait()
        part = lax.dot_general(col_v[s], dqkv_v[...], TN, preferred_element_type=f32).astype(bf)
        if i < 3:
            qkv_v[t_loc * i:t_loc * i + t_loc, :] = part
        else:
            dw_out[:, pl.ds(mult(r, hw), hw)] = part
        if i < 2:
            ld.append(local(5 + s, xg.at[:, pl.ds(mult(order[i + 2], t_loc), t_loc)], col_v.at[s]))

    def send_dw(i, k):
        send(DW + k, qkv_v.at[pl.ds(t_loc * i, t_loc)], dw_slot(r), {'row': others[k]})

    def d_x(j, half, dst):
        for n in range(h_loc // 256):
            rows = pl.ds(pl.multiple_of(half * h_loc + 256 * n, 256), 256)
            dst[pl.ds(2 * bt * j + bt * (n // 2), bt), 256 * (n % 2):256 * (n % 2) + 256] = lax.dot_general(
                dtok[pl.ds(j * bt, bt), :], w_v[rows, :], NT, preferred_element_type=f32)

    def d_x_send(j):
        for k in range(3):
            recv(DQ + 3 + 3 * j + k, tok_slot(others[k], 1, j, bt))
        d_x(j, 1 - y, dp_scr)
        part = pl.ds(2 * bt * j, 2 * bt)
        send(PX + j, dp_scr.at[part], px_recv.at[part], yn)

    d_w(0)
    send_dw(0, 1)
    d_w(1)
    send_dw(1, 2)
    for t in range(2, 4):
        recv(WB + 8 + t, wslot(r_xs, wq(t, x)))
    recv(DQE, tok_slot(r_x, 0, 0, t_loc, 0, D))
    for k in range(3):
        recv(DQ + k, tok_slot(others[k], 0, 0, t_loc, D if k == 1 else 0))
    d_x_send(0)

    @pl.when(near)
    def _():
        recv(DWF, relay)
        copy(DWG, DWG + c, relay, dwo_out.at[pl.ds(mult(c, ow), ow)], {'row': 2 * (1 - y) + x}).start()

    d_w(2)
    send_dw(2, 0)
    d_x_send(1)
    d_x(0, y, p_scr)
    d_w(3)
    d_x(1, y, p_scr)
    late = started[-(3 + NJ):]
    for cp in started[:-(3 + NJ)]:
        cp.wait_send()
    half = dwo_v.at[:, pl.ds(0, h_loc)]
    for k in range(2):
        @pl.when(jnp.logical_not((x == y) & (2 * c + k == r)))
        def _():
            copy(WOB + k, WOB + k, wo_ref.at[pl.ds(0, ow)], half, sib).wait_send()

        @pl.when(jnp.logical_not(((y == k) & (row_to == r)) | ((y != k) & (x != y))))
        def _():
            copy(DWO + k, DWO + k, half, relay, sib).wait_send()

    @pl.when(jnp.logical_not(near))
    def _():
        copy(DWF, DWF, half, relay, yn).wait_send()

    for j in range(NJ):
        recv(PX + j, px_recv.at[pl.ds(2 * bt * j, 2 * bt)])
        for q in range(2):
            part = pl.ds(2 * bt * j + bt * q, bt)
            dx_out[pl.ds(j * bt, bt), 512 * q:512 * q + 512] = (p_scr[part, :] + px_recv[part, :]).astype(bf)
    for k in range(3):
        recv(DW + k, dw_slot(others[k]))
    src_col, src_x = r // 2, lax.rem(r, 2)
    for k in range(2):
        piece = dwo_out.at[pl.ds(k * ow, ow)]
        mine = (src_col == y) & (2 * src_x + k == r)
        far = (src_col != y) & (src_x != src_col)

        @pl.when(mine)
        def _():
            pltpu.make_async_copy(dwo_v.at[:, pl.ds(0, h_loc)], piece, lsem.at[0]).wait()

        @pl.when(far)
        def _():
            recv(DWG + k, piece)

        @pl.when(jnp.logical_not(mine | far))
        def _():
            recv(DWO + k, piece)
    for cp in late:
        cp.wait_send()

    @pl.when(near)
    def _():
        copy(DWG, DWG, relay, relay, sib).wait_send()


def step_all(x_blk, w_blk, wo_blk, seg_blk, dy_blk):
    t_loc, h_loc = x_blk.shape
    w_loc = w_blk.shape[1]
    seq, hid = 4 * t_loc, 2 * h_loc
    hw, ow = w_loc // 4, w_loc // 12
    heads = ow // D
    bf, f32 = jnp.bfloat16, jnp.float32
    hbm = pl.BlockSpec(memory_space=pl.ANY)
    n_sem = 14 * NC + 12 + 2 + 3 + 3 + 3 * NJ + 3 + 2 + NJ + 1 + 2 + 1
    return pl.pallas_call(
        step_kernel,
        in_specs=[hbm] * 5,
        out_specs=[hbm] * 2 + [pl.BlockSpec(memory_space=pltpu.VMEM)] * 3,
        out_shape=[jax.ShapeDtypeStruct((seq, hid), bf)] * 2 + [pltpu.VMEM(b.shape, bf) for b in (x_blk, w_blk, wo_blk)],
        scratch_shapes=[
            pltpu.VMEM((hid, w_loc), bf), pltpu.VMEM((2, t_loc, hid), bf), pltpu.VMEM((2, seq, t_loc), bf),
            pltpu.VMEM((ow, hid), bf), pltpu.VMEM((seq, hw), bf), pltpu.VMEM((seq, ow), bf),
            pltpu.VMEM((4,) + seg_blk.shape, jnp.int32),
            pltpu.VMEM((seq, t_loc), f32), pltpu.VMEM((seq, t_loc), f32), pltpu.VMEM((seq // BK, 1, t_loc), f32),
            pltpu.VMEM((heads, D, seq), bf), pltpu.VMEM((heads, D, seq), bf),
            pltpu.VMEM((heads, seq, D), f32), pltpu.VMEM((heads, seq, D), f32),
            pltpu.VMEM((seq, hw), bf), pltpu.VMEM((seq, ow), bf),
            pltpu.VMEM((t_loc, w_loc), bf), pltpu.VMEM((ow, hid), bf), pltpu.VMEM((2 * t_loc, t_loc), f32),
            pltpu.VMEM((ow, h_loc), bf),
            pltpu.SemaphoreType.DMA((n_sem,)), pltpu.SemaphoreType.DMA((n_sem,)), pltpu.SemaphoreType.DMA((16,)),
        ],
        compiler_params=pltpu.CompilerParams(collective_id=0, has_side_effects=True, vmem_limit_bytes=STEP_LIMIT),
        name='mega_step',
    )(x_blk, w_blk, wo_blk, seg_blk, dy_blk)


def copy_kernel(parts, *refs):
    n = len(parts)
    ins, outs, sem = refs[:n], refs[n:2 * n], refs[2 * n]
    moves = []
    for i in range(n):
        step = ins[i].shape[0] // parts[i]
        for j in range(parts[i]):
            rows = pl.ds(j * step, step)
            move = pltpu.make_async_copy(ins[i].at[rows], outs[i].at[rows], sem.at[len(moves)])
            move.start()
            moves.append(move)
    for move in moves:
        move.wait()


def copy_out(*arrays):
    parts = [a.shape[0] // 128 for a in arrays]
    return pl.pallas_call(
        functools.partial(copy_kernel, parts),
        in_specs=[pl.BlockSpec(memory_space=pltpu.VMEM)] * len(arrays),
        out_specs=[pl.BlockSpec(memory_space=pl.ANY)] * len(arrays),
        out_shape=[jax.ShapeDtypeStruct(a.shape, a.dtype) for a in arrays],
        scratch_shapes=[pltpu.SemaphoreType.DMA((sum(parts),))],
        compiler_params=pltpu.CompilerParams(vmem_limit_bytes=1_000_000),
        name='copy_out',
    )(*arrays)


def solution(mesh):
    tok_spec = P(('dp', 'row'), 'col')
    mat_spec = P('row', 'col')
    seg_spec = P(('dp', 'row'))

    def grad_step(x_blk, wqkv_blk, wout_blk, seg_blk, dy_blk):
        _, _, grad_x, grad_wqkv, grad_wout = step_all(x_blk, wqkv_blk, wout_blk, seg_blk.reshape(4, -1), dy_blk)
        return copy_out(grad_x, grad_wqkv, grad_wout)

    return jax.shard_map(grad_step, mesh=mesh, in_specs=(tok_spec, mat_spec, mat_spec, seg_spec, tok_spec), out_specs=(tok_spec, tok_spec, tok_spec), check_vma=False)
```

```python
import functools

import jax
import jax.numpy as jnp
from jax import lax
from jax.experimental import pallas as pl
from jax.experimental.pallas import tpu as pltpu
from jax.sharding import PartitionSpec as P

NT = (((1,), (1,)), ((), ()))
TN = (((0,), (0,)), ((), ()))
MESH = pl.DeviceIdType.MESH
BK = 512
D = 128
NC = 2
NJ = 2
LOW = -3.0e38
VMEM_LIMIT = 66_000_000
STEP_LIMIT = 57_000_000


def mult(i, n):
    return pl.multiple_of(i * n, n)


def attention_block(q0, bq, h, c1, c2, qkv_v, do_v, p_scr, dp_scr, m_scr, kt, vt, dk_acc, dv_acc, dqkv_v, o_v, between):
    seq = qkv_v.shape[0]
    scale = D ** -0.5
    to_exp2 = scale * 1.4426950408889634
    f32 = jnp.float32
    rows = pl.ds(q0, bq)
    c0 = 3 * D * h
    iq = q0 + lax.broadcasted_iota(jnp.int32, (1, bq), 1)
    q_doc = (iq >= c1).astype(jnp.int32) + (iq >= c2).astype(jnp.int32)
    q = qkv_v[rows, c0:c0 + D]
    do = do_v[rows, D * h:D * h + D]

    def first(kb, carry):
        m, l, dd = carry
        k0 = pl.multiple_of(kb * BK, BK)
        keys = pl.ds(k0, BK)
        ik = k0 + lax.broadcasted_iota(jnp.int32, (BK, 1), 0)
        k_doc = (ik >= c1).astype(jnp.int32) + (ik >= c2).astype(jnp.int32)
        s = lax.dot_general(qkv_v[keys, c0 + D:c0 + 2 * D], q, NT, preferred_element_type=f32)
        s = jnp.where(q_doc == k_doc, s, LOW)
        dp = lax.dot_general(qkv_v[keys, c0 + 2 * D:c0 + 3 * D], do, NT, preferred_element_type=f32)
        dp_scr[keys, :] = dp
        m_new = jnp.maximum(m, jnp.max(s, axis=0, keepdims=True))
        p = jnp.exp2((s - m_new) * to_exp2)
        p_scr[keys, :] = p
        m_scr[kb] = m_new
        alpha = jnp.exp2((m - m_new) * to_exp2)
        return m_new, alpha * l + jnp.sum(p, axis=0, keepdims=True), alpha * dd + jnp.sum(p * dp, axis=0, keepdims=True)

    zero = jnp.zeros((1, bq), f32)
    m, l, dd = lax.fori_loop(0, seq // BK, first, (jnp.full((1, bq), LOW, f32), zero, zero))
    if between is not None:
        between()
    inv = 1.0 / l
    row_dot = dd * inv

    def second(kb, acc):
        o, dq = acc
        keys = pl.ds(pl.multiple_of(kb * BK, BK), BK)
        f = jnp.exp2((m_scr[kb] - m) * to_exp2) * inv
        p = p_scr[keys, :]
        p_bf = (p * f).astype(jnp.bfloat16)
        ds = ((p * (f * scale)) * (dp_scr[keys, :] - row_dot)).astype(jnp.bfloat16)
        o = o + jnp.dot(vt[h, :, keys], p_bf, preferred_element_type=f32)
        dq = dq + jnp.dot(kt[h, :, keys], ds, preferred_element_type=f32)
        dk_acc[h, keys, :] += jnp.dot(ds, q, preferred_element_type=f32)
        dv_acc[h, keys, :] += jnp.dot(p_bf, do, preferred_element_type=f32)
        return o, dq

    zacc = jnp.zeros((D, bq), f32)
    o, dq = lax.fori_loop(0, seq // BK, second, (zacc, zacc))
    o_v[rows, D * h:D * h + D] = o.T.astype(jnp.bfloat16)
    dqkv_v[rows, c0:c0 + D] = dq.T.astype(jnp.bfloat16)


def step_kernel(x_ref, w_ref, wo_ref, seg_ref, dy_ref, xg, dyg, dx_out, dw_out, dwo_out,
                w_v, tok, col_v, woh, qkv_v, do_v, seg_v, p_scr, dp_scr, m_scr, kt, vt, dk_acc, dv_acc, dqkv_v, o_v,
                dtok, dwo_v, px_recv, relay, ssem, rsem, lsem):
    y = lax.axis_index('col')
    r = lax.axis_index('row')
    x = r // 2
    c = lax.rem(r, 2)
    r_s = r + 1 - 2 * c
    r_x = lax.rem(r + 2, 4)
    r_xs = lax.rem(r_s + 2, 4)
    sib, xn, yn = {'row': r_s}, {'row': r_x}, {'col': 1 - y}
    t_loc, h_loc = x_ref.shape
    hw = qkv_v.shape[1]
    ow = woh.shape[0]
    heads = ow // D
    ct, bt = t_loc // NC, t_loc // NJ
    f32, bf = jnp.float32, jnp.bfloat16
    started = []
    XB, YB, WB = 0, 7 * NC, 14 * NC
    WOB = WB + 12
    SGB = WOB + 2
    DQ = SGB + 3
    DW = DQ + 3 + 3 * NJ
    DWO = DW + 3
    PX = DWO + 2
    DWF = PX + NJ
    DWG = DWF + 1
    DQE = DWG + 2

    def copy(i, k, src, dst, dev):
        return pltpu.make_async_remote_copy(src, dst, ssem.at[i], rsem.at[k], device_id=dev, device_id_type=MESH)

    def send(i, src, dst, dev):
        cp = copy(i, i, src, dst, dev)
        cp.start()
        started.append(cp)

    def recv(i, dst):
        copy(i, i, dst, dst, sib).wait_recv()

    def local(i, src, dst):
        cp = pltpu.make_async_copy(src, dst, lsem.at[i])
        cp.start()
        return cp

    def slot(g, yy, rr, j):
        return g.at[pl.ds(pl.multiple_of(rr * t_loc + j * ct, ct), ct), pl.ds(mult(yy, h_loc), h_loc)]

    def tid(base, kind, j):
        return base + kind * NC + j

    def got_from(kind):
        return ((y, r_s), (y, r_x), (1 - y, r), (y, r_xs), (1 - y, r_x), (1 - y, r_s), (1 - y, r_xs))[kind]

    def send_own(a, g, base, kind, dev):
        for j in range(NC):
            send(tid(base, kind, j), a.at[pl.ds(j * ct, ct)], slot(g, y, r, j), dev)

    def forward(g, base, kind_in, outs, j):
        yy, rr = got_from(kind_in)
        recv(tid(base, kind_in, j), slot(g, yy, rr, j))
        for kind_out, dev in outs:
            send(tid(base, kind_out, j), slot(g, yy, rr, j), slot(g, yy, rr, j), dev)

    def take(g, base, kind):
        yy, rr = got_from(kind)
        for j in range(NC):
            recv(tid(base, kind, j), slot(g, yy, rr, j))

    def wslot(rr, q):
        return w_v.at[pl.ds(mult(rr, t_loc), t_loc), pl.ds(mult(q, hw), hw)]

    def wq(t, xx):
        return lax.rem(2 * xx + t, 4)

    def w_own(t, kind, xx, dev):
        q = wq(t, xx)
        send(WB + 4 * kind + t, w_ref.at[:, pl.ds(mult(q, hw), hw)], wslot(r, q), dev)

    def w_forward(t):
        q = wq(t, x)
        recv(WB + 4 + t, wslot(r_x, q))
        send(WB + 8 + t, wslot(r_x, q), wslot(r_x, q), sib)

    barrier = pltpu.get_barrier_semaphore()
    for dev in (xn, yn, sib):
        pl.semaphore_signal(barrier, inc=1, device_id=dev, device_id_type=MESH)
    pl.semaphore_wait(barrier, 3)

    send_own(x_ref, xg, XB, 1, xn)
    send_own(x_ref, xg, XB, 2, yn)
    for t in range(2):
        w_own(t, 1, 1 - x, xn)
    send_own(x_ref, xg, XB, 0, sib)
    for t in range(4):
        w_own(t, 0, x, sib)
    send(SGB, seg_ref, seg_v.at[r], sib)
    send(SGB + 1, seg_ref, seg_v.at[r], xn)

    a = local(1, x_ref, tok.at[0, :, pl.ds(0, h_loc)])
    b = local(2, dy_ref, tok.at[1, :, pl.ds(0, h_loc)])
    d = local(3, w_ref, w_v.at[pl.ds(mult(r, t_loc), t_loc)])
    sg = local(4, seg_ref, seg_v.at[r])
    own_slot = lambda g: g.at[pl.ds(mult(r, t_loc), t_loc), pl.ds(mult(y, h_loc), h_loc)]
    a.wait()
    a = local(1, tok.at[0, :, pl.ds(0, h_loc)], own_slot(xg))
    b.wait()
    b = local(2, tok.at[1, :, pl.ds(0, h_loc)], own_slot(dyg))
    dk_acc[...] = jnp.zeros_like(dk_acc)
    dv_acc[...] = jnp.zeros_like(dv_acc)

    for j in range(NC):
        forward(xg, XB, 1, ((4, yn), (3, sib)), j)
        forward(xg, XB, 2, ((5, sib),), j)
    take(xg, XB, 5)
    send(SGB + 2, seg_ref, seg_v.at[r], {'row': r_xs})
    for k in range(2):
        row_to = 2 * c + k
        src = wo_ref.at[pl.ds(k * ow, ow)]
        dst = woh.at[:, pl.ds(mult(y, h_loc), h_loc)]
        mine = (x == y) & (row_to == r)

        @pl.when(mine)
        def _():
            pltpu.make_async_copy(src, dst, lsem.at[0]).start()

        @pl.when(jnp.logical_not(mine))
        def _():
            copy(WOB + k, WOB + y, src, dst, {'col': x, 'row': row_to}).start()
    send_own(dy_ref, dyg, YB, 2, yn)
    send_own(dy_ref, dyg, YB, 1, xn)
    send_own(dy_ref, dyg, YB, 0, sib)
    w_forward(0)
    for j in range(NC):
        forward(xg, XB, 4, ((6, sib),), j)
    a.wait()
    b.wait()
    d.wait()
    sg.wait()

    def load_tok(g, rr, s):
        return local(8 + s, g.at[pl.ds(mult(rr, t_loc), t_loc)], tok.at[s])

    def load_half(g, yy, rr, s, i):
        cols = pl.ds(mult(yy, h_loc), h_loc)
        return local(i, g.at[pl.ds(mult(rr, t_loc), t_loc), cols], tok.at[s, :, cols])

    blocks = (r, r_s, r_x, r_xs)
    for kind in (0, 3, 6):
        take(xg, XB, kind)
    loads = [load_tok(xg, blocks[i], i) for i in range(2)]
    w_forward(1)
    for t in range(4):
        recv(WB + t, wslot(r_s, wq(t, x)))
    for t in range(2):
        recv(WB + 8 + t, wslot(r_xs, wq(t, x)))
    for i in range(4):
        loads[i].wait()
        rows = pl.ds(mult(blocks[i], t_loc), t_loc)
        for n in range(hw // 256):
            mine = w_v[:, pl.ds(pl.multiple_of(r * hw + 256 * n, 256), 256)]
            qkv_v[rows, 256 * n:256 * n + 256] = jnp.dot(tok[i % 2], mine, preferred_element_type=f32).astype(bf)
        if i < 2:
            loads.append(load_tok(xg, blocks[i + 2], i))
        for h in range(heads):
            kt[h, :, rows] = qkv_v[rows, 3 * D * h + D:3 * D * h + 2 * D].T
            vt[h, :, rows] = qkv_v[rows, 3 * D * h + 2 * D:3 * D * h + 3 * D].T

    near_half = load_half(dyg, y, r, 0, 10)
    for i, rr in enumerate((r_s, r_x, r_xs)):
        recv(SGB + i, seg_v.at[rr])
    c1 = jnp.sum((seg_v[...] < 1).astype(jnp.int32))
    c2 = jnp.sum((seg_v[...] < 2).astype(jnp.int32))
    for j in range(NC):
        forward(dyg, YB, 2, ((5, sib),), j)
    far_half = load_half(dyg, 1 - y, r, 0, 11)
    for yy in range(2):
        piece = woh.at[:, pl.ds(yy * h_loc, h_loc)]
        mine = (y == yy) & (2 * y + x == r)

        @pl.when(mine)
        def _():
            pltpu.make_async_copy(wo_ref.at[pl.ds(0, ow)], piece, lsem.at[0]).wait()

        @pl.when(jnp.logical_not(mine))
        def _():
            recv(WOB + yy, piece)

    def d_out(i, s):
        rows = pl.ds(mult(blocks[i], t_loc), t_loc)
        do_v[rows, :] = lax.dot_general(tok[s], woh[...], NT, preferred_element_type=f32).astype(bf)

    def attend(i, h, between=None):
        attention_block(mult(blocks[i], t_loc), t_loc, h, c1, c2, qkv_v, do_v, p_scr, dp_scr, m_scr, kt, vt, dk_acc, dv_acc, dqkv_v, o_v, between)

    def dy_forward(j):
        forward(dyg, YB, 1, ((4, yn), (3, sib)), j)

    near_half.wait()
    far_half.wait()
    d_out(0, 0)
    attend(0, 0, lambda: dy_forward(0))
    for t in range(2, 4):
        w_own(t, 1, 1 - x, xn)
    others = (r_s, r_x, r_xs)

    def finish(h):
        c0 = 3 * D * h
        dqkv_v[:, c0 + D:c0 + 2 * D] = dk_acc[h].astype(bf)
        dqkv_v[:, c0 + 2 * D:c0 + 3 * D] = dv_acc[h].astype(bf)

    def tok_slot(rr, h, j, n, c0=0, c1=3 * D):
        return dtok.at[pl.ds(j * n, n), pl.ds(pl.multiple_of(rr * hw + 3 * D * h + c0, D), c1 - c0)]

    def send_dqkv(i, h, j, n):
        for k in (1, 2, 0):
            c0 = D if (h, k) == (0, 1) else 0
            src = dqkv_v.at[pl.ds(pl.multiple_of(others[k] * t_loc + j * n, n), n), pl.ds(3 * D * h + c0, 3 * D - c0)]
            send(i + k, src, tok_slot(r, h, j, n, c0), {'row': others[k]})

    def send_early_dq():
        src = dqkv_v.at[pl.ds(mult(r_x, t_loc), t_loc), pl.ds(0, D)]
        send(DQE, src, tok_slot(r, 0, 0, t_loc, 0, D), xn)

    loading = []

    def second_block():
        dy_forward(1)
        for kind in (0, 5):
            take(dyg, YB, kind)
        loading.append(load_tok(dyg, r_s, 1))

    def last_block():
        take(dyg, YB, 3)
        take(dyg, YB, 6)
        loading.append(load_tok(dyg, r_xs, 1))

    attend(0, 1, second_block)
    loading.pop().wait()
    d_out(1, 1)
    attend(1, 0)
    forward(dyg, YB, 4, ((6, sib),), 0)
    near_half = load_half(dyg, y, r_x, 0, 10)
    attend(1, 1)
    forward(dyg, YB, 4, ((6, sib),), 1)
    far_half = load_half(dyg, 1 - y, r_x, 0, 11)
    near_half.wait()
    far_half.wait()
    d_out(2, 0)
    attend(2, 0, last_block)
    send_early_dq()
    w_forward(2)
    loading.pop().wait()
    d_out(3, 1)
    ld = [local(5 + s, dyg.at[:, pl.ds(512 * s, 512)], col_v.at[s]) for s in range(2)]
    attend(3, 0)

    finish(0)
    send_dqkv(DQ, 0, 0, t_loc)
    attend(2, 1)
    w_forward(3)
    attend(3, 1)
    finish(1)
    for j in range(NJ):
        send_dqkv(DQ + 3 + 3 * j, 1, j, bt)
    dtok[:, pl.ds(mult(r, hw), hw)] = dqkv_v[pl.ds(mult(r, t_loc), t_loc), :]

    order = (r_x, r_xs, r_s, r)
    for s in range(4):
        ld[s].wait()
        dwo_v[:, 512 * s:512 * s + 512] = lax.dot_general(o_v[...], col_v[s % 2], TN, preferred_element_type=f32).astype(bf)
        if s < 2:
            ld.append(local(5 + s, dyg.at[:, pl.ds(512 * s + 1024, 512)], col_v.at[s]))
        else:
            ld.append(local(5 + s - 2, xg.at[:, pl.ds(mult(order[s - 2], t_loc), t_loc)], col_v.at[s - 2]))
    ld = ld[4:]
    row_to = 2 * y + x
    near = x == y
    for k in range(2):
        src = dwo_v.at[:, pl.ds(k * h_loc, h_loc)]
        dst = dwo_out.at[pl.ds(mult(c, ow), ow)]
        mine = (y == k) & (row_to == r)
        far = (y != k) & (x != y)

        @pl.when(mine)
        def _():
            pltpu.make_async_copy(src, dst, lsem.at[0]).start()

        @pl.when(far)
        def _():
            copy(DWF, DWF, src, relay, {'col': k}).start()

        @pl.when(jnp.logical_not(mine | far))
        def _():
            copy(DWO + k, DWO + c, src, dst, {'col': k, 'row': row_to}).start()

    def dw_slot(rr):
        return dw_out.at[:, pl.ds(mult(rr, hw), hw)]

    def d_w(i):
        s = i % 2
        ld[i].wait()
        part = lax.dot_general(col_v[s], dqkv_v[...], TN, preferred_element_type=f32).astype(bf)
        if i < 3:
            qkv_v[t_loc * i:t_loc * i + t_loc, :] = part
        else:
            dw_out[:, pl.ds(mult(r, hw), hw)] = part
        if i < 2:
            ld.append(local(5 + s, xg.at[:, pl.ds(mult(order[i + 2], t_loc), t_loc)], col_v.at[s]))

    def send_dw(i, k):
        send(DW + k, qkv_v.at[pl.ds(t_loc * i, t_loc)], dw_slot(r), {'row': others[k]})

    def d_x(j, half, dst):
        for n in range(h_loc // 256):
            rows = pl.ds(pl.multiple_of(half * h_loc + 256 * n, 256), 256)
            dst[pl.ds(2 * bt * j + bt * (n // 2), bt), 256 * (n % 2):256 * (n % 2) + 256] = lax.dot_general(
                dtok[pl.ds(j * bt, bt), :], w_v[rows, :], NT, preferred_element_type=f32)

    def d_x_send(j):
        for k in range(3):
            recv(DQ + 3 + 3 * j + k, tok_slot(others[k], 1, j, bt))
        d_x(j, 1 - y, dp_scr)
        part = pl.ds(2 * bt * j, 2 * bt)
        send(PX + j, dp_scr.at[part], px_recv.at[part], yn)

    d_w(0)
    send_dw(0, 1)
    d_w(1)
    send_dw(1, 2)
    for t in range(2, 4):
        recv(WB + 8 + t, wslot(r_xs, wq(t, x)))
    recv(DQE, tok_slot(r_x, 0, 0, t_loc, 0, D))
    for k in range(3):
        recv(DQ + k, tok_slot(others[k], 0, 0, t_loc, D if k == 1 else 0))
    d_x_send(0)

    @pl.when(near)
    def _():
        recv(DWF, relay)
        copy(DWG, DWG + c, relay, dwo_out.at[pl.ds(mult(c, ow), ow)], {'row': 2 * (1 - y) + x}).start()

    d_w(2)
    send_dw(2, 0)
    d_x_send(1)
    d_x(0, y, p_scr)
    d_w(3)
    d_x(1, y, p_scr)
    late = started[-(3 + NJ):]
    for cp in started[:-(3 + NJ)]:
        cp.wait_send()
    half = dwo_v.at[:, pl.ds(0, h_loc)]
    for k in range(2):
        @pl.when(jnp.logical_not((x == y) & (2 * c + k == r)))
        def _():
            copy(WOB + k, WOB + k, wo_ref.at[pl.ds(0, ow)], half, sib).wait_send()

        @pl.when(jnp.logical_not(((y == k) & (row_to == r)) | ((y != k) & (x != y))))
        def _():
            copy(DWO + k, DWO + k, half, relay, sib).wait_send()

    @pl.when(jnp.logical_not(near))
    def _():
        copy(DWF, DWF, half, relay, yn).wait_send()

    for j in range(NJ):
        recv(PX + j, px_recv.at[pl.ds(2 * bt * j, 2 * bt)])
        for q in range(2):
            part = pl.ds(2 * bt * j + bt * q, bt)
            dx_out[pl.ds(j * bt, bt), 512 * q:512 * q + 512] = (p_scr[part, :] + px_recv[part, :]).astype(bf)
    for k in range(3):
        recv(DW + k, dw_slot(others[k]))
    src_col, src_x = r // 2, lax.rem(r, 2)
    for k in range(2):
        piece = dwo_out.at[pl.ds(k * ow, ow)]
        mine = (src_col == y) & (2 * src_x + k == r)
        far = (src_col != y) & (src_x != src_col)

        @pl.when(mine)
        def _():
            pltpu.make_async_copy(dwo_v.at[:, pl.ds(0, h_loc)], piece, lsem.at[0]).wait()

        @pl.when(far)
        def _():
            recv(DWG + k, piece)

        @pl.when(jnp.logical_not(mine | far))
        def _():
            recv(DWO + k, piece)
    for cp in late:
        cp.wait_send()

    @pl.when(near)
    def _():
        copy(DWG, DWG, relay, relay, sib).wait_send()


def step_all(x_blk, w_blk, wo_blk, seg_blk, dy_blk):
    t_loc, h_loc = x_blk.shape
    w_loc = w_blk.shape[1]
    seq, hid = 4 * t_loc, 2 * h_loc
    hw, ow = w_loc // 4, w_loc // 12
    heads = ow // D
    bf, f32 = jnp.bfloat16, jnp.float32
    hbm = pl.BlockSpec(memory_space=pl.ANY)
    n_sem = 14 * NC + 12 + 2 + 3 + 3 + 3 * NJ + 3 + 2 + NJ + 1 + 2 + 1
    return pl.pallas_call(
        step_kernel,
        in_specs=[hbm] * 5,
        out_specs=[hbm] * 2 + [pl.BlockSpec(memory_space=pltpu.VMEM)] * 3,
        out_shape=[jax.ShapeDtypeStruct((seq, hid), bf)] * 2 + [pltpu.VMEM(b.shape, bf) for b in (x_blk, w_blk, wo_blk)],
        scratch_shapes=[
            pltpu.VMEM((hid, w_loc), bf), pltpu.VMEM((2, t_loc, hid), bf), pltpu.VMEM((2, seq, t_loc), bf),
            pltpu.VMEM((ow, hid), bf), pltpu.VMEM((seq, hw), bf), pltpu.VMEM((seq, ow), bf),
            pltpu.VMEM((4,) + seg_blk.shape, jnp.int32),
            pltpu.VMEM((seq, t_loc), f32), pltpu.VMEM((seq, t_loc), f32), pltpu.VMEM((seq // BK, 1, t_loc), f32),
            pltpu.VMEM((heads, D, seq), bf), pltpu.VMEM((heads, D, seq), bf),
            pltpu.VMEM((heads, seq, D), f32), pltpu.VMEM((heads, seq, D), f32),
            pltpu.VMEM((seq, hw), bf), pltpu.VMEM((seq, ow), bf),
            pltpu.VMEM((t_loc, w_loc), bf), pltpu.VMEM((ow, hid), bf), pltpu.VMEM((2 * t_loc, t_loc), f32),
            pltpu.VMEM((ow, h_loc), bf),
            pltpu.SemaphoreType.DMA((n_sem,)), pltpu.SemaphoreType.DMA((n_sem,)), pltpu.SemaphoreType.DMA((16,)),
        ],
        compiler_params=pltpu.CompilerParams(collective_id=0, has_side_effects=True, vmem_limit_bytes=STEP_LIMIT),
        name='mega_step',
    )(x_blk, w_blk, wo_blk, seg_blk, dy_blk)


def copy_kernel(parts, *refs):
    n = len(parts)
    ins, outs, sem = refs[:n], refs[n:2 * n], refs[2 * n]
    moves = []
    for i in range(n):
        step = ins[i].shape[0] // parts[i]
        for j in range(parts[i]):
            rows = pl.ds(j * step, step)
            move = pltpu.make_async_copy(ins[i].at[rows], outs[i].at[rows], sem.at[len(moves)])
            move.start()
            moves.append(move)
    for move in moves:
        move.wait()


def copy_out(*arrays):
    parts = [a.shape[0] // 512 for a in arrays]
    return pl.pallas_call(
        functools.partial(copy_kernel, parts),
        in_specs=[pl.BlockSpec(memory_space=pltpu.VMEM)] * len(arrays),
        out_specs=[pl.BlockSpec(memory_space=pl.ANY)] * len(arrays),
        out_shape=[jax.ShapeDtypeStruct(a.shape, a.dtype) for a in arrays],
        scratch_shapes=[pltpu.SemaphoreType.DMA((sum(parts),))],
        compiler_params=pltpu.CompilerParams(vmem_limit_bytes=1_000_000),
        name='copy_out',
    )(*arrays)


def solution(mesh):
    tok_spec = P(('dp', 'row'), 'col')
    mat_spec = P('row', 'col')
    seg_spec = P(('dp', 'row'))

    def grad_step(x_blk, wqkv_blk, wout_blk, seg_blk, dy_blk):
        _, _, grad_x, grad_wqkv, grad_wout = step_all(x_blk, wqkv_blk, wout_blk, seg_blk.reshape(4, -1), dy_blk)
        return copy_out(grad_x, grad_wqkv, grad_wout)

    return jax.shard_map(grad_step, mesh=mesh, in_specs=(tok_spec, mat_spec, mat_spec, seg_spec, tok_spec), out_specs=(tok_spec, tok_spec, tok_spec), check_vma=False)
```
